32 devices in a mesh: dp: 16 (over z, y, x), tensor: 2 (over core).
Axes of the slice: x: 2, y: 2, z: 4, core: 2. Of those that a mesh axis runs over, the one named last changes fastest.
Arguments:
- hidden_in: bfloat16 [4096, 2048], P('dp'), may hold values from -6 to 6
- norm_gain: bfloat16 [2048], P('dp'), may hold values from 0.099609375 to 1.8984375
- w_query: bfloat16 [2048, 3072], P('dp', 'tensor'), may hold values from -0.125 to 0.125
- w_latent: bfloat16 [2048, 576], P('dp'), may hold values from -0.125 to 0.125
- latent_gain: bfloat16 [512], P('dp'), may hold values from 0.099609375 to 1.8984375
- w_up: bfloat16 [512, 4096], P('dp', 'tensor'), may hold values from -0.25 to 0.25
- w_out: bfloat16 [2048, 2048], P('tensor', 'dp'), may hold values from -1 to 1
- ffn_gain: bfloat16 [2048], P('dp'), may hold values from 0.099609375 to 1.8984375
- shared_gate: bfloat16 [2048, 2816], P('dp', 'tensor'), may hold values from -0.125 to 0.125
- shared_up: bfloat16 [2048, 2816], P('dp', 'tensor'), may hold values from -0.125 to 0.125
- shared_down: bfloat16 [2816, 2048], P('tensor', 'dp'), may hold values from -0.109375 to 0.109375
- expert_gate: bfloat16 [16, 2048, 1408], P('dp', None, 'tensor'), may hold values from -0.125 to 0.125
- expert_up: bfloat16 [16, 2048, 1408], P('dp', None, 'tensor'), may hold values from -0.125 to 0.125
- expert_down: bfloat16 [16, 1408, 2048], P('dp', 'tensor'), may hold values from -0.625 to 0.625
- gate_values: float32 [4096, 6], P('dp'), may hold values from 0.05 to 0.8
- expert_ids: int32 [4096, 6], P('dp'), may hold values from 0 to 15, all different within a row; in each aligned block of 256 rows (0 to 255, 256 to 511, ...) at most 112 rows name the same one
- segment_ids: int32 [16, 256], P('dp'), may hold values from 0 to 1, never falling along the last dimension, each value on 1 to 200 neighbouring positions
- cotangent: float32 [4096, 2048], P('dp'), may hold values from -6 to 6
Outputs:
- output: bfloat16 [4096, 2048], P('dp')
- grad_input: float32 [4096, 2048], P('dp')
- grad_norm_gain: float32 [2048], P('dp')
- grad_w_query: float32 [2048, 3072], P('dp', 'tensor')
- grad_w_latent: float32 [2048, 576], P('dp')
- grad_latent_gain: float32 [512], P('dp')
- grad_w_up: float32 [512, 4096], P('dp', 'tensor')
- grad_w_out: float32 [2048, 2048], P('tensor', 'dp')
- grad_ffn_gain: float32 [2048], P('dp')
- grad_shared_gate: float32 [2048, 2816], P('dp', 'tensor')
- grad_shared_up: float32 [2048, 2816], P('dp', 'tensor')
- grad_shared_down: float32 [2816, 2048], P('tensor', 'dp')
- grad_expert_gate: float32 [16, 2048, 1408], P('dp', None, 'tensor')
- gradient_expert_upward: float32 [16, 2048, 1408], P('dp', None, 'tensor')
- grad_expert_down: float32 [16, 1408, 2048], P('dp', 'tensor')
The draws below stay inside these ranges and needn't reach their ends.
Inputs may be any that keep to these rules, and one draw needn't show every extreme that they name: `expert_ids`: each row names 6 different experts. Within the 256 rows of one sequence no expert is named by more than 112 rows, a bound that some block reaches. `segment_ids`: along a sequence the numbers never fall; a document holds at most 200 positions.
All inputs are finite; a program needn't handle non-finite values.
Results may differ from the reference program's by a relative error of at most 0.018.
Values may be sent and summed in bfloat16 or wider, within the bound.
A program may use at most 320 MiB of HBM per device.

```python
import math
import jax
import jax.numpy as jnp
import numpy as np
from jax import lax

D = 2048
HEADS = 16
NOPE = 128
ROPE = 64
VDIM = 128
KVRANK = 512
FE = 1408
FS = 2816
TOPK = 6
SEQ = 256
SEQS = 16
TOKENS = 4096
EXPERTS = 16
CAP = 112


def strengthened(values, key, source, target, parts, factor):
    owner, partner = [(jnp.arange(values.shape[dim]) // (values.shape[dim] // parts)).reshape([-1 if axis == dim else 1 for axis in range(values.ndim)]) for dim in (source, target)]
    chosen = jax.random.permutation(key, parts)[partner]
    strong = (owner == chosen) | (owner == (partner + parts // 2) % parts)
    return jnp.where(strong, factor * values, values)


def block_levels(own_key, dims, split, least, high):
    factor_of = 1.0
    for dim, parts in split:
        draws = jax.random.uniform(jax.random.fold_in(jax.random.fold_in(own_key, 6), dim), (parts,), jnp.float32, least / len(split), high / len(split))
        factor_of = factor_of * jnp.repeat(jnp.exp(draws), dims[dim] // parts).reshape((-1,) + (1,) * (len(dims) - 1 - dim))
    return factor_of


def profile(amount, total, reach, lean):
    loads = [(1 << 20) // math.isqrt(standing ** lean) + 1 for standing in range(2, amount + 1)]
    rest, counts = total - reach - (amount - 1), [1] * (amount - 1)
    while rest > 0:
        movable = [i for i in range(amount - 1) if counts[i] < reach]
        whole, left = sum([loads[i] for i in movable]), rest
        for i in movable:
            addition = min(reach - counts[i], max(1, left * loads[i] // whole), rest)
            counts[i] = counts[i] + addition
            rest = rest - addition
    return np.array([reach] + counts)


def uneven(stream_key, amount, total, reach, lean):
    if amount == 2:
        one = jax.random.randint(stream_key, (), max(1, total - reach), min(reach, total - 1) + 1)
        return jnp.stack([one, total - one])
    lengths = jnp.asarray(profile(amount, total, reach, lean), jnp.int32)
    twos = (amount - 1) // 2
    donor, sink = lengths[1:1 + 2 * twos:2], lengths[2:2 + 2 * twos:2]
    room = jnp.minimum(donor - 1, reach - sink)
    passed = jax.random.randint(jax.random.fold_in(stream_key, 1), (twos,), 0, 1 << 20) % (room + 1)
    lengths = lengths.at[1:1 + 2 * twos:2].set(donor - passed).at[2:2 + 2 * twos:2].set(sink + passed)
    return lengths[jax.random.permutation(jax.random.fold_in(stream_key, 2), amount)]


def routed_block(own_key, own, number, rows, amount, top, limit, skew):
    ranking = jax.random.permutation(own_key, amount)
    crowded, common = portions_of(amount, rows * top, limit, skew, True), portions_of(amount, rows * top, limit, skew, False)
    places = jnp.arange(amount)

    def named(lengths, offset_by):
        used = int((lengths > 0).sum())
        fixed = max(1, used // 4)
        moved = fixed + (places - fixed + offset_by * (used - fixed)) % max(1, amount - fixed)
        return jnp.zeros((amount,), jnp.int32).at[ranking[jnp.where(places < fixed, places, moved)]].set(jnp.asarray(lengths, jnp.int32))

    lengths = jnp.where(number % 4 == 0, named(crowded, number // 4), named(common, number - number // 4 - 1))
    mixed = jax.random.permutation(jax.random.fold_in(own, 3), amount)
    donor, sink = mixed[0:amount // 2 * 2:2], mixed[1:amount // 2 * 2:2]
    slack = jnp.minimum(lengths[donor] - 1, limit - lengths[sink]) // 2
    slack = jnp.where((donor == ranking[0]) | (sink == ranking[0]) | (lengths[sink] == 0), 0, jnp.maximum(slack, 0))
    moved = jax.random.randint(jax.random.fold_in(own, 4), (amount // 2,), 0, 1 << 20) % (slack + 1)
    lengths = lengths.at[donor].add(-moved).at[sink].add(moved)
    items = jnp.searchsorted(jnp.cumsum(lengths), jnp.arange(rows * top), side="right").astype(jnp.int32)
    listing = items.reshape(top, rows).T
    listing = listing[jax.random.permutation(jax.random.fold_in(own, 1), rows)]
    offset_by = jax.random.randint(jax.random.fold_in(own, 2), (rows, 1), 0, top)
    return jnp.take_along_axis(listing, (jnp.arange(top)[None, :] + offset_by) % top, axis=1)


def portions_of(number_of, total, limit, slope, full):
    loads = [(1 << 20) // math.isqrt(rank ** slope) + 1 for rank in range(1, number_of + 1)]
    largest = limit if full else min(limit, max(-(-total // number_of), total * loads[0] // sum(loads)))
    least = 1 if total - largest >= number_of - 1 else 0
    counts, spare = [largest] + [least] * (number_of - 1), total - largest - least * (number_of - 1)
    while spare > 0:
        movable = [i for i in range(1, number_of) if counts[i] < largest] or [i for i in range(1, number_of) if counts[i] < limit]
        mass, budget = sum([loads[i] for i in movable]), spare
        for i in movable:
            addition = min(limit - counts[i], max(1, budget * loads[i] // mass), spare)
            counts[i] = counts[i] + addition
            spare = spare - addition
    return np.array(counts)


def scatter_about(own_key, shape, width, bound, shards=(), held_as=jnp.bfloat16):
    level = block_levels(own_key, shape, shards, -0.22, 0.18) if shards else 1.0
    entries = jax.random.normal(own_key, shape, jnp.float32) * width * level
    return jnp.minimum(jnp.maximum(entries, -bound), bound).astype(held_as)


def bell_draw_with(key, shape, scale, bound, shards, heavy, kind=jnp.bfloat16):
    result = scale * jax.random.normal(key, shape, jnp.float32)
    if shards:
        result = result * block_levels(key, shape, shards, -0.22, 0.18)
    return jnp.clip(strengthened(result, jax.random.fold_in(key, 3), *heavy), -bound, bound).astype(kind)


def setup_inputs(seed: int = 0) -> dict:
    streams_of = jax.random.split(jax.random.key(seed), 19)
    hidden_in = bell_draw_with(streams_of[0], (TOKENS, D), 1.0, 6.0, ((0, 16),), (0, 1, 16, 2.0))
    norm_gain = jnp.clip(1.0 + 0.18 * jax.random.normal(streams_of[1], (D,), jnp.float32), 0.099609375, 1.8984375).astype(jnp.bfloat16)
    w_query = scatter_about(streams_of[2], (D, HEADS * (NOPE + ROPE)), D ** -0.5, 0.125, ((0, 16), (1, 2)))
    w_latent = scatter_about(streams_of[3], (D, KVRANK + ROPE), D ** -0.5, 0.125, ((0, 16),))
    latent_gain = jnp.clip(1.0 + 0.18 * jax.random.normal(streams_of[4], (KVRANK,), jnp.float32), 0.099609375, 1.8984375).astype(jnp.bfloat16)
    w_up = scatter_about(streams_of[5], (KVRANK, HEADS * (NOPE + VDIM)), KVRANK ** -0.5, 0.25, ((0, 16), (1, 2)))
    w_out = scatter_about(streams_of[6], (HEADS * VDIM, D), (max(1, HEADS * VDIM // 64)) ** -0.5, 1.0, ((0, 2), (1, 16)))
    ffn_gain = jnp.clip(1.0 + 0.18 * jax.random.normal(streams_of[7], (D,), jnp.float32), 0.099609375, 1.8984375).astype(jnp.bfloat16)
    shared_gate = scatter_about(streams_of[8], (D, FS), D ** -0.5, 0.125, ((0, 16), (1, 2)))
    shared_up = scatter_about(streams_of[9], (D, FS), D ** -0.5, 0.125, ((0, 16), (1, 2)))
    shared_down = scatter_about(streams_of[10], (FS, D), FS ** -0.5, 0.109375, ((0, 2), (1, 16)))
    expert_gate = scatter_about(streams_of[11], (EXPERTS, D, FE), D ** -0.5, 0.125, ((0, 16), (2, 2)))
    expert_up = scatter_about(streams_of[12], (EXPERTS, D, FE), D ** -0.5, 0.125, ((0, 16), (2, 2)))
    expert_down = scatter_about(streams_of[13], (EXPERTS, FE, D), (max(1, FE // 16)) ** -0.5, 0.625, ((0, 16), (1, 2)))
    gate_values = jnp.clip(jnp.exp(math.log(0.8) - 2.7725887 * jax.random.uniform(streams_of[14], (TOKENS, TOPK), jnp.float32) ** block_levels(streams_of[14], (TOKENS, TOPK), ((0, 16),), -0.2, 0.2)), 0.05, 0.8)
    expert_ids_keys = jax.random.split(jax.random.fold_in(streams_of[15], 1), TOKENS // SEQ)
    expert_ids_turns = jax.random.permutation(jax.random.fold_in(streams_of[15], 3), TOKENS // SEQ)
    expert_ids = jax.vmap(lambda own, number: routed_block(jax.random.fold_in(streams_of[15], 2), own, number, SEQ, EXPERTS, TOPK, CAP, 2))(expert_ids_keys, expert_ids_turns).reshape((TOKENS, TOPK))
    segment_ids = jax.vmap(lambda own: jnp.searchsorted(jnp.cumsum(uneven(own, 2, SEQ, max(SEQ // 2 + SEQ // 4, SEQ - 56), 2)), jnp.arange(SEQ), side="right"))(jax.random.split(streams_of[16], SEQS)).reshape((SEQS, SEQ)).astype(jnp.int32)
    cotangent = scatter_about(streams_of[17], (TOKENS, D), 1.0, 6.0, ((0, 16),), jnp.float32)
    return dict(hidden_in=hidden_in, norm_gain=norm_gain, w_query=w_query, w_latent=w_latent, latent_gain=latent_gain, w_up=w_up, w_out=w_out, ffn_gain=ffn_gain, shared_gate=shared_gate, shared_up=shared_up, shared_down=shared_down, expert_gate=expert_gate, expert_up=expert_up, expert_down=expert_down, gate_values=gate_values, expert_ids=expert_ids, segment_ids=segment_ids, cotangent=cotangent)


EPSILON = 1e-06

def rope_tables(length):
    half_width = ROPE // 2
    frequency = 10000.0 ** (-(jnp.arange(half_width, dtype=jnp.float32) * 2.0 / ROPE))
    angles = jnp.arange(length, dtype=jnp.float32)[:, None] * frequency[None, :]
    return (jnp.cos(angles), jnp.sin(angles))

def rotate(vectors, cosine, sine):
    half_width = vectors.shape[-1] // 2
    first_half = vectors[..., :half_width]
    second = vectors[..., half_width:]
    return jnp.concatenate([first_half * cosine - second * sine, second * cosine + first_half * sine], axis=-1)

def silu_slope(gate_projected):
    sigmoid_value = jax.nn.sigmoid(gate_projected)
    return sigmoid_value * (1.0 + gate_projected * (1.0 - sigmoid_value))

def rms_forward(vectors, gain):
    inverse = lax.rsqrt(lax.optimization_barrier(jnp.mean(vectors * vectors, axis=-1, keepdims=True)) + EPSILON)
    return (vectors * inverse * gain, inverse)

def rms_backward(vectors, inverse, gain, grad_out):
    scaled = gain * grad_out
    grad_in = inverse * scaled - vectors * inverse ** 3 * lax.optimization_barrier(jnp.mean(scaled * vectors, axis=-1, keepdims=True))
    return (grad_in, lax.optimization_barrier(jnp.sum(grad_out * vectors * inverse, axis=0)))

def mask_of(segment_row):
    position = jnp.arange(segment_row.shape[0], dtype=jnp.int32)
    same_doc = segment_row[:, None] == segment_row[None, :]
    return same_doc & (position[None, :] <= position[:, None])

def attention_forward(normed, w_query, w_latent, latent_gain, w_up, allowed, cosine, sine):
    length = normed.shape[0]
    head_count = w_query.shape[1] // (NOPE + ROPE)
    query_all = jnp.dot(normed, w_query, preferred_element_type=jnp.float32).reshape(length, head_count, NOPE + ROPE)
    query_rope = rotate(query_all[..., NOPE:], cosine[:, None, :], sine[:, None, :])
    queries = jnp.concatenate([query_all[..., :NOPE], query_rope], axis=-1).astype(jnp.bfloat16)
    latent_all = jnp.dot(normed, w_latent, preferred_element_type=jnp.float32)
    latent = latent_all[:, :KVRANK]
    latent_normed, latent_inverse = rms_forward(latent, latent_gain)
    latent_bf = latent_normed.astype(jnp.bfloat16)
    key_rope = rotate(latent_all[:, KVRANK:], cosine, sine).astype(jnp.bfloat16)
    expanded = jnp.dot(latent_bf, w_up, preferred_element_type=jnp.float32).astype(jnp.bfloat16)
    expanded = expanded.reshape(length, head_count, NOPE + VDIM)
    key_all = jnp.concatenate([expanded[..., :NOPE], jnp.broadcast_to(key_rope[:, None, :], (length, head_count, ROPE))], axis=-1)
    values = expanded[..., NOPE:]
    scale = (NOPE + ROPE) ** (-0.5)
    scores = jnp.einsum('qhd,khd->hqk', queries.astype(jnp.float32), key_all.astype(jnp.float32)) * scale
    raw_probs = jnp.where(allowed[None], jnp.exp(scores), 0.0)
    totals = lax.optimization_barrier(jnp.sum(raw_probs, axis=-1, keepdims=True))
    log_total = jnp.log(totals)
    attn_weights = (raw_probs / totals).astype(jnp.bfloat16)
    context = jnp.einsum('hqk,khd->qhd', attn_weights.astype(jnp.float32), values.astype(jnp.float32))
    context = context.reshape(length, head_count * VDIM).astype(jnp.bfloat16)
    return (context, queries, key_all, values, scores, log_total, latent, latent_inverse, latent_bf)

def reference(hidden_in, norm_gain, w_query, w_latent, latent_gain, w_up, w_out, ffn_gain, shared_gate, shared_up, shared_down, expert_gate, expert_up, expert_down, gate_values, expert_ids, segment_ids, cotangent):
    cosine, sine = rope_tables(SEQ)
    gain_one = norm_gain.astype(jnp.float32)
    gain_latent = latent_gain.astype(jnp.float32)
    gain_two = ffn_gain.astype(jnp.float32)
    scale = (NOPE + ROPE) ** (-0.5)
    inputs_seq = hidden_in.reshape(SEQS, SEQ, D)

    def front_part(tokens_in, segment_row):
        tokens_f = tokens_in.astype(jnp.float32)
        normed_f, inverse_one = rms_forward(tokens_f, gain_one)
        normed = normed_f.astype(jnp.bfloat16)
        allowed = mask_of(segment_row)
        saved = attention_forward(normed, w_query, w_latent, gain_latent, w_up, allowed, cosine, sine)
        residual = tokens_f + jnp.dot(saved[0], w_out, preferred_element_type=jnp.float32)
        ffn_f, inverse_two = rms_forward(residual, gain_two)
        ffn_in = ffn_f.astype(jnp.bfloat16)
        shared_gproj = jnp.dot(ffn_in, shared_gate, preferred_element_type=jnp.float32)
        shared_uproj = jnp.dot(ffn_in, shared_up, preferred_element_type=jnp.float32)
        shared_hidden = (jax.nn.silu(shared_gproj) * shared_uproj).astype(jnp.bfloat16)
        shared_out = jnp.dot(shared_hidden, shared_down, preferred_element_type=jnp.float32)
        return (tokens_f, normed, inverse_one, allowed, saved, residual, inverse_two, ffn_in, shared_gproj, shared_uproj, shared_hidden, shared_out)

    def forward_one(carried, packed):
        pieces = front_part(packed[0], packed[1])
        return (carried, (pieces[5], pieces[7], pieces[11]))
    _, (residual_all, ffn_all, shared_all) = lax.scan(forward_one, jnp.zeros((), jnp.int32), (inputs_seq, segment_ids))
    pair_count = SEQ * TOPK
    ids_seq = expert_ids.reshape(SEQS, pair_count).astype(jnp.int32)
    onehot = (ids_seq[:, :, None] == jnp.arange(EXPERTS, dtype=jnp.int32)[None, None, :]).astype(jnp.int32)
    earlier = (jnp.cumsum(onehot, axis=1) - onehot).astype(jnp.int32)
    slot_index = lax.optimization_barrier(jnp.sum(earlier * onehot, axis=2)).astype(jnp.int32)
    seq_index = jnp.arange(SEQS, dtype=jnp.int32)[:, None]
    target = (ids_seq * (SEQS * CAP) + seq_index * CAP + slot_index).astype(jnp.int32)
    global_pair = jnp.arange(SEQS * pair_count, dtype=jnp.int32)
    table = jnp.full((EXPERTS * SEQS * CAP,), SEQS * pair_count, jnp.int32)
    table = table.at[target.reshape(-1)].set(global_pair).reshape(EXPERTS, SEQS * CAP)
    ffn_flat = jnp.concatenate([ffn_all.reshape(TOKENS, D), jnp.zeros((1, D), jnp.bfloat16)], axis=0)
    cot_flat = jnp.concatenate([cotangent, jnp.zeros((1, D), jnp.float32)], axis=0)
    gate_flat = jnp.concatenate([gate_values.reshape(-1), jnp.zeros((1,), jnp.float32)], axis=0)

    def expert_one(carried, packed):
        routed_sum, back_sum = carried
        gate_matrix, upward_matrix, weight_down, pair_rows = packed
        token_rows = (pair_rows // TOPK).astype(jnp.int32)
        row_block = ffn_flat[token_rows]
        gate_projected = jnp.dot(row_block, gate_matrix, preferred_element_type=jnp.float32)
        up_proj = jnp.dot(row_block, upward_matrix, preferred_element_type=jnp.float32)
        hidden_rows = (jax.nn.silu(gate_projected) * up_proj).astype(jnp.bfloat16)
        out_rows = jnp.dot(hidden_rows, weight_down, preferred_element_type=jnp.float32).astype(jnp.bfloat16)
        weight_rows = gate_flat[pair_rows]
        routed_sum = routed_sum.at[token_rows].add(weight_rows[:, None] * out_rows.astype(jnp.float32))
        grad_rows = (weight_rows[:, None] * cot_flat[token_rows]).astype(jnp.bfloat16)
        hidden_gradient = jnp.dot(grad_rows, weight_down.T, preferred_element_type=jnp.float32)
        expert_gate_gradient = (hidden_gradient * up_proj * silu_slope(gate_projected)).astype(jnp.bfloat16)
        expert_up_gradient = (hidden_gradient * jax.nn.silu(gate_projected)).astype(jnp.bfloat16)
        down_grad = jnp.dot(hidden_rows.T, grad_rows, preferred_element_type=jnp.float32)
        gate_grad = jnp.dot(row_block.T, expert_gate_gradient, preferred_element_type=jnp.float32)
        upward_gradient = jnp.dot(row_block.T, expert_up_gradient, preferred_element_type=jnp.float32)
        returning_rows = (jnp.dot(expert_gate_gradient, gate_matrix.T, preferred_element_type=jnp.float32) + jnp.dot(expert_up_gradient, upward_matrix.T, preferred_element_type=jnp.float32)).astype(jnp.bfloat16)
        back_sum = back_sum.at[token_rows].add(returning_rows.astype(jnp.float32))
        return ((routed_sum, back_sum), (gate_grad, upward_gradient, down_grad))
    start_sums = (jnp.zeros((TOKENS + 1, D), jnp.float32), jnp.zeros((TOKENS + 1, D), jnp.float32))
    (routed_sum, back_sum), (grad_expert_gate, gradient_expert_upward, grad_expert_down) = lax.scan(expert_one, start_sums, (expert_gate, expert_up, expert_down, table))
    output = (residual_all.reshape(TOKENS, D) + shared_all.reshape(TOKENS, D) + routed_sum[:TOKENS]).astype(jnp.bfloat16)

    def backward_one(carried, packed):
        tokens_in, segment_row, cot_rows, routed_back = packed
        tokens_f, normed, inverse_one, allowed, saved, residual, inverse_two, ffn_in, shared_gproj, shared_uproj, shared_hidden, shared_out = front_part(tokens_in, segment_row)
        context, queries, key_all, values, scores, log_total, latent, latent_inverse, latent_bf = saved
        cot_bf = cot_rows.astype(jnp.bfloat16)
        grad_shidden = jnp.dot(cot_bf, shared_down.T, preferred_element_type=jnp.float32)
        grad_sgate = (grad_shidden * shared_uproj * silu_slope(shared_gproj)).astype(jnp.bfloat16)
        grad_sup = (grad_shidden * jax.nn.silu(shared_gproj)).astype(jnp.bfloat16)
        g_sdown = jnp.dot(shared_hidden.T, cot_bf, preferred_element_type=jnp.float32)
        g_sgate = jnp.dot(ffn_in.T, grad_sgate, preferred_element_type=jnp.float32)
        g_sup = jnp.dot(ffn_in.T, grad_sup, preferred_element_type=jnp.float32)
        grad_ffn = jnp.dot(grad_sgate, shared_gate.T, preferred_element_type=jnp.float32) + jnp.dot(grad_sup, shared_up.T, preferred_element_type=jnp.float32) + routed_back
        grad_res_part, g_fgain = rms_backward(residual, inverse_two, gain_two, grad_ffn)
        grad_residual = cot_rows + grad_res_part
        grad_attn = grad_residual.astype(jnp.bfloat16)
        g_out = jnp.dot(context.T, grad_attn, preferred_element_type=jnp.float32)
        grad_context = jnp.dot(grad_attn, w_out.T, preferred_element_type=jnp.float32).astype(jnp.bfloat16).reshape(SEQ, HEADS, VDIM)
        probs = jnp.where(allowed[None], jnp.exp(scores - log_total), 0.0)
        weights_back = probs.astype(jnp.bfloat16)
        grad_values = jnp.einsum('hqk,qhd->khd', weights_back.astype(jnp.float32), grad_context.astype(jnp.float32))
        grad_weights = jnp.einsum('qhd,khd->hqk', grad_context.astype(jnp.float32), values.astype(jnp.float32))
        row_delta = lax.optimization_barrier(jnp.sum(probs * grad_weights, axis=-1, keepdims=True))
        grad_scores = (probs * (grad_weights - row_delta) * scale).astype(jnp.bfloat16)
        grad_queries = jnp.einsum('hqk,khd->qhd', grad_scores.astype(jnp.float32), key_all.astype(jnp.float32))
        grad_keys = jnp.einsum('hqk,qhd->khd', grad_scores.astype(jnp.float32), queries.astype(jnp.float32))
        grad_qrope = rotate(grad_queries[..., NOPE:], cosine[:, None, :], -sine[:, None, :])
        grad_query_all = jnp.concatenate([grad_queries[..., :NOPE], grad_qrope], axis=-1).reshape(SEQ, HEADS * (NOPE + ROPE)).astype(jnp.bfloat16)
        grad_expanded = jnp.concatenate([grad_keys[..., :NOPE], grad_values], axis=-1).reshape(SEQ, HEADS * (NOPE + VDIM)).astype(jnp.bfloat16)
        g_up = jnp.dot(latent_bf.T, grad_expanded, preferred_element_type=jnp.float32)
        g_query = jnp.dot(normed.T, grad_query_all, preferred_element_type=jnp.float32)
        grad_latent_normed = jnp.dot(grad_expanded, w_up.T, preferred_element_type=jnp.float32)
        grad_key_rope = rotate(lax.optimization_barrier(jnp.sum(grad_keys[..., NOPE:], axis=1)), cosine, -sine)
        grad_latent, g_lgain = rms_backward(latent, latent_inverse, gain_latent, grad_latent_normed)
        grad_latent_all = jnp.concatenate([grad_latent, grad_key_rope], axis=-1).astype(jnp.bfloat16)
        g_latent = jnp.dot(normed.T, grad_latent_all, preferred_element_type=jnp.float32)
        grad_normed = jnp.dot(grad_query_all, w_query.T, preferred_element_type=jnp.float32) + jnp.dot(grad_latent_all, w_latent.T, preferred_element_type=jnp.float32)
        grad_in_part, g_norm = rms_backward(tokens_f, inverse_one, gain_one, grad_normed)
        grad_input = grad_residual + grad_in_part
        terms = (g_norm, g_query, g_latent, g_lgain, g_up, g_out, g_fgain, g_sgate, g_sup, g_sdown)
        carried = tuple((total_now + term_now for total_now, term_now in zip(carried, terms)))
        return (carried, grad_input)
    start_grads = (jnp.zeros((D,), jnp.float32), jnp.zeros(w_query.shape, jnp.float32), jnp.zeros(w_latent.shape, jnp.float32), jnp.zeros((KVRANK,), jnp.float32), jnp.zeros(w_up.shape, jnp.float32), jnp.zeros(w_out.shape, jnp.float32), jnp.zeros((D,), jnp.float32), jnp.zeros(shared_gate.shape, jnp.float32), jnp.zeros(shared_up.shape, jnp.float32), jnp.zeros(shared_down.shape, jnp.float32))
    routed_back_all = back_sum[:TOKENS].reshape(SEQS, SEQ, D)
    grads, grad_input = lax.scan(backward_one, start_grads, (inputs_seq, segment_ids, cotangent.reshape(SEQS, SEQ, D), routed_back_all))
    g_norm, g_query, g_latent, g_lgain, g_up, g_out, g_fgain, g_sgate, g_sup, g_sdown = grads
    return (output, grad_input.reshape(TOKENS, D), g_norm, g_query, g_latent, g_lgain, g_up, g_out, g_fgain, g_sgate, g_sup, g_sdown, grad_expert_gate, gradient_expert_upward, grad_expert_down)
```

```python
import functools

import jax
import jax.numpy as jnp
from jax import lax
from jax.experimental import pallas as pl
from jax.experimental.pallas import tpu as pltpu
from jax.sharding import PartitionSpec as P

NOPE = 128
ROPE = 64
VDIM = 128


EPSILON = 1e-06


def rope_tables(length):
    half_width = ROPE // 2
    frequency = 10000.0 ** (-(jnp.arange(half_width, dtype=jnp.float32) * 2.0 / ROPE))
    angles = jnp.arange(length, dtype=jnp.float32)[:, None] * frequency[None, :]
    return (jnp.cos(angles), jnp.sin(angles))


def rotate(vectors, cosine, sine):
    half_width = vectors.shape[-1] // 2
    first_half = vectors[..., :half_width]
    second = vectors[..., half_width:]
    return jnp.concatenate(
        [first_half * cosine - second * sine, second * cosine + first_half * sine], axis=-1
    )


def silu_slope(gate_projected):
    sigmoid_value = jax.nn.sigmoid(gate_projected)
    return sigmoid_value * (1.0 + gate_projected * (1.0 - sigmoid_value))


def rms_forward(vectors, gain):
    inverse = lax.rsqrt(jnp.mean(vectors * vectors, axis=-1, keepdims=True) + EPSILON)
    return (vectors * inverse * gain, inverse)


def rms_backward(vectors, inverse, gain, grad_out):
    scaled = gain * grad_out
    grad_in = inverse * scaled - vectors * inverse**3 * jnp.mean(
        scaled * vectors, axis=-1, keepdims=True
    )
    return (grad_in, jnp.sum(grad_out * vectors * inverse, axis=0))


def pick_owned(
    returned_rows, flat_ids, slot_index, half_rows, core_index, length, topk_count, width
):
    owned = slot_index // half_rows == core_index
    place = jnp.where(owned, flat_ids * half_rows + slot_index - core_index * half_rows, 0)
    picked = returned_rows[place].astype(jnp.float32) * owned[:, None].astype(jnp.float32)
    return picked.reshape(length, topk_count, width)


def shards(
    hidden_in,
    norm_gain,
    w_query,
    w_latent,
    latent_gain,
    w_up,
    w_out,
    ffn_gain,
    shared_gate,
    shared_up,
    shared_down,
    expert_gate,
    expert_up,
    expert_down,
    gate_values,
    expert_ids,
    segment_ids,
    cotangent,
):
    kept = (
        lax.all_gather(norm_gain, "dp", axis=0, tiled=True),
        lax.all_gather(w_query, "dp", axis=0, tiled=True),
        lax.all_gather(w_latent, "dp", axis=0, tiled=True),
        lax.all_gather(latent_gain, "dp", axis=0, tiled=True),
        lax.all_gather(w_up, "dp", axis=0, tiled=True),
        lax.all_gather(w_out, "dp", axis=1, tiled=True),
        lax.all_gather(ffn_gain, "dp", axis=0, tiled=True),
        lax.all_gather(shared_gate, "dp", axis=0, tiled=True),
        lax.all_gather(shared_up, "dp", axis=0, tiled=True),
        lax.all_gather(shared_down, "dp", axis=1, tiled=True),
    )
    (
        full_norm,
        full_query,
        full_latent,
        full_lgain,
        full_up,
        full_out,
        full_fgain,
        full_sgate,
        full_sup,
        full_sdown,
    ) = kept
    length = hidden_in.shape[0]
    width = hidden_in.shape[1]
    topk_count = expert_ids.shape[1]
    head_count = full_query.shape[1] // (NOPE + ROPE)
    kv_rank = full_up.shape[0]
    experts_total = lax.axis_size("dp")
    capacity = max(2, 2 * (length * topk_count * 7 // (12 * experts_total)))
    cosine, sine = rope_tables(length)
    scale = (NOPE + ROPE) ** (-0.5)
    segment_row = segment_ids[0]
    position = jnp.arange(length, dtype=jnp.int32)
    allowed = (segment_row[:, None] == segment_row[None, :]) & (
        position[None, :] <= position[:, None]
    )
    tokens_f = hidden_in.astype(jnp.float32)
    normed_f, inverse_one = rms_forward(tokens_f, full_norm.astype(jnp.float32))
    normed = normed_f.astype(jnp.bfloat16)
    query_all = jnp.dot(normed, full_query, preferred_element_type=jnp.float32).reshape(
        length, head_count, NOPE + ROPE
    )
    query_rope = rotate(query_all[..., NOPE:], cosine[:, None, :], sine[:, None, :])
    queries = jnp.concatenate([query_all[..., :NOPE], query_rope], axis=-1).astype(jnp.bfloat16)
    latent_all = jnp.dot(normed, full_latent, preferred_element_type=jnp.float32)
    latent = latent_all[:, :kv_rank]
    latent_normed, latent_inverse = rms_forward(latent, full_lgain.astype(jnp.float32))
    latent_bf = latent_normed.astype(jnp.bfloat16)
    key_rope = rotate(latent_all[:, kv_rank:], cosine, sine).astype(jnp.bfloat16)
    expanded = jnp.dot(latent_bf, full_up, preferred_element_type=jnp.float32).astype(jnp.bfloat16)
    expanded = expanded.reshape(length, head_count, NOPE + VDIM)
    key_all = jnp.concatenate(
        [expanded[..., :NOPE], jnp.broadcast_to(key_rope[:, None, :], (length, head_count, ROPE))],
        axis=-1,
    )
    values = expanded[..., NOPE:]
    scores = (
        jnp.einsum("qhd,khd->hqk", queries, key_all, preferred_element_type=jnp.float32) * scale
    )
    raw_probs = jnp.where(allowed[None], jnp.exp(scores), 0.0)
    totals = jnp.sum(raw_probs, axis=-1, keepdims=True)
    log_total = jnp.log(totals)
    attn_weights = (raw_probs / totals).astype(jnp.bfloat16)
    context = jnp.einsum("hqk,khd->qhd", attn_weights, values, preferred_element_type=jnp.float32)
    context = context.reshape(length, head_count * VDIM).astype(jnp.bfloat16)
    attended_part = jnp.dot(context, full_out, preferred_element_type=jnp.float32)
    attended = lax.psum(attended_part, "tensor")
    residual = tokens_f + attended
    ffn_gain_f = full_fgain.astype(jnp.float32)
    ffn_f, inverse_two = rms_forward(residual, ffn_gain_f)
    ffn_in = ffn_f.astype(jnp.bfloat16)
    pair_count = length * topk_count
    flat_ids = expert_ids.reshape(-1)
    onehot = (flat_ids[:, None] == jnp.arange(experts_total, dtype=jnp.int32)[None, :]).astype(
        jnp.int32
    )
    earlier = jnp.cumsum(onehot, axis=0) - onehot
    slot_index = jnp.sum(earlier * onehot, axis=1)
    target = flat_ids * capacity + slot_index
    pair_of_slot = (
        jnp.full((experts_total * capacity,), pair_count, jnp.int32)
        .at[target]
        .set(jnp.arange(pair_count, dtype=jnp.int32))
    )
    token_of_slot = pair_of_slot // topk_count
    ffn_padded = jnp.concatenate([ffn_in, jnp.zeros((1, width), jnp.bfloat16)], axis=0)
    outgoing = ffn_padded[token_of_slot].reshape(experts_total, capacity, width)
    cot_bf = cotangent.astype(jnp.bfloat16)
    grad_rows = (
        (gate_values[:, :, None] * cotangent[:, None, :])
        .astype(jnp.bfloat16)
        .reshape(pair_count, width)
    )
    grad_padded = jnp.concatenate([grad_rows, jnp.zeros((1, width), jnp.bfloat16)], axis=0)
    grad_outgoing = grad_padded[pair_of_slot].reshape(experts_total, capacity, width)
    half_rows = capacity // lax.axis_size("tensor")
    core_index = lax.axis_index("tensor")
    portion = lax.dynamic_slice_in_dim(outgoing, core_index * half_rows, half_rows, 1)
    grad_portion = lax.dynamic_slice_in_dim(grad_outgoing, core_index * half_rows, half_rows, 1)
    arrived_half, grad_half = (
        lax.all_to_all(portion, "dp", split_axis=0, concat_axis=0, tiled=True),
        lax.all_to_all(grad_portion, "dp", split_axis=0, concat_axis=0, tiled=True),
    )
    arrived, grad_arrived = (
        lax.all_gather(arrived_half, "tensor", axis=1, tiled=True),
        lax.all_gather(grad_half, "tensor", axis=1, tiled=True),
    )
    rows_per_expert = arrived.reshape(-1, width)
    grad_arrived = grad_arrived.reshape(-1, width)
    local_gate = expert_gate[0]
    resident_up_weight = expert_up[0]
    local_down = expert_down[0]
    gate_projected = jnp.dot(rows_per_expert, local_gate, preferred_element_type=jnp.float32)
    up_proj = jnp.dot(rows_per_expert, resident_up_weight, preferred_element_type=jnp.float32)
    expert_hidden = (jax.nn.silu(gate_projected) * up_proj).astype(jnp.bfloat16)
    expert_part = jnp.dot(expert_hidden, local_down, preferred_element_type=jnp.float32)
    shared_gproj = jnp.dot(ffn_in, full_sgate, preferred_element_type=jnp.float32)
    shared_uproj = jnp.dot(ffn_in, full_sup, preferred_element_type=jnp.float32)
    shared_hidden = (jax.nn.silu(shared_gproj) * shared_uproj).astype(jnp.bfloat16)
    shared_part = jnp.dot(shared_hidden, full_sdown, preferred_element_type=jnp.float32)
    expert_half = lax.psum_scatter(
        expert_part.reshape(experts_total, capacity, width),
        "tensor",
        scatter_dimension=1,
        tiled=True,
    )
    returned_half = lax.all_to_all(
        expert_half.astype(jnp.bfloat16), "dp", split_axis=0, concat_axis=0, tiled=True
    ).reshape(-1, width)
    picked = pick_owned(
        returned_half, flat_ids, slot_index, half_rows, core_index, length, topk_count, width
    )
    routed_part = jnp.sum(picked * gate_values[:, :, None], axis=1)
    ffn_total = lax.psum(shared_part + routed_part, "tensor")
    output = (residual + ffn_total).astype(jnp.bfloat16)
    expert_hidden_gradient = jnp.dot(grad_arrived, local_down.T, preferred_element_type=jnp.float32)
    expert_gate_gradient = (expert_hidden_gradient * up_proj * silu_slope(gate_projected)).astype(
        jnp.bfloat16
    )
    expert_up_gradient = (expert_hidden_gradient * jax.nn.silu(gate_projected)).astype(jnp.bfloat16)
    grad_expert_down = jnp.dot(expert_hidden.T, grad_arrived, preferred_element_type=jnp.float32)
    grad_expert_gate = jnp.dot(
        rows_per_expert.T, expert_gate_gradient, preferred_element_type=jnp.float32
    )
    gradient_expert_upward = jnp.dot(
        rows_per_expert.T, expert_up_gradient, preferred_element_type=jnp.float32
    )
    expert_back_part = jnp.dot(
        expert_gate_gradient, local_gate.T, preferred_element_type=jnp.float32
    ) + jnp.dot(expert_up_gradient, resident_up_weight.T, preferred_element_type=jnp.float32)
    grad_shidden = jnp.dot(cot_bf, full_sdown.T, preferred_element_type=jnp.float32)
    grad_sgate = (grad_shidden * shared_uproj * silu_slope(shared_gproj)).astype(jnp.bfloat16)
    grad_sup = (grad_shidden * jax.nn.silu(shared_gproj)).astype(jnp.bfloat16)
    g_sdown = jnp.dot(shared_hidden.T, cot_bf, preferred_element_type=jnp.float32)
    g_sgate = jnp.dot(ffn_in.T, grad_sgate, preferred_element_type=jnp.float32)
    g_sup = jnp.dot(ffn_in.T, grad_sup, preferred_element_type=jnp.float32)
    shared_back_part = jnp.dot(
        grad_sgate, full_sgate.T, preferred_element_type=jnp.float32
    ) + jnp.dot(grad_sup, full_sup.T, preferred_element_type=jnp.float32)
    back_half = lax.psum_scatter(
        expert_back_part.reshape(experts_total, capacity, width),
        "tensor",
        scatter_dimension=1,
        tiled=True,
    )
    back_returned_half = lax.all_to_all(
        back_half.astype(jnp.bfloat16), "dp", split_axis=0, concat_axis=0, tiled=True
    ).reshape(-1, width)
    back_picked = pick_owned(
        back_returned_half, flat_ids, slot_index, half_rows, core_index, length, topk_count, width
    )
    grad_ffn = lax.psum(shared_back_part + jnp.sum(back_picked, axis=1), "tensor")
    grad_res_part, g_fgain = rms_backward(residual, inverse_two, ffn_gain_f, grad_ffn)
    grad_residual = cotangent + grad_res_part
    grad_attn = grad_residual.astype(jnp.bfloat16)
    g_out = jnp.dot(context.T, grad_attn, preferred_element_type=jnp.float32)
    grad_context = (
        jnp.dot(grad_attn, full_out.T, preferred_element_type=jnp.float32)
        .astype(jnp.bfloat16)
        .reshape(length, head_count, VDIM)
    )
    probs = jnp.where(allowed[None], jnp.exp(scores - log_total), 0.0)
    weights_back = probs.astype(jnp.bfloat16)
    grad_values = jnp.einsum(
        "hqk,qhd->khd", weights_back, grad_context, preferred_element_type=jnp.float32
    )
    grad_weights = jnp.einsum(
        "qhd,khd->hqk", grad_context, values, preferred_element_type=jnp.float32
    )
    row_delta = jnp.sum(probs * grad_weights, axis=-1, keepdims=True)
    grad_scores = (probs * (grad_weights - row_delta) * scale).astype(jnp.bfloat16)
    grad_queries = jnp.einsum(
        "hqk,khd->qhd", grad_scores, key_all, preferred_element_type=jnp.float32
    )
    grad_keys = jnp.einsum("hqk,qhd->khd", grad_scores, queries, preferred_element_type=jnp.float32)
    grad_qrope = rotate(grad_queries[..., NOPE:], cosine[:, None, :], -sine[:, None, :])
    grad_query_all = (
        jnp.concatenate([grad_queries[..., :NOPE], grad_qrope], axis=-1)
        .reshape(length, head_count * (NOPE + ROPE))
        .astype(jnp.bfloat16)
    )
    grad_expanded = (
        jnp.concatenate([grad_keys[..., :NOPE], grad_values], axis=-1)
        .reshape(length, head_count * (NOPE + VDIM))
        .astype(jnp.bfloat16)
    )
    g_up = jnp.dot(latent_bf.T, grad_expanded, preferred_element_type=jnp.float32)
    g_query = jnp.dot(normed.T, grad_query_all, preferred_element_type=jnp.float32)
    latent_part = jnp.dot(grad_expanded, full_up.T, preferred_element_type=jnp.float32)
    rope_part = rotate(jnp.sum(grad_keys[..., NOPE:], axis=1), cosine, -sine)
    grad_latent_normed, grad_key_rope = lax.psum((latent_part, rope_part), "tensor")
    grad_latent, g_lgain = rms_backward(
        latent, latent_inverse, full_lgain.astype(jnp.float32), grad_latent_normed
    )
    grad_latent_all = jnp.concatenate([grad_latent, grad_key_rope], axis=-1).astype(jnp.bfloat16)
    g_latent = jnp.dot(normed.T, grad_latent_all, preferred_element_type=jnp.float32)
    input_part = jnp.dot(grad_query_all, full_query.T, preferred_element_type=jnp.float32)
    grad_normed = lax.psum(input_part, "tensor") + jnp.dot(
        grad_latent_all, full_latent.T, preferred_element_type=jnp.float32
    )
    grad_in_part, g_norm = rms_backward(
        tokens_f, inverse_one, full_norm.astype(jnp.float32), grad_normed
    )
    grad_input = grad_residual + grad_in_part
    summed = (
        lax.psum_scatter(g_norm, "dp", scatter_dimension=0, tiled=True),
        lax.psum_scatter(g_query, "dp", scatter_dimension=0, tiled=True),
        lax.psum_scatter(g_latent, "dp", scatter_dimension=0, tiled=True),
        lax.psum_scatter(g_lgain, "dp", scatter_dimension=0, tiled=True),
        lax.psum_scatter(g_up, "dp", scatter_dimension=0, tiled=True),
        lax.psum_scatter(g_out, "dp", scatter_dimension=1, tiled=True),
        lax.psum_scatter(g_fgain, "dp", scatter_dimension=0, tiled=True),
        lax.psum_scatter(g_sgate, "dp", scatter_dimension=0, tiled=True),
        lax.psum_scatter(g_sup, "dp", scatter_dimension=0, tiled=True),
        lax.psum_scatter(g_sdown, "dp", scatter_dimension=1, tiled=True),
    )
    s_norm, s_query, s_latent, s_lgain, s_up, s_out, s_fgain, s_sgate, s_sup, s_sdown = summed
    return (
        output,
        grad_input,
        s_norm,
        s_query,
        s_latent,
        s_lgain,
        s_up,
        s_out,
        s_fgain,
        s_sgate,
        s_sup,
        s_sdown,
        grad_expert_gate[None],
        gradient_expert_upward[None],
        grad_expert_down[None],
    )


MESH = pl.DeviceIdType.MESH


def place_of(grid):
    index = lax.axis_index("dp")
    place = []
    for size in reversed(grid):
        place.append(lax.rem(index, size))
        index = index // size
    return tuple(reversed(place)) + (lax.axis_index("tensor"),)


def device_at(grid, place):
    index = place[0]
    for size, spot in zip(grid[1:], place[1:-1]):
        index = index * size + spot
    return (index, place[-1])


def moved(place, dim, spot):
    return tuple(spot if axis == dim else at for axis, at in enumerate(place))


def greet(grid, place):
    sizes = grid + (2,)
    barrier = pltpu.get_barrier_semaphore()
    for dim, size in enumerate(sizes):
        for step in (-1, 1):
            if size == 2:
                if step == 1:
                    pl.semaphore_signal(barrier, inc=1, device_id=device_at(grid, moved(place, dim, 1 - place[dim])), device_id_type=MESH)
                continue
            spot = place[dim] + step

            @pl.when((spot >= 0) & (spot < size))
            def _():
                pl.semaphore_signal(barrier, inc=1, device_id=device_at(grid, moved(place, dim, spot)), device_id_type=MESH)

    peers = 0
    for dim, size in enumerate(sizes):
        if size == 2:
            peers += 1
        else:
            peers += jnp.minimum(place[dim], 1) + jnp.minimum(size - 1 - place[dim], 1)
    pl.semaphore_wait(barrier, peers)


def stage_plan(sizes, order, weight, first):
    plan, now, held = [], 0.0, 1
    for dim in order:
        for step in range(sizes[dim] - 1):
            cost = weight * held * (0.15 if dim == 3 else 1.0)
            plan.append((now, dim, step))
            now += cost
        held *= sizes[dim]
    plan.append((now, None, 0))
    return plan


def gather_body(grid, pieces, shared_flags, input_count, *refs):
    sizes = grid + (2,)
    inputs = refs[:input_count]
    outputs = refs[input_count : 2 * input_count]
    send_sem, recv_sem, own_sem = refs[2 * input_count :]
    place = place_of(grid)

    def window(number, piece, chosen):
        which, start, rows, order = piece
        spots = tuple(chosen.get(dim, place[dim]) for dim in range(4 if shared_flags[which] else 3))
        return outputs[which].at[spots + (pl.ds(start, rows),)]

    own = []
    for number, piece in enumerate(pieces):
        which, start, rows, order = piece
        copy = pltpu.make_async_copy(inputs[which].at[pl.ds(start, rows)], window(number, piece, {}), own_sem.at[number])
        copy.start()
        own.append(copy)
    greet(grid, place)

    stages = []
    for number, piece in enumerate(pieces):
        which, start, rows, order = piece
        weight = rows * inputs[which].shape[1]
        for rank, (when, dim, step) in enumerate(stage_plan(sizes, order, weight, 0.0)):
            stages.append((when, number, rank, dim, step))
    stages.sort(key=lambda s: s[:3])
    pending_recv = {number: [] for number in range(len(pieces))}
    sends = []
    slot_of = {}

    def copies(number, rank, dim, step):
        piece = pieces[number]
        which, start, rows, order = piece
        gathered = {}
        for earlier in order[: order.index(dim)]:
            gathered[earlier] = slice(None)
        size = sizes[dim]
        made = []
        base = 2 * rank
        if size == 2:
            part = window(number, piece, gathered)
            if not gathered:
                source = inputs[which].at[pl.ds(start, rows)]
            else:
                source = part
            copy = pltpu.make_async_remote_copy(
                source, part, send_sem.at[number, base], recv_sem.at[number, base],
                device_id=device_at(grid, moved(place, dim, 1 - place[dim])), device_id_type=MESH)
            made.append((None, None, copy))
            return made
        for way, sign in enumerate((1, -1)):
            spot = place[dim] + sign
            block = place[dim] - sign * step
            inside = (spot >= 0) & (spot < size) & (block >= 0) & (block < size)
            back = place[dim] - sign
            back_block = back - sign * step
            arrives = (back >= 0) & (back < size) & (back_block >= 0) & (back_block < size)
            chosen = dict(gathered)
            chosen[dim] = jnp.clip(block, 0, size - 1)
            part = window(number, piece, chosen)
            if not gathered and step == 0:
                source = inputs[which].at[pl.ds(start, rows)]
            else:
                source = part
            copy = pltpu.make_async_remote_copy(
                source, part, send_sem.at[number, base + way], recv_sem.at[number, base + way],
                device_id=device_at(grid, moved(place, dim, jnp.clip(spot, 0, size - 1))), device_id_type=MESH)
            made.append((inside, arrives, copy))
        return made

    for when, number, rank, dim, step in stages:
        for condition, copy in pending_recv[number]:
            if condition is None:
                copy.wait_recv()
            else:
                pl.when(condition)(copy.wait_recv)
        pending_recv[number] = []
        if rank == 1:
            own[number].wait()
        if dim is None:
            continue
        for send_ok, recv_ok, copy in copies(number, rank, dim, step):
            if send_ok is None:
                copy.start()
            else:
                pl.when(send_ok)(copy.start)
            sends.append((send_ok, copy))
            pending_recv[number].append((recv_ok, copy))
    for condition, copy in sends:
        if condition is None:
            copy.wait_send()
        else:
            pl.when(condition)(copy.wait_send)


def gather(grid, arrays, shared_flags, pieces, collective_id):
    out_shape = [
        jax.ShapeDtypeStruct(grid + ((2,) if shared else ()) + array.shape, array.dtype)
        for array, shared in zip(arrays, shared_flags)
    ]
    most = sum(size - 1 for size in grid) + 1
    return pl.pallas_call(
        functools.partial(gather_body, grid, pieces, shared_flags, len(arrays)),
        out_shape=out_shape,
        in_specs=[pl.BlockSpec(memory_space=pltpu.VMEM)] * len(arrays),
        out_specs=[pl.BlockSpec(memory_space=pl.ANY)] * len(arrays),
        scratch_shapes=[
            pltpu.SemaphoreType.DMA((len(pieces), 2 * most)),
            pltpu.SemaphoreType.DMA((len(pieces), 2 * most)),
            pltpu.SemaphoreType.DMA((len(pieces),)),
        ],
        compiler_params=pltpu.CompilerParams(collective_id=collective_id, has_side_effects=True, vmem_limit_bytes=16 << 20),
        name="gather_rows",
    )(*arrays)


def reduce_plan(sizes, order, weight):
    plan, now, held = [], 0.0, 1
    for dim in order:
        held *= sizes[dim]
    for dim in order:
        held //= sizes[dim]
        for step in range(sizes[dim] - 1):
            plan.append((now, dim, step))
            now += weight * held * (0.25 if dim == 3 else 1.0)
    plan.append((now, None, 0))
    return plan


def landing_shapes(sizes, order, rows, width):
    shapes = []
    for rank, dim in enumerate(order):
        left = tuple(sizes[d] for d in sorted(order[rank + 1 :]))
        ways = 1 if sizes[dim] == 2 else 2
        shapes.extend([left + (rows, width)] * (ways * (sizes[dim] - 1)))
    return shapes


def kept_index(place, later, dim, dims, kept, spots):
    left = sorted(later)
    return tuple(spots[left.index(d)] if d in later else (kept if d == dim else place[d]) for d in range(dims))


def add_into(target, target_index, source, lead, rows):
    chunk = 16
    total = 1
    for size in lead:
        total *= size

    def step(number, carry):
        block, row = number // (rows // chunk), lax.rem(number, rows // chunk)
        spots, rest = [], block
        for size in reversed(lead):
            spots.append(lax.rem(rest, size))
            rest = rest // size
        spots = tuple(reversed(spots))
        span = pl.ds(pl.multiple_of(row * chunk, chunk), chunk)
        here = target_index(spots) + (span,)
        value = target[here].astype(jnp.float32) + source[spots + (span,)].astype(jnp.float32)
        target[here] = value.astype(target.dtype)
        return carry

    lax.fori_loop(0, total * (rows // chunk), step, 0)


def reduce_body(grid, pieces, shared_flags, input_count, *refs):
    sizes = grid + (2,)
    inputs = refs[:input_count]
    outputs = refs[input_count : 2 * input_count]
    scratch = list(refs[2 * input_count :])
    held = [scratch.pop(0) for _ in pieces]
    landings = []
    for which, start, rows, order in pieces:
        count = len(landing_shapes(sizes, order, rows, inputs[which].shape[-1]))
        landings.append([scratch.pop(0) for _ in range(count)])
    send_sem, recv_sem, own_sem = scratch
    place = place_of(grid)

    loads = []
    for number, (which, start, rows, order) in enumerate(pieces):
        dims = 4 if shared_flags[which] else 3
        source = inputs[which].at[(slice(None),) * dims + (pl.ds(start, rows),)]
        copy = pltpu.make_async_copy(source, held[number], own_sem.at[number])
        copy.start()
        loads.append(copy)
    greet(grid, place)

    stages = []
    for number, (which, start, rows, order) in enumerate(pieces):
        weight = rows * inputs[which].shape[-1]
        slot = 0
        for rank, (when, dim, step) in enumerate(reduce_plan(sizes, order, weight)):
            stages.append((when, number, rank, dim, step))
    stages.sort(key=lambda s: s[:3])
    pending = {number: [] for number in range(len(pieces))}
    slots = {number: 0 for number in range(len(pieces))}
    sends = []

    for when, number, rank, dim, step in stages:
        which, start, rows, order = pieces[number]
        width = inputs[which].shape[-1]
        dims = 4 if shared_flags[which] else 3
        if rank == 0:
            loads[number].wait()
        for arrives, copy, add in pending[number]:
            if arrives is None:
                copy.wait_recv()
                add()
            else:

                @pl.when(arrives)
                def _():
                    copy.wait_recv()
                    add()

        pending[number] = []
        if dim is None:
            result = outputs[which]

            def finish(chunk_number, carry):
                span = pl.ds(pl.multiple_of(chunk_number * 16, 16), 16)
                value = held[number][tuple(place[:dims]) + (span,)].astype(jnp.float32)
                result[pl.ds(pl.multiple_of(start + chunk_number * 16, 16), 16)] = value
                return carry

            lax.fori_loop(0, rows // 16, finish, 0)
            continue
        later = order[order.index(dim) + 1 :]
        lead = tuple(sizes[d] for d in sorted(later))
        size = sizes[dim]

        def whole(block):
            return tuple(slice(None) if d in later else (block if d == dim else place[d]) for d in range(dims))

        for sign in (1,) if size == 2 else (1, -1):
            landing = landings[number][slots[number]]
            sem = slots[number]
            slots[number] += 1
            if size == 2:
                to, block, kept = 1 - place[dim], 1 - place[dim], place[dim]
                goes = arrives = None
            else:
                to = place[dim] + sign
                block = place[dim] + sign * (size - 1 - step)
                back = place[dim] - sign
                kept = place[dim] + sign * (size - 2 - step)
                goes = (to >= 0) & (to < size) & (block >= 0) & (block < size)
                arrives = (back >= 0) & (back < size) & (kept >= 0) & (kept < size)
                to, block, kept = (jnp.clip(v, 0, size - 1) for v in (to, block, kept))
            copy = pltpu.make_async_remote_copy(
                held[number].at[whole(block)], landing, send_sem.at[number, sem], recv_sem.at[number, sem],
                device_id=device_at(grid, moved(place, dim, to)), device_id_type=MESH)
            if goes is None:
                copy.start()
            else:
                pl.when(goes)(copy.start)
            sends.append((goes, copy))

            index = functools.partial(kept_index, place, later, dim, dims, kept)
            add = functools.partial(add_into, held[number], index, landing, lead, rows)
            pending[number].append((arrives, copy, add))
    for condition, copy in sends:
        if condition is None:
            copy.wait_send()
        else:
            pl.when(condition)(copy.wait_send)


def reduce(grid, arrays, shared_flags, pieces, collective_id):
    sizes = grid + (2,)
    out_shape = [
        jax.ShapeDtypeStruct(array.shape[-2:], jnp.float32)
        for array in arrays
    ]
    scratch, most = [], 1
    for which, start, rows, order in pieces:
        scratch.append(pltpu.VMEM(arrays[which].shape[:-2] + (rows, arrays[which].shape[-1]), arrays[which].dtype))
    for which, start, rows, order in pieces:
        shapes = landing_shapes(sizes, order, rows, arrays[which].shape[-1])
        most = max(most, len(shapes) + 1)
        scratch.extend(pltpu.VMEM(shape, arrays[which].dtype) for shape in shapes)
    return pl.pallas_call(
        functools.partial(reduce_body, grid, pieces, shared_flags, len(arrays)),
        out_shape=out_shape,
        in_specs=[pl.BlockSpec(memory_space=pl.ANY)] * len(arrays),
        out_specs=[pl.BlockSpec(memory_space=pltpu.VMEM)] * len(arrays),
        scratch_shapes=scratch + [
            pltpu.SemaphoreType.DMA((len(pieces), most)),
            pltpu.SemaphoreType.DMA((len(pieces), most)),
            pltpu.SemaphoreType.DMA((len(pieces),)),
        ],
        compiler_params=pltpu.CompilerParams(collective_id=collective_id, has_side_effects=True, vmem_limit_bytes=60 << 20),
        name="reduce_rows",
    )(*arrays)


def pair_body(grid, keep, count, *refs):
    inputs, outputs = refs[:count], refs[count : 2 * count]
    send_sem, recv_sem, own_sem = refs[2 * count :]
    place = place_of(grid)
    partner = device_at(grid, moved(place, 3, 1 - place[3]))
    barrier = pltpu.get_barrier_semaphore()
    pl.semaphore_signal(barrier, inc=1, device_id=partner, device_id_type=MESH)
    own = []
    for number in range(count if keep else 0):
        copy = pltpu.make_async_copy(inputs[number], outputs[number].at[place[3]], own_sem.at[number])
        copy.start()
        own.append(copy)
    pl.semaphore_wait(barrier, 1)
    sent = []
    for number in range(count):
        target = outputs[number].at[place[3]] if keep else outputs[number]
        copy = pltpu.make_async_remote_copy(
            inputs[number], target, send_sem.at[number], recv_sem.at[number],
            device_id=partner, device_id_type=MESH)
        copy.start()
        sent.append(copy)
    for copy in own + sent:
        copy.wait()


def pair(grid, arrays, keep, collective_id):
    count = len(arrays)
    return pl.pallas_call(
        functools.partial(pair_body, grid, keep, count),
        out_shape=[jax.ShapeDtypeStruct(((2,) if keep else ()) + array.shape, array.dtype) for array in arrays],
        in_specs=[pl.BlockSpec(memory_space=pltpu.VMEM if keep else pl.ANY)] * count,
        out_specs=[pl.BlockSpec(memory_space=pl.ANY)] * count,
        scratch_shapes=[pltpu.SemaphoreType.DMA((count,))] * 3,
        compiler_params=pltpu.CompilerParams(
            collective_id=collective_id, has_side_effects=True, vmem_limit_bytes=16 << 20),
        name="pair_rows",
    )(*arrays)


Z, Y, X, C = 0, 1, 2, 3


def cut(which, rows, orders, core_last=False, core_first=False):
    chunks = rows // 16
    total = sum(share for share, _ in orders)
    pieces, start, used = [], 0, 0
    for share, order in orders:
        used += share
        end = chunks * used // total * 16
        if end > start:
            full = ((C,) if core_first else ()) + order + ((C,) if core_last else ())
            pieces.append((which, start, end - start, full))
            start = end
    return pieces


GATHER_ORDERS = ((2, (Z, Y, X)), (2, (Z, X, Y)), (1, (Z, Y, X)), (1, (Z, X, Y)), (2, (Y, X, Z)))
REDUCE_ORDERS = ((1, (X, Y, Z)), (1, (Y, X, Z))) * 3 + ((1, (Z, X, Y)),) * 2
REDUCE_COARSE = ((2, (X, Y, Z)), (2, (Y, X, Z)), (1, (X, Y, Z)), (1, (Y, X, Z)), (2, (Z, X, Y)))


def dense_shards(
    grid,
    hidden_in,
    norm_gain,
    w_query,
    w_latent,
    latent_gain,
    w_up,
    w_out,
    ffn_gain,
    shared_gate,
    shared_up,
    shared_down,
    expert_gate,
    expert_up,
    expert_down,
    gate_values,
    expert_ids,
    segment_ids,
    cotangent,
):
    f32, bf16 = jnp.float32, jnp.bfloat16
    length, width = hidden_in.shape
    half = length // 2
    topk_count = expert_ids.shape[1]
    chips = lax.axis_size("dp")
    head_count = w_query.shape[1] // (NOPE + ROPE)
    kv_rank = latent_gain.shape[0] * chips
    capacity = max(2, 2 * (length * topk_count * 7 // (12 * chips)))
    core = lax.axis_index("tensor")
    chip = lax.axis_index("dp")

    def rows_of(array, which):
        count = array.shape[0] // 2
        return lax.dynamic_slice_in_dim(array, which * count, count, 0)

    part_units = shared_gate.shape[1] // chips
    model_rows = shared_gate.shape[0]
    stacked = jnp.stack([shared_gate, shared_up, shared_down.T]).reshape(3, model_rows, chips, part_units)
    resharded = lax.all_to_all(stacked.transpose(2, 0, 1, 3), "dp", split_axis=0, concat_axis=0, tiled=True)
    s_gate, s_up, s_down_t = (resharded[:, i].reshape(width, part_units) for i in range(3))

    gain_rows = norm_gain.shape[0]
    latent_rows = latent_gain.shape[0]
    gains = jnp.zeros((16, 3 * gain_rows), bf16)
    gains = gains.at[0, :gain_rows].set(norm_gain).at[0, gain_rows : 2 * gain_rows].set(ffn_gain)
    gains = gains.at[0, 2 * gain_rows : 2 * gain_rows + latent_rows].set(latent_gain)
    named = expert_ids[:, :, None] == jnp.arange(chips, dtype=jnp.int32)[None, None, :]
    gate_map = jnp.sum(jnp.where(named, gate_values[:, :, None], 0.0), axis=1).T
    mine = [w_query, w_out.T, w_up, rows_of(w_latent, core), gains, gate_map]
    shared = [False, False, False, True, False, False]
    pieces = (
        cut(0, mine[0].shape[0], GATHER_ORDERS)
        + cut(1, mine[1].shape[0], GATHER_ORDERS)
        + cut(2, mine[2].shape[0], ((1, (Z, Y, X)), (1, (Z, X, Y))))
        + cut(3, mine[3].shape[0], ((1, (X, Y, Z)),), core_last=True)
        + cut(4, mine[4].shape[0], ((1, (Z, Y, X)),))
        + cut(5, mine[5].shape[0], ((1, (Z, X, Y)),))
    )
    got = gather(grid, mine, shared, pieces, 1)
    full_query = got[0].reshape(width, -1)
    full_out_t = got[1].reshape(width, -1)
    full_up = got[2].reshape(kv_rank, -1)
    full_latent = got[3].reshape(width, -1)
    all_gains = got[4].reshape(chips, 16, -1)[:, 0].astype(f32)
    gain_one = all_gains[:, :gain_rows].reshape(-1)
    gain_two = all_gains[:, gain_rows : 2 * gain_rows].reshape(-1)
    gain_latent = all_gains[:, 2 * gain_rows : 2 * gain_rows + latent_rows].reshape(-1)
    gates = lax.dynamic_index_in_dim(got[5].reshape(chips, -1, length), chip, 1, keepdims=False)

    cosine, sine = rope_tables(length)
    scale = (NOPE + ROPE) ** (-0.5)
    segment_row = segment_ids[0]
    position = jnp.arange(length, dtype=jnp.int32)
    allowed = (segment_row[:, None] == segment_row[None, :]) & (
        position[None, :] <= position[:, None]
    )
    tokens_f = hidden_in.astype(f32)
    normed_f, inverse_one = rms_forward(tokens_f, gain_one)
    normed = normed_f.astype(bf16)
    query_all = jnp.dot(normed, full_query, preferred_element_type=f32).reshape(
        length, head_count, NOPE + ROPE
    )
    query_rope = rotate(query_all[..., NOPE:], cosine[:, None, :], sine[:, None, :])
    queries = jnp.concatenate([query_all[..., :NOPE], query_rope], axis=-1).astype(bf16)
    latent_all = jnp.dot(normed, full_latent, preferred_element_type=f32)
    latent = latent_all[:, :kv_rank]
    latent_normed, latent_inverse = rms_forward(latent, gain_latent)
    latent_bf = latent_normed.astype(bf16)
    key_rope = rotate(latent_all[:, kv_rank:], cosine, sine).astype(bf16)
    expanded = jnp.dot(latent_bf, full_up, preferred_element_type=f32).astype(bf16)
    expanded = expanded.reshape(length, head_count, NOPE + VDIM)
    key_all = jnp.concatenate(
        [expanded[..., :NOPE], jnp.broadcast_to(key_rope[:, None, :], (length, head_count, ROPE))],
        axis=-1,
    )
    values = expanded[..., NOPE:]
    scores = jnp.einsum("qhd,khd->hqk", queries, key_all, preferred_element_type=f32) * scale
    raw_probs = jnp.where(allowed[None], jnp.exp(scores), 0.0)
    totals = jnp.sum(raw_probs, axis=-1, keepdims=True)
    log_total = jnp.log(totals)
    attn_weights = (raw_probs / totals).astype(bf16)
    context = jnp.einsum("hqk,khd->qhd", attn_weights, values, preferred_element_type=f32)
    context = context.reshape(length, head_count * VDIM).astype(bf16)
    attended_part = lax.dot_general(
        context, full_out_t, (((1,), (1,)), ((), ())), preferred_element_type=f32
    )
    (other,) = pair(grid, [rows_of(attended_part, 1 - core)], False, 5)
    residual = rows_of(tokens_f, core) + (rows_of(attended_part, core) + other)
    ffn_f, inverse_two = rms_forward(residual, gain_two)
    ffn_in = ffn_f.astype(bf16)

    cot_half = rows_of(cotangent, core)
    pieces = cut(0, half, GATHER_ORDERS, core_last=True) + cut(1, half, GATHER_ORDERS, core_last=True)
    ffn_all, cot_all = gather(grid, [ffn_in, cot_half.astype(bf16)], [True, True], pieces, 2)
    ffn_all = ffn_all.reshape(-1, width)
    cot_all = cot_all.reshape(-1, width)

    routed = gates > 0.0
    triangle = (position[:, None] < position[None, :]).astype(bf16)
    slot = jnp.dot(routed.astype(bf16), triangle, preferred_element_type=f32).astype(jnp.int32)
    chosen = routed[:, None, :] & (slot[:, None, :] == jnp.arange(capacity, dtype=jnp.int32)[None, :, None])
    pick = chosen.astype(bf16)
    gate_slot = jnp.sum(jnp.where(chosen, gates[:, None, :], 0.0), axis=-1)[..., None]

    def take(rows):
        return jnp.einsum(
            "sct,std->scd", pick, rows.reshape(chips, length, width), preferred_element_type=f32
        )

    def spread(rows):
        return jnp.einsum(
            "sct,scd->std", pick, rows.reshape(chips, capacity, width), preferred_element_type=f32
        ).reshape(chips * length, width)

    expert_rows = take(ffn_all).astype(bf16).reshape(-1, width)
    grad_rows = (gate_slot * take(cot_all)).astype(bf16).reshape(-1, width)
    gate_rows = gate_slot.reshape(-1, 1)
    local_gate, local_up, local_down = expert_gate[0], expert_up[0], expert_down[0]
    gate_projected = jnp.dot(expert_rows, local_gate, preferred_element_type=f32)
    up_projected = jnp.dot(expert_rows, local_up, preferred_element_type=f32)
    expert_hidden = (jax.nn.silu(gate_projected) * up_projected).astype(bf16)
    expert_part = jnp.dot(expert_hidden, local_down, preferred_element_type=f32)
    weighted = (gate_rows * expert_part).astype(bf16)
    shared_g = jnp.dot(ffn_all, s_gate, preferred_element_type=f32)
    shared_u = jnp.dot(ffn_all, s_up, preferred_element_type=f32)
    shared_hidden = (jax.nn.silu(shared_g) * shared_u).astype(bf16)
    shared_part = lax.dot_general(
        shared_hidden, s_down_t, (((1,), (1,)), ((), ())), preferred_element_type=f32
    )
    forward_part = (shared_part + spread(weighted)).astype(bf16)
    block_shape = grid + (2, half, width)
    reduce_pieces = cut(0, half, REDUCE_ORDERS, core_first=True)
    (ffn_total,) = reduce(grid, [forward_part.reshape(block_shape)], [True], reduce_pieces, 3)
    output_half = (residual + ffn_total).astype(bf16)

    hidden_gradient = lax.dot_general(
        grad_rows, local_down, (((1,), (1,)), ((), ())), preferred_element_type=f32
    )
    gate_gradient = (hidden_gradient * up_projected * silu_slope(gate_projected)).astype(bf16)
    up_gradient = (hidden_gradient * jax.nn.silu(gate_projected)).astype(bf16)
    back_part = lax.dot_general(
        gate_gradient, local_gate, (((1,), (1,)), ((), ())), preferred_element_type=f32
    ) + lax.dot_general(up_gradient, local_up, (((1,), (1,)), ((), ())), preferred_element_type=f32)
    shared_hg = jnp.dot(cot_all, s_down_t, preferred_element_type=f32)
    grad_sgate = (shared_hg * shared_u * silu_slope(shared_g)).astype(bf16)
    grad_sup = (shared_hg * jax.nn.silu(shared_g)).astype(bf16)
    shared_back = lax.dot_general(
        grad_sgate, s_gate, (((1,), (1,)), ((), ())), preferred_element_type=f32
    ) + lax.dot_general(grad_sup, s_up, (((1,), (1,)), ((), ())), preferred_element_type=f32)
    backward_part = (shared_back + spread(back_part.astype(bf16))).astype(bf16)
    (grad_ffn,) = reduce(grid, [backward_part.reshape(block_shape)], [True], reduce_pieces, 3)

    grad_expert_down = jnp.dot(expert_hidden.T, grad_rows, preferred_element_type=f32)
    grad_expert_gate = jnp.dot(expert_rows.T, gate_gradient, preferred_element_type=f32)
    gradient_expert_upward = jnp.dot(expert_rows.T, up_gradient, preferred_element_type=f32)
    shared_grads = jnp.stack(
        [
            jnp.dot(ffn_all.T, grad_sgate, preferred_element_type=f32),
            jnp.dot(ffn_all.T, grad_sup, preferred_element_type=f32),
            jnp.dot(cot_all.T, shared_hidden, preferred_element_type=f32),
        ]
    ).astype(bf16)
    returned = lax.all_to_all(
        shared_grads.reshape(3, chips, model_rows, part_units).transpose(1, 0, 2, 3),
        "dp",
        split_axis=0,
        concat_axis=0,
        tiled=True,
    )
    returned = returned.transpose(1, 2, 0, 3).reshape(3, model_rows, -1).astype(f32)
    s_sgate, s_sup, s_sdown = returned[0], returned[1], returned[2].T

    grad_res_part, g_fgain = rms_backward(residual, inverse_two, gain_two, grad_ffn)
    grad_residual = cot_half + grad_res_part
    (grad_attn,) = pair(grid, [grad_residual.astype(bf16)], True, 6)
    grad_attn = grad_attn.reshape(length, width)
    g_out_t = jnp.dot(grad_attn.T, context, preferred_element_type=f32)
    grad_context = (
        jnp.dot(grad_attn, full_out_t, preferred_element_type=f32)
        .astype(bf16)
        .reshape(length, head_count, VDIM)
    )
    probs = jnp.where(allowed[None], jnp.exp(scores - log_total), 0.0)
    weights_back = probs.astype(bf16)
    grad_values = jnp.einsum("hqk,qhd->khd", weights_back, grad_context, preferred_element_type=f32)
    grad_weights = jnp.einsum("qhd,khd->hqk", grad_context, values, preferred_element_type=f32)
    row_delta = jnp.sum(probs * grad_weights, axis=-1, keepdims=True)
    grad_scores = (probs * (grad_weights - row_delta) * scale).astype(bf16)
    grad_queries = jnp.einsum("hqk,khd->qhd", grad_scores, key_all, preferred_element_type=f32)
    grad_keys = jnp.einsum("hqk,qhd->khd", grad_scores, queries, preferred_element_type=f32)
    grad_qrope = rotate(grad_queries[..., NOPE:], cosine[:, None, :], -sine[:, None, :])
    grad_query_all = (
        jnp.concatenate([grad_queries[..., :NOPE], grad_qrope], axis=-1)
        .reshape(length, head_count * (NOPE + ROPE))
        .astype(bf16)
    )
    grad_expanded = (
        jnp.concatenate([grad_keys[..., :NOPE], grad_values], axis=-1)
        .reshape(length, head_count * (NOPE + VDIM))
        .astype(bf16)
    )
    g_up = jnp.dot(latent_bf.T, grad_expanded, preferred_element_type=f32)
    g_query = jnp.dot(normed.T, grad_query_all, preferred_element_type=f32)
    latent_part = lax.dot_general(
        grad_expanded, full_up, (((1,), (1,)), ((), ())), preferred_element_type=f32
    )
    rope_part = rotate(jnp.sum(grad_keys[..., NOPE:], axis=1), cosine, -sine)
    latent_part = jnp.concatenate([latent_part, rope_part], axis=-1)
    input_part = lax.dot_general(
        grad_query_all, full_query, (((1,), (1,)), ((), ())), preferred_element_type=f32
    )
    latent_other, input_other = pair(
        grid, [rows_of(latent_part, 1 - core), rows_of(input_part, 1 - core)], False, 7
    )
    latent_sum = rows_of(latent_part, core) + latent_other
    grad_latent, g_lgain = rms_backward(
        rows_of(latent, core), rows_of(latent_inverse, core), gain_latent, latent_sum[:, :kv_rank]
    )
    grad_latent_all = jnp.concatenate([grad_latent, latent_sum[:, kv_rank:]], axis=-1).astype(bf16)
    g_latent = jnp.dot(rows_of(normed, core).T, grad_latent_all, preferred_element_type=f32)
    grad_normed = (rows_of(input_part, core) + input_other) + lax.dot_general(
        grad_latent_all, full_latent, (((1,), (1,)), ((), ())), preferred_element_type=f32
    )
    grad_in_part, g_norm = rms_backward(
        rows_of(tokens_f, core), rows_of(inverse_one, core), gain_one, grad_normed
    )
    grad_input_half = grad_residual + grad_in_part

    g_gains = jnp.concatenate(
        [
            g_norm.reshape(chips, gain_rows),
            g_fgain.reshape(chips, gain_rows),
            jnp.pad(g_lgain.reshape(chips, latent_rows), ((0, 0), (0, gain_rows - latent_rows))),
        ],
        axis=1,
    )
    g_gains = jnp.pad(g_gains[:, None, :], ((0, 0), (0, 15), (0, 0)))
    terms = [
        g_query.astype(bf16).reshape(grid + (-1, g_query.shape[1])),
        g_out_t.astype(bf16).reshape(grid + (-1, g_out_t.shape[1])),
        g_up.astype(bf16).reshape(grid + (-1, g_up.shape[1])),
        g_latent.astype(bf16).reshape(grid + (2, -1, g_latent.shape[1])),
        g_gains.astype(bf16).reshape(grid + (16, -1)),
    ]
    pieces = (
        cut(0, terms[0].shape[-2], REDUCE_COARSE)
        + cut(1, terms[1].shape[-2], REDUCE_COARSE)
        + cut(2, terms[2].shape[-2], ((1, (X, Y, Z)), (1, (Y, X, Z))))
        + cut(3, terms[3].shape[-2], ((1, (Z, X, Y)),), core_first=True)
        + cut(4, terms[4].shape[-2], ((1, (X, Y, Z)),))
    )
    s_query, s_out_t, s_up, latent_half, gain_sums = reduce(
        grid, terms, [False, False, False, True, False], pieces, 4
    )
    output, grad_input, s_latent, gain_sums = pair(
        grid, [output_half, grad_input_half, latent_half, gain_sums], True, 8
    )
    gain_sums = gain_sums[0, 0] + gain_sums[1, 0]
    return (
        output.reshape(length, width),
        grad_input.reshape(length, width),
        gain_sums[:gain_rows],
        s_query,
        s_latent.reshape(-1, s_latent.shape[-1]),
        gain_sums[2 * gain_rows : 2 * gain_rows + latent_rows],
        s_up,
        s_out_t.T,
        gain_sums[gain_rows : 2 * gain_rows],
        s_sgate,
        s_sup,
        s_sdown,
        grad_expert_gate[None],
        gradient_expert_upward[None],
        grad_expert_down[None],
    )


def chip_grid(mesh):
    coords = [tuple(getattr(device, "coords", ())) for device in mesh.devices[:, 0]]
    if any(len(spot) != 3 for spot in coords):
        return None
    low = [min(spot[axis] for spot in coords) for axis in range(3)]
    sizes = [max(spot[axis] for spot in coords) - low[axis] + 1 for axis in range(3)]
    steps = []
    for axis in range(3):
        steps.append(next((i for i, spot in enumerate(coords) if spot[axis] != low[axis]), 0))
    order = sorted(range(3), key=lambda axis: -steps[axis])
    grid = tuple(sizes[axis] for axis in order)
    for index, spot in enumerate(coords):
        for axis in reversed(order):
            if index % sizes[axis] != spot[axis] - low[axis]:
                return None
            index //= sizes[axis]
    return grid if min(grid) >= 2 else None


def solution(mesh):
    in_specs = (
        P("dp", None),
        P("dp"),
        P("dp", "tensor"),
        P("dp", None),
        P("dp"),
        P("dp", "tensor"),
        P("tensor", "dp"),
        P("dp"),
        P("dp", "tensor"),
        P("dp", "tensor"),
        P("tensor", "dp"),
        P("dp", None, "tensor"),
        P("dp", None, "tensor"),
        P("dp", "tensor", None),
        P("dp", None),
        P("dp", None),
        P("dp", None),
        P("dp", None),
    )
    out_specs = (
        P("dp", None),
        P("dp", None),
        P("dp"),
        P("dp", "tensor"),
        P("dp", None),
        P("dp"),
        P("dp", "tensor"),
        P("tensor", "dp"),
        P("dp"),
        P("dp", "tensor"),
        P("dp", "tensor"),
        P("tensor", "dp"),
        P("dp", None, "tensor"),
        P("dp", None, "tensor"),
        P("dp", "tensor", None),
    )
    grid = chip_grid(mesh)

    def step(*args):
        dense = grid is not None and 4 * args[15].shape[1] >= mesh.shape["dp"]
        body = functools.partial(dense_shards, grid) if dense else shards
        return jax.shard_map(
            body, mesh=mesh, in_specs=in_specs, out_specs=out_specs, check_vma=False
        )(*args)

    return step
```

```python
import functools

import jax
import jax.numpy as jnp
from jax import lax
from jax.experimental import pallas as pl
from jax.experimental.pallas import tpu as pltpu
from jax.sharding import PartitionSpec as P

NOPE = 128
ROPE = 64
VDIM = 128


EPSILON = 1e-06


def rope_tables(length):
    half_width = ROPE // 2
    frequency = 10000.0 ** (-(jnp.arange(half_width, dtype=jnp.float32) * 2.0 / ROPE))
    angles = jnp.arange(length, dtype=jnp.float32)[:, None] * frequency[None, :]
    return (jnp.cos(angles), jnp.sin(angles))


def rotate(vectors, cosine, sine):
    half_width = vectors.shape[-1] // 2
    first_half = vectors[..., :half_width]
    second = vectors[..., half_width:]
    return jnp.concatenate(
        [first_half * cosine - second * sine, second * cosine + first_half * sine], axis=-1
    )


def silu_slope(gate_projected):
    sigmoid_value = jax.nn.sigmoid(gate_projected)
    return sigmoid_value * (1.0 + gate_projected * (1.0 - sigmoid_value))


def rms_forward(vectors, gain):
    inverse = lax.rsqrt(jnp.mean(vectors * vectors, axis=-1, keepdims=True) + EPSILON)
    return (vectors * inverse * gain, inverse)


def rms_backward(vectors, inverse, gain, grad_out):
    scaled = gain * grad_out
    grad_in = inverse * scaled - vectors * inverse**3 * jnp.mean(
        scaled * vectors, axis=-1, keepdims=True
    )
    return (grad_in, jnp.sum(grad_out * vectors * inverse, axis=0))


def pick_owned(
    returned_rows, flat_ids, slot_index, half_rows, core_index, length, topk_count, width
):
    owned = slot_index // half_rows == core_index
    place = jnp.where(owned, flat_ids * half_rows + slot_index - core_index * half_rows, 0)
    picked = returned_rows[place].astype(jnp.float32) * owned[:, None].astype(jnp.float32)
    return picked.reshape(length, topk_count, width)


def shards(
    hidden_in,
    norm_gain,
    w_query,
    w_latent,
    latent_gain,
    w_up,
    w_out,
    ffn_gain,
    shared_gate,
    shared_up,
    shared_down,
    expert_gate,
    expert_up,
    expert_down,
    gate_values,
    expert_ids,
    segment_ids,
    cotangent,
):
    kept = (
        lax.all_gather(norm_gain, "dp", axis=0, tiled=True),
        lax.all_gather(w_query, "dp", axis=0, tiled=True),
        lax.all_gather(w_latent, "dp", axis=0, tiled=True),
        lax.all_gather(latent_gain, "dp", axis=0, tiled=True),
        lax.all_gather(w_up, "dp", axis=0, tiled=True),
        lax.all_gather(w_out, "dp", axis=1, tiled=True),
        lax.all_gather(ffn_gain, "dp", axis=0, tiled=True),
        lax.all_gather(shared_gate, "dp", axis=0, tiled=True),
        lax.all_gather(shared_up, "dp", axis=0, tiled=True),
        lax.all_gather(shared_down, "dp", axis=1, tiled=True),
    )
    (
        full_norm,
        full_query,
        full_latent,
        full_lgain,
        full_up,
        full_out,
        full_fgain,
        full_sgate,
        full_sup,
        full_sdown,
    ) = kept
    length = hidden_in.shape[0]
    width = hidden_in.shape[1]
    topk_count = expert_ids.shape[1]
    head_count = full_query.shape[1] // (NOPE + ROPE)
    kv_rank = full_up.shape[0]
    experts_total = lax.axis_size("dp")
    capacity = max(2, 2 * (length * topk_count * 7 // (12 * experts_total)))
    cosine, sine = rope_tables(length)
    scale = (NOPE + ROPE) ** (-0.5)
    segment_row = segment_ids[0]
    position = jnp.arange(length, dtype=jnp.int32)
    allowed = (segment_row[:, None] == segment_row[None, :]) & (
        position[None, :] <= position[:, None]
    )
    tokens_f = hidden_in.astype(jnp.float32)
    normed_f, inverse_one = rms_forward(tokens_f, full_norm.astype(jnp.float32))
    normed = normed_f.astype(jnp.bfloat16)
    query_all = jnp.dot(normed, full_query, preferred_element_type=jnp.float32).reshape(
        length, head_count, NOPE + ROPE
    )
    query_rope = rotate(query_all[..., NOPE:], cosine[:, None, :], sine[:, None, :])
    queries = jnp.concatenate([query_all[..., :NOPE], query_rope], axis=-1).astype(jnp.bfloat16)
    latent_all = jnp.dot(normed, full_latent, preferred_element_type=jnp.float32)
    latent = latent_all[:, :kv_rank]
    latent_normed, latent_inverse = rms_forward(latent, full_lgain.astype(jnp.float32))
    latent_bf = latent_normed.astype(jnp.bfloat16)
    key_rope = rotate(latent_all[:, kv_rank:], cosine, sine).astype(jnp.bfloat16)
    expanded = jnp.dot(latent_bf, full_up, preferred_element_type=jnp.float32).astype(jnp.bfloat16)
    expanded = expanded.reshape(length, head_count, NOPE + VDIM)
    key_all = jnp.concatenate(
        [expanded[..., :NOPE], jnp.broadcast_to(key_rope[:, None, :], (length, head_count, ROPE))],
        axis=-1,
    )
    values = expanded[..., NOPE:]
    scores = (
        jnp.einsum("qhd,khd->hqk", queries, key_all, preferred_element_type=jnp.float32) * scale
    )
    raw_probs = jnp.where(allowed[None], jnp.exp(scores), 0.0)
    totals = jnp.sum(raw_probs, axis=-1, keepdims=True)
    log_total = jnp.log(totals)
    attn_weights = (raw_probs / totals).astype(jnp.bfloat16)
    context = jnp.einsum("hqk,khd->qhd", attn_weights, values, preferred_element_type=jnp.float32)
    context = context.reshape(length, head_count * VDIM).astype(jnp.bfloat16)
    attended_part = jnp.dot(context, full_out, preferred_element_type=jnp.float32)
    attended = lax.psum(attended_part, "tensor")
    residual = tokens_f + attended
    ffn_gain_f = full_fgain.astype(jnp.float32)
    ffn_f, inverse_two = rms_forward(residual, ffn_gain_f)
    ffn_in = ffn_f.astype(jnp.bfloat16)
    pair_count = length * topk_count
    flat_ids = expert_ids.reshape(-1)
    onehot = (flat_ids[:, None] == jnp.arange(experts_total, dtype=jnp.int32)[None, :]).astype(
        jnp.int32
    )
    earlier = jnp.cumsum(onehot, axis=0) - onehot
    slot_index = jnp.sum(earlier * onehot, axis=1)
    target = flat_ids * capacity + slot_index
    pair_of_slot = (
        jnp.full((experts_total * capacity,), pair_count, jnp.int32)
        .at[target]
        .set(jnp.arange(pair_count, dtype=jnp.int32))
    )
    token_of_slot = pair_of_slot // topk_count
    ffn_padded = jnp.concatenate([ffn_in, jnp.zeros((1, width), jnp.bfloat16)], axis=0)
    outgoing = ffn_padded[token_of_slot].reshape(experts_total, capacity, width)
    cot_bf = cotangent.astype(jnp.bfloat16)
    grad_rows = (
        (gate_values[:, :, None] * cotangent[:, None, :])
        .astype(jnp.bfloat16)
        .reshape(pair_count, width)
    )
    grad_padded = jnp.concatenate([grad_rows, jnp.zeros((1, width), jnp.bfloat16)], axis=0)
    grad_outgoing = grad_padded[pair_of_slot].reshape(experts_total, capacity, width)
    half_rows = capacity // lax.axis_size("tensor")
    core_index = lax.axis_index("tensor")
    portion = lax.dynamic_slice_in_dim(outgoing, core_index * half_rows, half_rows, 1)
    grad_portion = lax.dynamic_slice_in_dim(grad_outgoing, core_index * half_rows, half_rows, 1)
    arrived_half, grad_half = (
        lax.all_to_all(portion, "dp", split_axis=0, concat_axis=0, tiled=True),
        lax.all_to_all(grad_portion, "dp", split_axis=0, concat_axis=0, tiled=True),
    )
    arrived, grad_arrived = (
        lax.all_gather(arrived_half, "tensor", axis=1, tiled=True),
        lax.all_gather(grad_half, "tensor", axis=1, tiled=True),
    )
    rows_per_expert = arrived.reshape(-1, width)
    grad_arrived = grad_arrived.reshape(-1, width)
    local_gate = expert_gate[0]
    resident_up_weight = expert_up[0]
    local_down = expert_down[0]
    gate_projected = jnp.dot(rows_per_expert, local_gate, preferred_element_type=jnp.float32)
    up_proj = jnp.dot(rows_per_expert, resident_up_weight, preferred_element_type=jnp.float32)
    expert_hidden = (jax.nn.silu(gate_projected) * up_proj).astype(jnp.bfloat16)
    expert_part = jnp.dot(expert_hidden, local_down, preferred_element_type=jnp.float32)
    shared_gproj = jnp.dot(ffn_in, full_sgate, preferred_element_type=jnp.float32)
    shared_uproj = jnp.dot(ffn_in, full_sup, preferred_element_type=jnp.float32)
    shared_hidden = (jax.nn.silu(shared_gproj) * shared_uproj).astype(jnp.bfloat16)
    shared_part = jnp.dot(shared_hidden, full_sdown, preferred_element_type=jnp.float32)
    expert_half = lax.psum_scatter(
        expert_part.reshape(experts_total, capacity, width),
        "tensor",
        scatter_dimension=1,
        tiled=True,
    )
    returned_half = lax.all_to_all(
        expert_half.astype(jnp.bfloat16), "dp", split_axis=0, concat_axis=0, tiled=True
    ).reshape(-1, width)
    picked = pick_owned(
        returned_half, flat_ids, slot_index, half_rows, core_index, length, topk_count, width
    )
    routed_part = jnp.sum(picked * gate_values[:, :, None], axis=1)
    ffn_total = lax.psum(shared_part + routed_part, "tensor")
    output = (residual + ffn_total).astype(jnp.bfloat16)
    expert_hidden_gradient = jnp.dot(grad_arrived, local_down.T, preferred_element_type=jnp.float32)
    expert_gate_gradient = (expert_hidden_gradient * up_proj * silu_slope(gate_projected)).astype(
        jnp.bfloat16
    )
    expert_up_gradient = (expert_hidden_gradient * jax.nn.silu(gate_projected)).astype(jnp.bfloat16)
    grad_expert_down = jnp.dot(expert_hidden.T, grad_arrived, preferred_element_type=jnp.float32)
    grad_expert_gate = jnp.dot(
        rows_per_expert.T, expert_gate_gradient, preferred_element_type=jnp.float32
    )
    gradient_expert_upward = jnp.dot(
        rows_per_expert.T, expert_up_gradient, preferred_element_type=jnp.float32
    )
    expert_back_part = jnp.dot(
        expert_gate_gradient, local_gate.T, preferred_element_type=jnp.float32
    ) + jnp.dot(expert_up_gradient, resident_up_weight.T, preferred_element_type=jnp.float32)
    grad_shidden = jnp.dot(cot_bf, full_sdown.T, preferred_element_type=jnp.float32)
    grad_sgate = (grad_shidden * shared_uproj * silu_slope(shared_gproj)).astype(jnp.bfloat16)
    grad_sup = (grad_shidden * jax.nn.silu(shared_gproj)).astype(jnp.bfloat16)
    g_sdown = jnp.dot(shared_hidden.T, cot_bf, preferred_element_type=jnp.float32)
    g_sgate = jnp.dot(ffn_in.T, grad_sgate, preferred_element_type=jnp.float32)
    g_sup = jnp.dot(ffn_in.T, grad_sup, preferred_element_type=jnp.float32)
    shared_back_part = jnp.dot(
        grad_sgate, full_sgate.T, preferred_element_type=jnp.float32
    ) + jnp.dot(grad_sup, full_sup.T, preferred_element_type=jnp.float32)
    back_half = lax.psum_scatter(
        expert_back_part.reshape(experts_total, capacity, width),
        "tensor",
        scatter_dimension=1,
        tiled=True,
    )
    back_returned_half = lax.all_to_all(
        back_half.astype(jnp.bfloat16), "dp", split_axis=0, concat_axis=0, tiled=True
    ).reshape(-1, width)
    back_picked = pick_owned(
        back_returned_half, flat_ids, slot_index, half_rows, core_index, length, topk_count, width
    )
    grad_ffn = lax.psum(shared_back_part + jnp.sum(back_picked, axis=1), "tensor")
    grad_res_part, g_fgain = rms_backward(residual, inverse_two, ffn_gain_f, grad_ffn)
    grad_residual = cotangent + grad_res_part
    grad_attn = grad_residual.astype(jnp.bfloat16)
    g_out = jnp.dot(context.T, grad_attn, preferred_element_type=jnp.float32)
    grad_context = (
        jnp.dot(grad_attn, full_out.T, preferred_element_type=jnp.float32)
        .astype(jnp.bfloat16)
        .reshape(length, head_count, VDIM)
    )
    probs = jnp.where(allowed[None], jnp.exp(scores - log_total), 0.0)
    weights_back = probs.astype(jnp.bfloat16)
    grad_values = jnp.einsum(
        "hqk,qhd->khd", weights_back, grad_context, preferred_element_type=jnp.float32
    )
    grad_weights = jnp.einsum(
        "qhd,khd->hqk", grad_context, values, preferred_element_type=jnp.float32
    )
    row_delta = jnp.sum(probs * grad_weights, axis=-1, keepdims=True)
    grad_scores = (probs * (grad_weights - row_delta) * scale).astype(jnp.bfloat16)
    grad_queries = jnp.einsum(
        "hqk,khd->qhd", grad_scores, key_all, preferred_element_type=jnp.float32
    )
    grad_keys = jnp.einsum("hqk,qhd->khd", grad_scores, queries, preferred_element_type=jnp.float32)
    grad_qrope = rotate(grad_queries[..., NOPE:], cosine[:, None, :], -sine[:, None, :])
    grad_query_all = (
        jnp.concatenate([grad_queries[..., :NOPE], grad_qrope], axis=-1)
        .reshape(length, head_count * (NOPE + ROPE))
        .astype(jnp.bfloat16)
    )
    grad_expanded = (
        jnp.concatenate([grad_keys[..., :NOPE], grad_values], axis=-1)
        .reshape(length, head_count * (NOPE + VDIM))
        .astype(jnp.bfloat16)
    )
    g_up = jnp.dot(latent_bf.T, grad_expanded, preferred_element_type=jnp.float32)
    g_query = jnp.dot(normed.T, grad_query_all, preferred_element_type=jnp.float32)
    latent_part = jnp.dot(grad_expanded, full_up.T, preferred_element_type=jnp.float32)
    rope_part = rotate(jnp.sum(grad_keys[..., NOPE:], axis=1), cosine, -sine)
    grad_latent_normed, grad_key_rope = lax.psum((latent_part, rope_part), "tensor")
    grad_latent, g_lgain = rms_backward(
        latent, latent_inverse, full_lgain.astype(jnp.float32), grad_latent_normed
    )
    grad_latent_all = jnp.concatenate([grad_latent, grad_key_rope], axis=-1).astype(jnp.bfloat16)
    g_latent = jnp.dot(normed.T, grad_latent_all, preferred_element_type=jnp.float32)
    input_part = jnp.dot(grad_query_all, full_query.T, preferred_element_type=jnp.float32)
    grad_normed = lax.psum(input_part, "tensor") + jnp.dot(
        grad_latent_all, full_latent.T, preferred_element_type=jnp.float32
    )
    grad_in_part, g_norm = rms_backward(
        tokens_f, inverse_one, full_norm.astype(jnp.float32), grad_normed
    )
    grad_input = grad_residual + grad_in_part
    summed = (
        lax.psum_scatter(g_norm, "dp", scatter_dimension=0, tiled=True),
        lax.psum_scatter(g_query, "dp", scatter_dimension=0, tiled=True),
        lax.psum_scatter(g_latent, "dp", scatter_dimension=0, tiled=True),
        lax.psum_scatter(g_lgain, "dp", scatter_dimension=0, tiled=True),
        lax.psum_scatter(g_up, "dp", scatter_dimension=0, tiled=True),
        lax.psum_scatter(g_out, "dp", scatter_dimension=1, tiled=True),
        lax.psum_scatter(g_fgain, "dp", scatter_dimension=0, tiled=True),
        lax.psum_scatter(g_sgate, "dp", scatter_dimension=0, tiled=True),
        lax.psum_scatter(g_sup, "dp", scatter_dimension=0, tiled=True),
        lax.psum_scatter(g_sdown, "dp", scatter_dimension=1, tiled=True),
    )
    s_norm, s_query, s_latent, s_lgain, s_up, s_out, s_fgain, s_sgate, s_sup, s_sdown = summed
    return (
        output,
        grad_input,
        s_norm,
        s_query,
        s_latent,
        s_lgain,
        s_up,
        s_out,
        s_fgain,
        s_sgate,
        s_sup,
        s_sdown,
        grad_expert_gate[None],
        gradient_expert_upward[None],
        grad_expert_down[None],
    )


MESH = pl.DeviceIdType.MESH


def place_of(grid):
    index = lax.axis_index("dp")
    place = []
    for size in reversed(grid):
        place.append(lax.rem(index, size))
        index = index // size
    return tuple(reversed(place)) + (lax.axis_index("tensor"),)


def device_at(grid, place):
    index = place[0]
    for size, spot in zip(grid[1:], place[1:-1]):
        index = index * size + spot
    return (index, place[-1])


def moved(place, dim, spot):
    return tuple(spot if axis == dim else at for axis, at in enumerate(place))


def greet(grid, place):
    sizes = grid + (2,)
    barrier = pltpu.get_barrier_semaphore()
    for dim, size in enumerate(sizes):
        for step in (-1, 1):
            if size == 2:
                if step == 1:
                    pl.semaphore_signal(barrier, inc=1, device_id=device_at(grid, moved(place, dim, 1 - place[dim])), device_id_type=MESH)
                continue
            spot = place[dim] + step

            @pl.when((spot >= 0) & (spot < size))
            def _():
                pl.semaphore_signal(barrier, inc=1, device_id=device_at(grid, moved(place, dim, spot)), device_id_type=MESH)

    peers = 0
    for dim, size in enumerate(sizes):
        if size == 2:
            peers += 1
        else:
            peers += jnp.minimum(place[dim], 1) + jnp.minimum(size - 1 - place[dim], 1)
    pl.semaphore_wait(barrier, peers)


def stage_plan(sizes, order, weight, first):
    plan, now, held = [], 0.0, 1
    for dim in order:
        for step in range(sizes[dim] - 1):
            cost = weight * held * (0.15 if dim == 3 else 1.0)
            plan.append((now, dim, step))
            now += cost
        held *= sizes[dim]
    plan.append((now, None, 0))
    return plan


def gather_body(grid, pieces, shared_flags, input_count, *refs):
    sizes = grid + (2,)
    inputs = refs[:input_count]
    outputs = refs[input_count : 2 * input_count]
    send_sem, recv_sem, own_sem = refs[2 * input_count :]
    place = place_of(grid)

    def window(number, piece, chosen):
        which, start, rows, order = piece
        spots = tuple(chosen.get(dim, place[dim]) for dim in range(4 if shared_flags[which] else 3))
        return outputs[which].at[spots + (pl.ds(start, rows),)]

    own = []
    for number, piece in enumerate(pieces):
        which, start, rows, order = piece
        copy = pltpu.make_async_copy(inputs[which].at[pl.ds(start, rows)], window(number, piece, {}), own_sem.at[number])
        copy.start()
        own.append(copy)
    greet(grid, place)

    stages = []
    for number, piece in enumerate(pieces):
        which, start, rows, order = piece
        weight = rows * inputs[which].shape[1]
        for rank, (when, dim, step) in enumerate(stage_plan(sizes, order, weight, 0.0)):
            stages.append((when, number, rank, dim, step))
    stages.sort(key=lambda s: s[:3])
    pending_recv = {number: [] for number in range(len(pieces))}
    sends = []
    slot_of = {}

    def copies(number, rank, dim, step):
        piece = pieces[number]
        which, start, rows, order = piece
        gathered = {}
        for earlier in order[: order.index(dim)]:
            gathered[earlier] = slice(None)
        size = sizes[dim]
        made = []
        base = 2 * rank
        if size == 2:
            part = window(number, piece, gathered)
            if not gathered:
                source = inputs[which].at[pl.ds(start, rows)]
            else:
                source = part
            copy = pltpu.make_async_remote_copy(
                source, part, send_sem.at[number, base], recv_sem.at[number, base],
                device_id=device_at(grid, moved(place, dim, 1 - place[dim])), device_id_type=MESH)
            made.append((None, None, copy))
            return made
        for way, sign in enumerate((1, -1)):
            spot = place[dim] + sign
            block = place[dim] - sign * step
            inside = (spot >= 0) & (spot < size) & (block >= 0) & (block < size)
            back = place[dim] - sign
            back_block = back - sign * step
            arrives = (back >= 0) & (back < size) & (back_block >= 0) & (back_block < size)
            chosen = dict(gathered)
            chosen[dim] = jnp.clip(block, 0, size - 1)
            part = window(number, piece, chosen)
            if not gathered and step == 0:
                source = inputs[which].at[pl.ds(start, rows)]
            else:
                source = part
            copy = pltpu.make_async_remote_copy(
                source, part, send_sem.at[number, base + way], recv_sem.at[number, base + way],
                device_id=device_at(grid, moved(place, dim, jnp.clip(spot, 0, size - 1))), device_id_type=MESH)
            made.append((inside, arrives, copy))
        return made

    for when, number, rank, dim, step in stages:
        for condition, copy in pending_recv[number]:
            if condition is None:
                copy.wait_recv()
            else:
                pl.when(condition)(copy.wait_recv)
        pending_recv[number] = []
        if rank == 1:
            own[number].wait()
        if dim is None:
            continue
        for send_ok, recv_ok, copy in copies(number, rank, dim, step):
            if send_ok is None:
                copy.start()
            else:
                pl.when(send_ok)(copy.start)
            sends.append((send_ok, copy))
            pending_recv[number].append((recv_ok, copy))
    for condition, copy in sends:
        if condition is None:
            copy.wait_send()
        else:
            pl.when(condition)(copy.wait_send)


def gather(grid, arrays, shared_flags, pieces, collective_id):
    out_shape = [
        jax.ShapeDtypeStruct(grid + ((2,) if shared else ()) + array.shape, array.dtype)
        for array, shared in zip(arrays, shared_flags)
    ]
    most = sum(size - 1 for size in grid) + 1
    return pl.pallas_call(
        functools.partial(gather_body, grid, pieces, shared_flags, len(arrays)),
        out_shape=out_shape,
        in_specs=[pl.BlockSpec(memory_space=pltpu.VMEM)] * len(arrays),
        out_specs=[pl.BlockSpec(memory_space=pl.ANY)] * len(arrays),
        scratch_shapes=[
            pltpu.SemaphoreType.DMA((len(pieces), 2 * most)),
            pltpu.SemaphoreType.DMA((len(pieces), 2 * most)),
            pltpu.SemaphoreType.DMA((len(pieces),)),
        ],
        compiler_params=pltpu.CompilerParams(collective_id=collective_id, has_side_effects=True, vmem_limit_bytes=16 << 20),
        name="gather_rows",
    )(*arrays)


def reduce_plan(sizes, order, weight):
    plan, now, held = [], 0.0, 1
    for dim in order:
        held *= sizes[dim]
    for dim in order:
        held //= sizes[dim]
        for step in range(sizes[dim] - 1):
            plan.append((now, dim, step))
            now += weight * held * (0.25 if dim == 3 else 1.0)
    plan.append((now, None, 0))
    return plan


def landing_shapes(sizes, order, rows, width):
    shapes = []
    for rank, dim in enumerate(order):
        left = tuple(sizes[d] for d in sorted(order[rank + 1 :]))
        ways = 1 if sizes[dim] == 2 else 2
        shapes.extend([left + (rows, width)] * (ways * (sizes[dim] - 1)))
    return shapes


def kept_index(place, later, dim, dims, kept, spots):
    left = sorted(later)
    return tuple(spots[left.index(d)] if d in later else (kept if d == dim else place[d]) for d in range(dims))


def add_into(target, target_index, source, lead, rows):
    chunk = 16
    total = 1
    for size in lead:
        total *= size

    def step(number, carry):
        block, row = number // (rows // chunk), lax.rem(number, rows // chunk)
        spots, rest = [], block
        for size in reversed(lead):
            spots.append(lax.rem(rest, size))
            rest = rest // size
        spots = tuple(reversed(spots))
        span = pl.ds(pl.multiple_of(row * chunk, chunk), chunk)
        here = target_index(spots) + (span,)
        value = target[here].astype(jnp.float32) + source[spots + (span,)].astype(jnp.float32)
        target[here] = value.astype(target.dtype)
        return carry

    lax.fori_loop(0, total * (rows // chunk), step, 0)


def reduce_body(grid, pieces, shared_flags, input_count, *refs):
    sizes = grid + (2,)
    inputs = refs[:input_count]
    outputs = refs[input_count : 2 * input_count]
    scratch = list(refs[2 * input_count :])
    held = [scratch.pop(0) for _ in pieces]
    landings = []
    for which, start, rows, order in pieces:
        count = len(landing_shapes(sizes, order, rows, inputs[which].shape[-1]))
        landings.append([scratch.pop(0) for _ in range(count)])
    send_sem, recv_sem, own_sem = scratch
    place = place_of(grid)

    loads = []
    for number, (which, start, rows, order) in enumerate(pieces):
        dims = 4 if shared_flags[which] else 3
        source = inputs[which].at[(slice(None),) * dims + (pl.ds(start, rows),)]
        copy = pltpu.make_async_copy(source, held[number], own_sem.at[number])
        copy.start()
        loads.append(copy)
    greet(grid, place)

    stages = []
    for number, (which, start, rows, order) in enumerate(pieces):
        weight = rows * inputs[which].shape[-1]
        slot = 0
        for rank, (when, dim, step) in enumerate(reduce_plan(sizes, order, weight)):
            stages.append((when, number, rank, dim, step))
    stages.sort(key=lambda s: s[:3])
    pending = {number: [] for number in range(len(pieces))}
    slots = {number: 0 for number in range(len(pieces))}
    sends = []

    for when, number, rank, dim, step in stages:
        which, start, rows, order = pieces[number]
        width = inputs[which].shape[-1]
        dims = 4 if shared_flags[which] else 3
        if rank == 0:
            loads[number].wait()
        for arrives, copy, add in pending[number]:
            if arrives is None:
                copy.wait_recv()
                add()
            else:

                @pl.when(arrives)
                def _():
                    copy.wait_recv()
                    add()

        pending[number] = []
        if dim is None:
            result = outputs[which]

            def finish(chunk_number, carry):
                span = pl.ds(pl.multiple_of(chunk_number * 16, 16), 16)
                value = held[number][tuple(place[:dims]) + (span,)].astype(jnp.float32)
                result[pl.ds(pl.multiple_of(start + chunk_number * 16, 16), 16)] = value
                return carry

            lax.fori_loop(0, rows // 16, finish, 0)
            continue
        later = order[order.index(dim) + 1 :]
        lead = tuple(sizes[d] for d in sorted(later))
        size = sizes[dim]

        def whole(block):
            return tuple(slice(None) if d in later else (block if d == dim else place[d]) for d in range(dims))

        for sign in (1,) if size == 2 else (1, -1):
            landing = landings[number][slots[number]]
            sem = slots[number]
            slots[number] += 1
            if size == 2:
                to, block, kept = 1 - place[dim], 1 - place[dim], place[dim]
                goes = arrives = None
            else:
                to = place[dim] + sign
                block = place[dim] + sign * (size - 1 - step)
                back = place[dim] - sign
                kept = place[dim] + sign * (size - 2 - step)
                goes = (to >= 0) & (to < size) & (block >= 0) & (block < size)
                arrives = (back >= 0) & (back < size) & (kept >= 0) & (kept < size)
                to, block, kept = (jnp.clip(v, 0, size - 1) for v in (to, block, kept))
            copy = pltpu.make_async_remote_copy(
                held[number].at[whole(block)], landing, send_sem.at[number, sem], recv_sem.at[number, sem],
                device_id=device_at(grid, moved(place, dim, to)), device_id_type=MESH)
            if goes is None:
                copy.start()
            else:
                pl.when(goes)(copy.start)
            sends.append((goes, copy))

            index = functools.partial(kept_index, place, later, dim, dims, kept)
            add = functools.partial(add_into, held[number], index, landing, lead, rows)
            pending[number].append((arrives, copy, add))
    for condition, copy in sends:
        if condition is None:
            copy.wait_send()
        else:
            pl.when(condition)(copy.wait_send)


def reduce(grid, arrays, shared_flags, pieces, collective_id):
    sizes = grid + (2,)
    out_shape = [
        jax.ShapeDtypeStruct(array.shape[-2:], jnp.float32)
        for array in arrays
    ]
    scratch, most = [], 1
    for which, start, rows, order in pieces:
        scratch.append(pltpu.VMEM(arrays[which].shape[:-2] + (rows, arrays[which].shape[-1]), arrays[which].dtype))
    for which, start, rows, order in pieces:
        shapes = landing_shapes(sizes, order, rows, arrays[which].shape[-1])
        most = max(most, len(shapes) + 1)
        scratch.extend(pltpu.VMEM(shape, arrays[which].dtype) for shape in shapes)
    return pl.pallas_call(
        functools.partial(reduce_body, grid, pieces, shared_flags, len(arrays)),
        out_shape=out_shape,
        in_specs=[pl.BlockSpec(memory_space=pl.ANY)] * len(arrays),
        out_specs=[pl.BlockSpec(memory_space=pltpu.VMEM)] * len(arrays),
        scratch_shapes=scratch + [
            pltpu.SemaphoreType.DMA((len(pieces), most)),
            pltpu.SemaphoreType.DMA((len(pieces), most)),
            pltpu.SemaphoreType.DMA((len(pieces),)),
        ],
        compiler_params=pltpu.CompilerParams(collective_id=collective_id, has_side_effects=True, vmem_limit_bytes=60 << 20),
        name="reduce_rows",
    )(*arrays)


def pair_body(grid, keep, count, *refs):
    inputs, outputs = refs[:count], refs[count : 2 * count]
    send_sem, recv_sem, own_sem = refs[2 * count :]
    place = place_of(grid)
    partner = device_at(grid, moved(place, 3, 1 - place[3]))
    barrier = pltpu.get_barrier_semaphore()
    pl.semaphore_signal(barrier, inc=1, device_id=partner, device_id_type=MESH)
    own = []
    for number in range(count if keep else 0):
        copy = pltpu.make_async_copy(inputs[number], outputs[number].at[place[3]], own_sem.at[number])
        copy.start()
        own.append(copy)
    pl.semaphore_wait(barrier, 1)
    sent = []
    for number in range(count):
        target = outputs[number].at[place[3]] if keep else outputs[number]
        copy = pltpu.make_async_remote_copy(
            inputs[number], target, send_sem.at[number], recv_sem.at[number],
            device_id=partner, device_id_type=MESH)
        copy.start()
        sent.append(copy)
    for copy in own + sent:
        copy.wait()


def pair(grid, arrays, keep, collective_id):
    count = len(arrays)
    return pl.pallas_call(
        functools.partial(pair_body, grid, keep, count),
        out_shape=[jax.ShapeDtypeStruct(((2,) if keep else ()) + array.shape, array.dtype) for array in arrays],
        in_specs=[pl.BlockSpec(memory_space=pltpu.VMEM if keep else pl.ANY)] * count,
        out_specs=[pl.BlockSpec(memory_space=pl.ANY)] * count,
        scratch_shapes=[pltpu.SemaphoreType.DMA((count,))] * 3,
        compiler_params=pltpu.CompilerParams(
            collective_id=collective_id, has_side_effects=True, vmem_limit_bytes=16 << 20),
        name="pair_rows",
    )(*arrays)


Z, Y, X, C = 0, 1, 2, 3


def cut(which, rows, orders, core_last=False, core_first=False):
    chunks = rows // 16
    total = sum(share for share, _ in orders)
    pieces, start, used = [], 0, 0
    for share, order in orders:
        used += share
        end = chunks * used // total * 16
        if end > start:
            full = ((C,) if core_first else ()) + order + ((C,) if core_last else ())
            pieces.append((which, start, end - start, full))
            start = end
    return pieces


GATHER_ORDERS = ((2, (Z, Y, X)), (2, (Z, X, Y)), (1, (Z, Y, X)), (1, (Z, X, Y)), (2, (Y, X, Z)))
REDUCE_ORDERS = ((1, (X, Y, Z)), (1, (Y, X, Z))) * 3 + ((1, (Z, X, Y)),) * 2


def spread_body(pick_ref, rows_ref, units_ref, weight_ref, out_ref):
    routed = lax.dot_general(
        pick_ref[0], rows_ref[0], (((0,), (0,)), ((), ())), preferred_element_type=jnp.float32
    )
    shared = lax.dot_general(
        units_ref[...], weight_ref[...], (((1,), (1,)), ((), ())), preferred_element_type=jnp.float32
    )
    out_ref[...] = (routed + shared).astype(out_ref.dtype)


def spread_rows(pick, rows, units, weight):
    count, capacity, length = pick.shape
    width = rows.shape[-1]
    lanes = units.shape[-1]
    return pl.pallas_call(
        spread_body,
        grid=(count,),
        out_shape=jax.ShapeDtypeStruct((count * length, width), rows.dtype),
        in_specs=[
            pl.BlockSpec((1, capacity, length), lambda s: (s, 0, 0)),
            pl.BlockSpec((1, capacity, width), lambda s: (s, 0, 0)),
            pl.BlockSpec((length, lanes), lambda s: (s, 0)),
            pl.BlockSpec((width, lanes), lambda s: (0, 0)),
        ],
        out_specs=pl.BlockSpec((length, width), lambda s: (s, 0)),
        compiler_params=pltpu.CompilerParams(vmem_limit_bytes=32 << 20),
        cost_estimate=pl.CostEstimate(
            flops=2 * count * length * width * (capacity + lanes),
            bytes_accessed=2 * count * (length + capacity) * width,
            transcendentals=0,
        ),
        name="spread_rows",
    )(pick, rows, units, weight)


def dense_shards(
    grid,
    hidden_in,
    norm_gain,
    w_query,
    w_latent,
    latent_gain,
    w_up,
    w_out,
    ffn_gain,
    shared_gate,
    shared_up,
    shared_down,
    expert_gate,
    expert_up,
    expert_down,
    gate_values,
    expert_ids,
    segment_ids,
    cotangent,
):
    f32, bf16 = jnp.float32, jnp.bfloat16
    length, width = hidden_in.shape
    half = length // 2
    topk_count = expert_ids.shape[1]
    chips = lax.axis_size("dp")
    head_count = w_query.shape[1] // (NOPE + ROPE)
    kv_rank = latent_gain.shape[0] * chips
    capacity = max(2, 2 * (length * topk_count * 7 // (12 * chips)))
    core = lax.axis_index("tensor")
    chip = lax.axis_index("dp")

    def rows_of(array, which):
        count = array.shape[0] // 2
        return lax.dynamic_slice_in_dim(array, which * count, count, 0)

    part_units = shared_gate.shape[1] // chips
    model_rows = shared_gate.shape[0]
    lanes = -(-part_units // 128) * 128

    def sliced(weight):
        slices = weight.reshape(model_rows, chips, part_units).transpose(1, 0, 2)
        return jnp.pad(slices, ((0, 0), (0, 0), (0, lanes - part_units)))

    stacked = jnp.concatenate([sliced(shared_gate), sliced(shared_up), sliced(shared_down.T)], axis=2)
    resharded = lax.all_to_all(stacked, "dp", split_axis=0, concat_axis=0, tiled=True)
    resharded = resharded.reshape(width, 3 * lanes)
    s_gate_up, s_down_t = resharded[:, : 2 * lanes], resharded[:, 2 * lanes :]
    gain_rows = norm_gain.shape[0]
    latent_rows = latent_gain.shape[0]
    gains = jnp.concatenate([norm_gain, ffn_gain, latent_gain])
    gains = jnp.pad(gains[None], ((0, 15), (0, gain_rows - latent_rows)))
    ids_t, gates_t = expert_ids.T, gate_values.T
    numbers = jnp.arange(chips, dtype=jnp.int32)[:, None]
    gate_map = jnp.zeros((chips, length), f32)
    for k in range(topk_count):
        gate_map += jnp.where(ids_t[k][None, :] == numbers, gates_t[k][None, :], 0.0)
    mine = [w_query, w_out.T, w_up, rows_of(w_latent, core), gains, gate_map]
    shared = [False, False, False, True, False, False]
    pieces = (
        cut(0, mine[0].shape[0], GATHER_ORDERS)
        + cut(1, mine[1].shape[0], GATHER_ORDERS)
        + cut(2, mine[2].shape[0], ((1, (Z, Y, X)), (1, (Z, X, Y))))
        + cut(3, mine[3].shape[0], ((1, (X, Y, Z)),), core_last=True)
        + cut(4, mine[4].shape[0], ((1, (Z, Y, X)),))
        + cut(5, mine[5].shape[0], ((1, (Z, X, Y)),))
    )
    got = gather(grid, mine, shared, pieces, 1)
    full_query = got[0].reshape(width, -1)
    full_out_t = got[1].reshape(width, -1)
    full_up = got[2].reshape(kv_rank, -1)
    full_latent = got[3].reshape(width, -1)
    all_gains = got[4].reshape(chips, 16, -1)[:, 0].astype(f32)
    gain_one = all_gains[:, :gain_rows].reshape(-1)
    gain_two = all_gains[:, gain_rows : 2 * gain_rows].reshape(-1)
    gain_latent = all_gains[:, 2 * gain_rows : 2 * gain_rows + latent_rows].reshape(-1)
    gates = lax.dynamic_index_in_dim(got[5].reshape(chips, -1, length), chip, 1, keepdims=False)

    def all_rows(part, after):
        part, after = lax.optimization_barrier((part, after))
        return lax.all_gather(part, ("dp", "tensor"), axis=0, tiled=True), after

    cot_half = rows_of(cotangent, core)
    cot_bf = cot_half.astype(bf16)
    cot_left, gain_two = all_rows(cot_bf[:, : width // 2], gain_two)

    cosine, sine = rope_tables(length)
    scale = (NOPE + ROPE) ** (-0.5)
    segment_row = segment_ids[0]
    position = jnp.arange(length, dtype=jnp.int32)
    allowed = (segment_row[:, None] == segment_row[None, :]) & (
        position[None, :] <= position[:, None]
    )
    tokens_f = hidden_in.astype(f32)
    normed_f, inverse_one = rms_forward(tokens_f, gain_one)
    normed = normed_f.astype(bf16)
    query_all = lax.optimization_barrier(jnp.dot(normed, full_query, preferred_element_type=f32))
    query_all = query_all.reshape(length, head_count, NOPE + ROPE)
    query_rope = rotate(query_all[..., NOPE:], cosine[:, None, :], sine[:, None, :])
    queries = jnp.concatenate([query_all[..., :NOPE], query_rope], axis=-1).astype(bf16)
    latent_all = jnp.dot(normed, full_latent, preferred_element_type=f32)
    latent = latent_all[:, :kv_rank]
    latent_normed, latent_inverse = rms_forward(latent, gain_latent)
    latent_bf = latent_normed.astype(bf16)
    key_rope = rotate(latent_all[:, kv_rank:], cosine, sine).astype(bf16)
    expanded = jnp.dot(latent_bf, full_up, preferred_element_type=f32).astype(bf16)
    expanded = expanded.reshape(length, head_count, NOPE + VDIM)
    key_all = jnp.concatenate(
        [expanded[..., :NOPE], jnp.broadcast_to(key_rope[:, None, :], (length, head_count, ROPE))],
        axis=-1,
    )
    values = expanded[..., NOPE:]
    scores = jnp.einsum("qhd,khd->hqk", queries, key_all, preferred_element_type=f32) * scale
    raw_probs = jnp.where(allowed[None], jnp.exp(scores), 0.0)
    totals = jnp.sum(raw_probs, axis=-1, keepdims=True)
    log_total = jnp.log(totals)
    attn_weights = (raw_probs / totals).astype(bf16)
    context = jnp.einsum("hqk,khd->qhd", attn_weights, values, preferred_element_type=f32)
    context = context.reshape(length, head_count * VDIM).astype(bf16)
    attended_part = lax.dot_general(
        context, full_out_t, (((1,), (1,)), ((), ())), preferred_element_type=f32
    )
    (other,) = pair(grid, [rows_of(attended_part, 1 - core)], False, 5)
    residual = rows_of(tokens_f, core) + (rows_of(attended_part, core) + other)
    ffn_f, inverse_two = rms_forward(residual, gain_two)
    ffn_in = ffn_f.astype(bf16)

    (ffn_all,) = gather(grid, [ffn_in], [True], cut(0, half, GATHER_ORDERS, core_last=True), 2)
    ffn_all = ffn_all.reshape(-1, width)
    cot_right, ffn_all = all_rows(cot_bf[:, width // 2 :], ffn_all)

    routed = gates > 0.0
    triangle = (position[:, None] < position[None, :]).astype(bf16)
    slot = jnp.dot(routed.astype(bf16), triangle, preferred_element_type=f32).astype(jnp.int32)
    chosen = routed[:, None, :] & (slot[:, None, :] == jnp.arange(capacity, dtype=jnp.int32)[None, :, None])
    pick = chosen.astype(bf16)
    gate_slot = jnp.sum(jnp.where(chosen, gates[:, None, :], 0.0), axis=-1)[..., None]

    def take(rows):
        return jnp.einsum(
            "sct,std->scd", pick, rows.reshape(chips, length, -1), preferred_element_type=f32
        )

    def spread(rows, units, weight):
        return spread_rows(pick, rows.reshape(chips, capacity, width), units, weight)

    expert_rows = take(ffn_all).astype(bf16).reshape(-1, width)
    gate_rows = gate_slot.reshape(-1, 1)
    local_gate, local_up, local_down = expert_gate[0], expert_up[0], expert_down[0]
    gate_projected = jnp.dot(expert_rows, local_gate, preferred_element_type=f32)
    up_projected = jnp.dot(expert_rows, local_up, preferred_element_type=f32)
    expert_hidden = (jax.nn.silu(gate_projected) * up_projected).astype(bf16)
    expert_part = jnp.dot(expert_hidden, local_down, preferred_element_type=f32)
    weighted = (gate_rows * expert_part).astype(bf16)
    shared_gu = jnp.dot(ffn_all, s_gate_up, preferred_element_type=f32)
    shared_g, shared_u = shared_gu[:, :lanes], shared_gu[:, lanes:]
    shared_hidden = (jax.nn.silu(shared_g) * shared_u).astype(bf16)
    forward_part = spread(weighted, shared_hidden, s_down_t)
    block_shape = grid + (2, half, width)
    reduce_pieces = cut(0, half, REDUCE_ORDERS, core_first=True)
    forward_part, cot_left, cot_right = lax.optimization_barrier((forward_part, cot_left, cot_right))
    grad_rows = jnp.concatenate(
        [(gate_slot * take(part)).astype(bf16) for part in (cot_left, cot_right)], axis=-1
    ).reshape(-1, width)
    ffn_total = lax.psum_scatter(forward_part, ("dp", "tensor"), scatter_dimension=0, tiled=True)

    hidden_gradient = lax.dot_general(
        grad_rows, local_down, (((1,), (1,)), ((), ())), preferred_element_type=f32
    )
    gate_gradient = (hidden_gradient * up_projected * silu_slope(gate_projected)).astype(bf16)
    up_gradient = (hidden_gradient * jax.nn.silu(gate_projected)).astype(bf16)
    back_part = lax.dot_general(
        gate_gradient, local_gate, (((1,), (1,)), ((), ())), preferred_element_type=f32
    ) + lax.dot_general(up_gradient, local_up, (((1,), (1,)), ((), ())), preferred_element_type=f32)
    shared_hg = jnp.dot(cot_left, s_down_t[: width // 2], preferred_element_type=f32) + jnp.dot(
        cot_right, s_down_t[width // 2 :], preferred_element_type=f32
    )
    grad_units = jnp.concatenate(
        [shared_hg * shared_u * silu_slope(shared_g), shared_hg * jax.nn.silu(shared_g)], axis=1
    ).astype(bf16)
    backward_part = spread(back_part.astype(bf16), grad_units, s_gate_up)
    (grad_ffn,) = reduce(grid, [backward_part.reshape(block_shape)], [True], reduce_pieces, 3)

    grad_expert_down = jnp.dot(expert_hidden.T, grad_rows, preferred_element_type=f32)
    grad_expert_gate = jnp.dot(expert_rows.T, gate_gradient, preferred_element_type=f32)
    gradient_expert_upward = jnp.dot(expert_rows.T, up_gradient, preferred_element_type=f32)
    over_rows = (((0,), (0,)), ((), ()))
    down_parts = [
        lax.dot_general(shared_hidden, part, over_rows, preferred_element_type=f32).astype(bf16)
        for part in (cot_left, cot_right)
    ]
    unit_grads = lax.dot_general(grad_units, ffn_all, over_rows, preferred_element_type=f32)
    unit_grads, *down_parts = lax.optimization_barrier((unit_grads.astype(bf16), *down_parts))
    shared_grads = jnp.concatenate([unit_grads, jnp.concatenate(down_parts, axis=1)])
    returned = lax.all_to_all(
        shared_grads.reshape(3 * lanes, chips, model_rows).transpose(1, 0, 2),
        "dp",
        split_axis=0,
        concat_axis=0,
        tiled=True,
    ).astype(f32)
    s_sgate, s_sup, s_sdown = (
        returned[:, i * lanes : i * lanes + part_units].reshape(-1, model_rows) for i in range(3)
    )
    s_sgate, s_sup = s_sgate.T, s_sup.T

    grad_res_part, g_fgain = rms_backward(residual, inverse_two, gain_two, grad_ffn)
    grad_residual = cot_half + grad_res_part
    (grad_attn,) = pair(grid, [grad_residual.astype(bf16)], True, 6)
    grad_attn = grad_attn.reshape(length, width)
    g_out_t = jnp.dot(grad_attn.T, context, preferred_element_type=f32)
    s_out_t = lax.psum_scatter(g_out_t.astype(bf16), "dp", scatter_dimension=0, tiled=True)
    grad_context = (
        jnp.dot(grad_attn, full_out_t, preferred_element_type=f32)
        .astype(bf16)
        .reshape(length, head_count, VDIM)
    )
    probs = jnp.where(allowed[None], jnp.exp(scores - log_total), 0.0)
    weights_back = probs.astype(bf16)
    grad_values = jnp.einsum("hqk,qhd->khd", weights_back, grad_context, preferred_element_type=f32)
    grad_weights = jnp.einsum("qhd,khd->hqk", grad_context, values, preferred_element_type=f32)
    row_delta = jnp.sum(probs * grad_weights, axis=-1, keepdims=True)
    grad_scores = (probs * (grad_weights - row_delta) * scale).astype(bf16)
    grad_queries = jnp.einsum("hqk,khd->qhd", grad_scores, key_all, preferred_element_type=f32)
    grad_keys = jnp.einsum("hqk,qhd->khd", grad_scores, queries, preferred_element_type=f32)
    grad_qrope = rotate(grad_queries[..., NOPE:], cosine[:, None, :], -sine[:, None, :])
    grad_query_all = (
        jnp.concatenate([grad_queries[..., :NOPE], grad_qrope], axis=-1)
        .reshape(length, head_count * (NOPE + ROPE))
        .astype(bf16)
    )
    grad_expanded = (
        jnp.concatenate([grad_keys[..., :NOPE], grad_values], axis=-1)
        .reshape(length, head_count * (NOPE + VDIM))
        .astype(bf16)
    )
    g_up = jnp.dot(latent_bf.T, grad_expanded, preferred_element_type=f32)
    g_query = jnp.dot(normed.T, grad_query_all, preferred_element_type=f32)
    latent_part = lax.dot_general(
        grad_expanded, full_up, (((1,), (1,)), ((), ())), preferred_element_type=f32
    )
    rope_part = rotate(jnp.sum(grad_keys[..., NOPE:], axis=1), cosine, -sine)
    latent_part = jnp.concatenate([latent_part, rope_part], axis=-1)
    input_part = lax.dot_general(
        grad_query_all, full_query, (((1,), (1,)), ((), ())), preferred_element_type=f32
    )
    latent_other, input_other = pair(
        grid, [rows_of(latent_part, 1 - core), rows_of(input_part, 1 - core)], False, 7
    )
    latent_sum = rows_of(latent_part, core) + latent_other
    grad_latent, g_lgain = rms_backward(
        rows_of(latent, core), rows_of(latent_inverse, core), gain_latent, latent_sum[:, :kv_rank]
    )
    grad_latent_all = jnp.concatenate([grad_latent, latent_sum[:, kv_rank:]], axis=-1).astype(bf16)
    g_latent = jnp.dot(rows_of(normed, core).T, grad_latent_all, preferred_element_type=f32)
    grad_normed = (rows_of(input_part, core) + input_other) + lax.dot_general(
        grad_latent_all, full_latent, (((1,), (1,)), ((), ())), preferred_element_type=f32
    )
    grad_in_part, g_norm = rms_backward(
        rows_of(tokens_f, core), rows_of(inverse_one, core), gain_one, grad_normed
    )
    grad_input_half = grad_residual + grad_in_part

    g_gains = jnp.concatenate(
        [
            g_norm.reshape(chips, gain_rows),
            g_fgain.reshape(chips, gain_rows),
            jnp.pad(g_lgain.reshape(chips, latent_rows), ((0, 0), (0, gain_rows - latent_rows))),
        ],
        axis=1,
    )
    g_gains = jnp.pad(g_gains[:, None, :], ((0, 0), (0, 15), (0, 0)))
    terms = [
        g_query.astype(bf16).reshape(grid + (-1, g_query.shape[1])),
        g_up.astype(bf16).reshape(grid + (-1, g_up.shape[1])),
        g_latent.astype(bf16).reshape(grid + (2, -1, g_latent.shape[1])),
        g_gains.astype(bf16).reshape(grid + (16, -1)),
    ]
    pieces = (
        cut(0, terms[0].shape[-2], REDUCE_ORDERS)
        + cut(1, terms[1].shape[-2], ((1, (X, Y, Z)), (1, (Y, X, Z))))
        + cut(2, terms[2].shape[-2], ((1, (Z, X, Y)),), core_first=True)
        + cut(3, terms[3].shape[-2], ((1, (X, Y, Z)),))
    )
    s_query, s_up, latent_half, gain_sums = reduce(
        grid, terms, [False, False, True, False], pieces, 4
    )
    ffn_total, s_out_t, gain_sums = lax.optimization_barrier((ffn_total, s_out_t, gain_sums))
    s_out_t = s_out_t.astype(f32)
    output_half = (residual + ffn_total.astype(f32)).astype(bf16)
    output, grad_input, s_latent, gain_sums = pair(
        grid, [output_half, grad_input_half, latent_half, gain_sums], True, 8
    )
    gain_sums = gain_sums[0, 0] + gain_sums[1, 0]
    return (
        output.reshape(length, width),
        grad_input.reshape(length, width),
        gain_sums[:gain_rows],
        s_query,
        s_latent.reshape(-1, s_latent.shape[-1]),
        gain_sums[2 * gain_rows : 2 * gain_rows + latent_rows],
        s_up,
        s_out_t.T,
        gain_sums[gain_rows : 2 * gain_rows],
        s_sgate,
        s_sup,
        s_sdown,
        grad_expert_gate[None],
        gradient_expert_upward[None],
        grad_expert_down[None],
    )


def chip_grid(mesh):
    coords = [tuple(getattr(device, "coords", ())) for device in mesh.devices[:, 0]]
    if any(len(spot) != 3 for spot in coords):
        return None
    low = [min(spot[axis] for spot in coords) for axis in range(3)]
    sizes = [max(spot[axis] for spot in coords) - low[axis] + 1 for axis in range(3)]
    steps = []
    for axis in range(3):
        steps.append(next((i for i, spot in enumerate(coords) if spot[axis] != low[axis]), 0))
    order = sorted(range(3), key=lambda axis: -steps[axis])
    grid = tuple(sizes[axis] for axis in order)
    for index, spot in enumerate(coords):
        for axis in reversed(order):
            if index % sizes[axis] != spot[axis] - low[axis]:
                return None
            index //= sizes[axis]
    return grid if min(grid) >= 2 else None


def solution(mesh):
    in_specs = (
        P("dp", None),
        P("dp"),
        P("dp", "tensor"),
        P("dp", None),
        P("dp"),
        P("dp", "tensor"),
        P("tensor", "dp"),
        P("dp"),
        P("dp", "tensor"),
        P("dp", "tensor"),
        P("tensor", "dp"),
        P("dp", None, "tensor"),
        P("dp", None, "tensor"),
        P("dp", "tensor", None),
        P("dp", None),
        P("dp", None),
        P("dp", None),
        P("dp", None),
    )
    out_specs = (
        P("dp", None),
        P("dp", None),
        P("dp"),
        P("dp", "tensor"),
        P("dp", None),
        P("dp"),
        P("dp", "tensor"),
        P("tensor", "dp"),
        P("dp"),
        P("dp", "tensor"),
        P("dp", "tensor"),
        P("tensor", "dp"),
        P("dp", None, "tensor"),
        P("dp", None, "tensor"),
        P("dp", "tensor", None),
    )
    grid = chip_grid(mesh)

    def step(*args):
        dense = grid is not None and 4 * args[15].shape[1] >= mesh.shape["dp"]
        body = functools.partial(dense_shards, grid) if dense else shards
        return jax.shard_map(
            body, mesh=mesh, in_specs=in_specs, out_specs=out_specs, check_vma=False
        )(*args)

    return step
```

```python
import functools

import jax
import jax.numpy as jnp
from jax import lax
from jax.experimental import pallas as pl
from jax.experimental.pallas import tpu as pltpu
from jax.sharding import PartitionSpec as P


NOPE = 128
ROPE = 64
VDIM = 128


EPSILON = 1e-06


def rope_tables(length):
    half_width = ROPE // 2
    frequency = 10000.0 ** (-(jnp.arange(half_width, dtype=jnp.float32) * 2.0 / ROPE))
    angles = jnp.arange(length, dtype=jnp.float32)[:, None] * frequency[None, :]
    return (jnp.cos(angles), jnp.sin(angles))


def rotate(vectors, cosine, sine):
    half_width = vectors.shape[-1] // 2
    first_half = vectors[..., :half_width]
    second = vectors[..., half_width:]
    return jnp.concatenate(
        [first_half * cosine - second * sine, second * cosine + first_half * sine], axis=-1
    )


def silu_slope(gate_projected):
    sigmoid_value = jax.nn.sigmoid(gate_projected)
    return sigmoid_value * (1.0 + gate_projected * (1.0 - sigmoid_value))


def rms_forward(vectors, gain):
    inverse = lax.rsqrt(jnp.mean(vectors * vectors, axis=-1, keepdims=True) + EPSILON)
    return (vectors * inverse * gain, inverse)


def rms_backward(vectors, inverse, gain, grad_out):
    scaled = gain * grad_out
    grad_in = inverse * scaled - vectors * inverse**3 * jnp.mean(
        scaled * vectors, axis=-1, keepdims=True
    )
    return (grad_in, jnp.sum(grad_out * vectors * inverse, axis=0))


def pick_owned(
    returned_rows, flat_ids, slot_index, half_rows, core_index, length, topk_count, width
):
    owned = slot_index // half_rows == core_index
    place = jnp.where(owned, flat_ids * half_rows + slot_index - core_index * half_rows, 0)
    picked = returned_rows[place].astype(jnp.float32) * owned[:, None].astype(jnp.float32)
    return picked.reshape(length, topk_count, width)


def shards(
    hidden_in,
    norm_gain,
    w_query,
    w_latent,
    latent_gain,
    w_up,
    w_out,
    ffn_gain,
    shared_gate,
    shared_up,
    shared_down,
    expert_gate,
    expert_up,
    expert_down,
    gate_values,
    expert_ids,
    segment_ids,
    cotangent,
):
    kept = (
        lax.all_gather(norm_gain, "dp", axis=0, tiled=True),
        lax.all_gather(w_query, "dp", axis=0, tiled=True),
        lax.all_gather(w_latent, "dp", axis=0, tiled=True),
        lax.all_gather(latent_gain, "dp", axis=0, tiled=True),
        lax.all_gather(w_up, "dp", axis=0, tiled=True),
        lax.all_gather(w_out, "dp", axis=1, tiled=True),
        lax.all_gather(ffn_gain, "dp", axis=0, tiled=True),
        lax.all_gather(shared_gate, "dp", axis=0, tiled=True),
        lax.all_gather(shared_up, "dp", axis=0, tiled=True),
        lax.all_gather(shared_down, "dp", axis=1, tiled=True),
    )
    (
        full_norm,
        full_query,
        full_latent,
        full_lgain,
        full_up,
        full_out,
        full_fgain,
        full_sgate,
        full_sup,
        full_sdown,
    ) = kept
    length = hidden_in.shape[0]
    width = hidden_in.shape[1]
    topk_count = expert_ids.shape[1]
    head_count = full_query.shape[1] // (NOPE + ROPE)
    kv_rank = full_up.shape[0]
    experts_total = lax.axis_size("dp")
    capacity = max(2, 2 * (length * topk_count * 7 // (12 * experts_total)))
    cosine, sine = rope_tables(length)
    scale = (NOPE + ROPE) ** (-0.5)
    segment_row = segment_ids[0]
    position = jnp.arange(length, dtype=jnp.int32)
    allowed = (segment_row[:, None] == segment_row[None, :]) & (
        position[None, :] <= position[:, None]
    )
    tokens_f = hidden_in.astype(jnp.float32)
    normed_f, inverse_one = rms_forward(tokens_f, full_norm.astype(jnp.float32))
    normed = normed_f.astype(jnp.bfloat16)
    query_all = jnp.dot(normed, full_query, preferred_element_type=jnp.float32).reshape(
        length, head_count, NOPE + ROPE
    )
    query_rope = rotate(query_all[..., NOPE:], cosine[:, None, :], sine[:, None, :])
    queries = jnp.concatenate([query_all[..., :NOPE], query_rope], axis=-1).astype(jnp.bfloat16)
    latent_all = jnp.dot(normed, full_latent, preferred_element_type=jnp.float32)
    latent = latent_all[:, :kv_rank]
    latent_normed, latent_inverse = rms_forward(latent, full_lgain.astype(jnp.float32))
    latent_bf = latent_normed.astype(jnp.bfloat16)
    key_rope = rotate(latent_all[:, kv_rank:], cosine, sine).astype(jnp.bfloat16)
    expanded = jnp.dot(latent_bf, full_up, preferred_element_type=jnp.float32).astype(jnp.bfloat16)
    expanded = expanded.reshape(length, head_count, NOPE + VDIM)
    key_all = jnp.concatenate(
        [expanded[..., :NOPE], jnp.broadcast_to(key_rope[:, None, :], (length, head_count, ROPE))],
        axis=-1,
    )
    values = expanded[..., NOPE:]
    scores = (
        jnp.einsum("qhd,khd->hqk", queries, key_all, preferred_element_type=jnp.float32) * scale
    )
    raw_probs = jnp.where(allowed[None], jnp.exp(scores), 0.0)
    totals = jnp.sum(raw_probs, axis=-1, keepdims=True)
    log_total = jnp.log(totals)
    attn_weights = (raw_probs / totals).astype(jnp.bfloat16)
    context = jnp.einsum("hqk,khd->qhd", attn_weights, values, preferred_element_type=jnp.float32)
    context = context.reshape(length, head_count * VDIM).astype(jnp.bfloat16)
    attended_part = jnp.dot(context, full_out, preferred_element_type=jnp.float32)
    attended = lax.psum(attended_part, "tensor")
    residual = tokens_f + attended
    ffn_gain_f = full_fgain.astype(jnp.float32)
    ffn_f, inverse_two = rms_forward(residual, ffn_gain_f)
    ffn_in = ffn_f.astype(jnp.bfloat16)
    pair_count = length * topk_count
    flat_ids = expert_ids.reshape(-1)
    onehot = (flat_ids[:, None] == jnp.arange(experts_total, dtype=jnp.int32)[None, :]).astype(
        jnp.int32
    )
    earlier = jnp.cumsum(onehot, axis=0) - onehot
    slot_index = jnp.sum(earlier * onehot, axis=1)
    target = flat_ids * capacity + slot_index
    pair_of_slot = (
        jnp.full((experts_total * capacity,), pair_count, jnp.int32)
        .at[target]
        .set(jnp.arange(pair_count, dtype=jnp.int32))
    )
    token_of_slot = pair_of_slot // topk_count
    ffn_padded = jnp.concatenate([ffn_in, jnp.zeros((1, width), jnp.bfloat16)], axis=0)
    outgoing = ffn_padded[token_of_slot].reshape(experts_total, capacity, width)
    cot_bf = cotangent.astype(jnp.bfloat16)
    grad_rows = (
        (gate_values[:, :, None] * cotangent[:, None, :])
        .astype(jnp.bfloat16)
        .reshape(pair_count, width)
    )
    grad_padded = jnp.concatenate([grad_rows, jnp.zeros((1, width), jnp.bfloat16)], axis=0)
    grad_outgoing = grad_padded[pair_of_slot].reshape(experts_total, capacity, width)
    half_rows = capacity // lax.axis_size("tensor")
    core_index = lax.axis_index("tensor")
    portion = lax.dynamic_slice_in_dim(outgoing, core_index * half_rows, half_rows, 1)
    grad_portion = lax.dynamic_slice_in_dim(grad_outgoing, core_index * half_rows, half_rows, 1)
    arrived_half, grad_half = (
        lax.all_to_all(portion, "dp", split_axis=0, concat_axis=0, tiled=True),
        lax.all_to_all(grad_portion, "dp", split_axis=0, concat_axis=0, tiled=True),
    )
    arrived, grad_arrived = (
        lax.all_gather(arrived_half, "tensor", axis=1, tiled=True),
        lax.all_gather(grad_half, "tensor", axis=1, tiled=True),
    )
    rows_per_expert = arrived.reshape(-1, width)
    grad_arrived = grad_arrived.reshape(-1, width)
    local_gate = expert_gate[0]
    resident_up_weight = expert_up[0]
    local_down = expert_down[0]
    gate_projected = jnp.dot(rows_per_expert, local_gate, preferred_element_type=jnp.float32)
    up_proj = jnp.dot(rows_per_expert, resident_up_weight, preferred_element_type=jnp.float32)
    expert_hidden = (jax.nn.silu(gate_projected) * up_proj).astype(jnp.bfloat16)
    expert_part = jnp.dot(expert_hidden, local_down, preferred_element_type=jnp.float32)
    shared_gproj = jnp.dot(ffn_in, full_sgate, preferred_element_type=jnp.float32)
    shared_uproj = jnp.dot(ffn_in, full_sup, preferred_element_type=jnp.float32)
    shared_hidden = (jax.nn.silu(shared_gproj) * shared_uproj).astype(jnp.bfloat16)
    shared_part = jnp.dot(shared_hidden, full_sdown, preferred_element_type=jnp.float32)
    expert_half = lax.psum_scatter(
        expert_part.reshape(experts_total, capacity, width),
        "tensor",
        scatter_dimension=1,
        tiled=True,
    )
    returned_half = lax.all_to_all(
        expert_half.astype(jnp.bfloat16), "dp", split_axis=0, concat_axis=0, tiled=True
    ).reshape(-1, width)
    picked = pick_owned(
        returned_half, flat_ids, slot_index, half_rows, core_index, length, topk_count, width
    )
    routed_part = jnp.sum(picked * gate_values[:, :, None], axis=1)
    ffn_total = lax.psum(shared_part + routed_part, "tensor")
    output = (residual + ffn_total).astype(jnp.bfloat16)
    expert_hidden_gradient = jnp.dot(grad_arrived, local_down.T, preferred_element_type=jnp.float32)
    expert_gate_gradient = (expert_hidden_gradient * up_proj * silu_slope(gate_projected)).astype(
        jnp.bfloat16
    )
    expert_up_gradient = (expert_hidden_gradient * jax.nn.silu(gate_projected)).astype(jnp.bfloat16)
    grad_expert_down = jnp.dot(expert_hidden.T, grad_arrived, preferred_element_type=jnp.float32)
    grad_expert_gate = jnp.dot(
        rows_per_expert.T, expert_gate_gradient, preferred_element_type=jnp.float32
    )
    gradient_expert_upward = jnp.dot(
        rows_per_expert.T, expert_up_gradient, preferred_element_type=jnp.float32
    )
    expert_back_part = jnp.dot(
        expert_gate_gradient, local_gate.T, preferred_element_type=jnp.float32
    ) + jnp.dot(expert_up_gradient, resident_up_weight.T, preferred_element_type=jnp.float32)
    grad_shidden = jnp.dot(cot_bf, full_sdown.T, preferred_element_type=jnp.float32)
    grad_sgate = (grad_shidden * shared_uproj * silu_slope(shared_gproj)).astype(jnp.bfloat16)
    grad_sup = (grad_shidden * jax.nn.silu(shared_gproj)).astype(jnp.bfloat16)
    g_sdown = jnp.dot(shared_hidden.T, cot_bf, preferred_element_type=jnp.float32)
    g_sgate = jnp.dot(ffn_in.T, grad_sgate, preferred_element_type=jnp.float32)
    g_sup = jnp.dot(ffn_in.T, grad_sup, preferred_element_type=jnp.float32)
    shared_back_part = jnp.dot(
        grad_sgate, full_sgate.T, preferred_element_type=jnp.float32
    ) + jnp.dot(grad_sup, full_sup.T, preferred_element_type=jnp.float32)
    back_half = lax.psum_scatter(
        expert_back_part.reshape(experts_total, capacity, width),
        "tensor",
        scatter_dimension=1,
        tiled=True,
    )
    back_returned_half = lax.all_to_all(
        back_half.astype(jnp.bfloat16), "dp", split_axis=0, concat_axis=0, tiled=True
    ).reshape(-1, width)
    back_picked = pick_owned(
        back_returned_half, flat_ids, slot_index, half_rows, core_index, length, topk_count, width
    )
    grad_ffn = lax.psum(shared_back_part + jnp.sum(back_picked, axis=1), "tensor")
    grad_res_part, g_fgain = rms_backward(residual, inverse_two, ffn_gain_f, grad_ffn)
    grad_residual = cotangent + grad_res_part
    grad_attn = grad_residual.astype(jnp.bfloat16)
    g_out = jnp.dot(context.T, grad_attn, preferred_element_type=jnp.float32)
    grad_context = (
        jnp.dot(grad_attn, full_out.T, preferred_element_type=jnp.float32)
        .astype(jnp.bfloat16)
        .reshape(length, head_count, VDIM)
    )
    probs = jnp.where(allowed[None], jnp.exp(scores - log_total), 0.0)
    weights_back = probs.astype(jnp.bfloat16)
    grad_values = jnp.einsum(
        "hqk,qhd->khd", weights_back, grad_context, preferred_element_type=jnp.float32
    )
    grad_weights = jnp.einsum(
        "qhd,khd->hqk", grad_context, values, preferred_element_type=jnp.float32
    )
    row_delta = jnp.sum(probs * grad_weights, axis=-1, keepdims=True)
    grad_scores = (probs * (grad_weights - row_delta) * scale).astype(jnp.bfloat16)
    grad_queries = jnp.einsum(
        "hqk,khd->qhd", grad_scores, key_all, preferred_element_type=jnp.float32
    )
    grad_keys = jnp.einsum("hqk,qhd->khd", grad_scores, queries, preferred_element_type=jnp.float32)
    grad_qrope = rotate(grad_queries[..., NOPE:], cosine[:, None, :], -sine[:, None, :])
    grad_query_all = (
        jnp.concatenate([grad_queries[..., :NOPE], grad_qrope], axis=-1)
        .reshape(length, head_count * (NOPE + ROPE))
        .astype(jnp.bfloat16)
    )
    grad_expanded = (
        jnp.concatenate([grad_keys[..., :NOPE], grad_values], axis=-1)
        .reshape(length, head_count * (NOPE + VDIM))
        .astype(jnp.bfloat16)
    )
    g_up = jnp.dot(latent_bf.T, grad_expanded, preferred_element_type=jnp.float32)
    g_query = jnp.dot(normed.T, grad_query_all, preferred_element_type=jnp.float32)
    latent_part = jnp.dot(grad_expanded, full_up.T, preferred_element_type=jnp.float32)
    rope_part = rotate(jnp.sum(grad_keys[..., NOPE:], axis=1), cosine, -sine)
    grad_latent_normed, grad_key_rope = lax.psum((latent_part, rope_part), "tensor")
    grad_latent, g_lgain = rms_backward(
        latent, latent_inverse, full_lgain.astype(jnp.float32), grad_latent_normed
    )
    grad_latent_all = jnp.concatenate([grad_latent, grad_key_rope], axis=-1).astype(jnp.bfloat16)
    g_latent = jnp.dot(normed.T, grad_latent_all, preferred_element_type=jnp.float32)
    input_part = jnp.dot(grad_query_all, full_query.T, preferred_element_type=jnp.float32)
    grad_normed = lax.psum(input_part, "tensor") + jnp.dot(
        grad_latent_all, full_latent.T, preferred_element_type=jnp.float32
    )
    grad_in_part, g_norm = rms_backward(
        tokens_f, inverse_one, full_norm.astype(jnp.float32), grad_normed
    )
    grad_input = grad_residual + grad_in_part
    summed = (
        lax.psum_scatter(g_norm, "dp", scatter_dimension=0, tiled=True),
        lax.psum_scatter(g_query, "dp", scatter_dimension=0, tiled=True),
        lax.psum_scatter(g_latent, "dp", scatter_dimension=0, tiled=True),
        lax.psum_scatter(g_lgain, "dp", scatter_dimension=0, tiled=True),
        lax.psum_scatter(g_up, "dp", scatter_dimension=0, tiled=True),
        lax.psum_scatter(g_out, "dp", scatter_dimension=1, tiled=True),
        lax.psum_scatter(g_fgain, "dp", scatter_dimension=0, tiled=True),
        lax.psum_scatter(g_sgate, "dp", scatter_dimension=0, tiled=True),
        lax.psum_scatter(g_sup, "dp", scatter_dimension=0, tiled=True),
        lax.psum_scatter(g_sdown, "dp", scatter_dimension=1, tiled=True),
    )
    s_norm, s_query, s_latent, s_lgain, s_up, s_out, s_fgain, s_sgate, s_sup, s_sdown = summed
    return (
        output,
        grad_input,
        s_norm,
        s_query,
        s_latent,
        s_lgain,
        s_up,
        s_out,
        s_fgain,
        s_sgate,
        s_sup,
        s_sdown,
        grad_expert_gate[None],
        gradient_expert_upward[None],
        grad_expert_down[None],
    )


MESH = pl.DeviceIdType.MESH


def place_of(grid):
    index = lax.axis_index("dp")
    place = []
    for size in reversed(grid):
        place.append(lax.rem(index, size))
        index = index // size
    return tuple(reversed(place)) + (lax.axis_index("tensor"),)


def device_at(grid, place):
    index = place[0]
    for size, spot in zip(grid[1:], place[1:-1]):
        index = index * size + spot
    return (index, place[-1])


def moved(place, dim, spot):
    return tuple(spot if axis == dim else at for axis, at in enumerate(place))


def greet(grid, place):
    sizes = grid + (2,)
    barrier = pltpu.get_barrier_semaphore()
    for dim, size in enumerate(sizes):
        for step in (-1, 1):
            if size == 2:
                if step == 1:
                    pl.semaphore_signal(barrier, inc=1, device_id=device_at(grid, moved(place, dim, 1 - place[dim])), device_id_type=MESH)
                continue
            spot = place[dim] + step

            @pl.when((spot >= 0) & (spot < size))
            def _():
                pl.semaphore_signal(barrier, inc=1, device_id=device_at(grid, moved(place, dim, spot)), device_id_type=MESH)

    peers = 0
    for dim, size in enumerate(sizes):
        if size == 2:
            peers += 1
        else:
            peers += jnp.minimum(place[dim], 1) + jnp.minimum(size - 1 - place[dim], 1)
    pl.semaphore_wait(barrier, peers)


def stage_plan(sizes, order, weight):
    plan, now, held = [], 0.0, 1
    for dim in order:
        for step in range(sizes[dim] - 1):
            cost = weight * held * (0.15 if dim == 3 else 1.0)
            plan.append((now, dim, step))
            now += cost
        held *= sizes[dim]
    plan.append((now, None, 0))
    return plan


def gather_body(grid, pieces, shared_flags, input_count, *refs):
    sizes = grid + (2,)
    inputs = refs[:input_count]
    outputs = refs[input_count : 2 * input_count]
    send_sem, recv_sem, own_sem = refs[2 * input_count :]
    place = place_of(grid)

    def window(piece, chosen):
        which, start, rows, _ = piece
        spots = tuple(chosen.get(dim, place[dim]) for dim in range(4 if shared_flags[which] else 3))
        return outputs[which].at[spots + (pl.ds(start, rows),)]

    own = []
    for number, piece in enumerate(pieces):
        which, start, rows, order = piece
        copy = pltpu.make_async_copy(inputs[which].at[pl.ds(start, rows)], window(piece, {}), own_sem.at[number])
        copy.start()
        own.append(copy)
    greet(grid, place)

    stages = []
    for number, piece in enumerate(pieces):
        which, start, rows, order = piece
        weight = rows * inputs[which].shape[1]
        for rank, (when, dim, step) in enumerate(stage_plan(sizes, order, weight)):
            stages.append((when, number, rank, dim, step))
    stages.sort(key=lambda s: s[:3])
    pending_recv = {number: [] for number in range(len(pieces))}
    sends = []

    def copies(number, rank, dim, step):
        piece = pieces[number]
        which, start, rows, order = piece
        gathered = {}
        for earlier in order[: order.index(dim)]:
            gathered[earlier] = slice(None)
        size = sizes[dim]
        made = []
        base = 2 * rank
        if size == 2:
            part = window(piece, gathered)
            if not gathered:
                source = inputs[which].at[pl.ds(start, rows)]
            else:
                source = part
            copy = pltpu.make_async_remote_copy(
                source, part, send_sem.at[number, base], recv_sem.at[number, base],
                device_id=device_at(grid, moved(place, dim, 1 - place[dim])), device_id_type=MESH)
            made.append((None, None, copy))
            return made
        for way, sign in enumerate((1, -1)):
            spot = place[dim] + sign
            block = place[dim] - sign * step
            inside = (spot >= 0) & (spot < size) & (block >= 0) & (block < size)
            back = place[dim] - sign
            back_block = back - sign * step
            arrives = (back >= 0) & (back < size) & (back_block >= 0) & (back_block < size)
            chosen = dict(gathered)
            chosen[dim] = jnp.clip(block, 0, size - 1)
            part = window(piece, chosen)
            if not gathered and step == 0:
                source = inputs[which].at[pl.ds(start, rows)]
            else:
                source = part
            copy = pltpu.make_async_remote_copy(
                source, part, send_sem.at[number, base + way], recv_sem.at[number, base + way],
                device_id=device_at(grid, moved(place, dim, jnp.clip(spot, 0, size - 1))), device_id_type=MESH)
            made.append((inside, arrives, copy))
        return made

    for when, number, rank, dim, step in stages:
        for condition, copy in pending_recv[number]:
            if condition is None:
                copy.wait_recv()
            else:
                pl.when(condition)(copy.wait_recv)
        pending_recv[number] = []
        if rank == 1:
            own[number].wait()
        if dim is None:
            continue
        for send_ok, recv_ok, copy in copies(number, rank, dim, step):
            if send_ok is None:
                copy.start()
            else:
                pl.when(send_ok)(copy.start)
            sends.append((send_ok, copy))
            pending_recv[number].append((recv_ok, copy))
    for condition, copy in sends:
        if condition is None:
            copy.wait_send()
        else:
            pl.when(condition)(copy.wait_send)


def gather(grid, arrays, shared_flags, pieces, collective_id):
    out_shape = [
        jax.ShapeDtypeStruct(grid + ((2,) if shared else ()) + array.shape, array.dtype)
        for array, shared in zip(arrays, shared_flags)
    ]
    most = sum(size - 1 for size in grid) + 1
    return pl.pallas_call(
        functools.partial(gather_body, grid, pieces, shared_flags, len(arrays)),
        out_shape=out_shape,
        in_specs=[pl.BlockSpec(memory_space=pltpu.VMEM)] * len(arrays),
        out_specs=[pl.BlockSpec(memory_space=pl.ANY)] * len(arrays),
        scratch_shapes=[
            pltpu.SemaphoreType.DMA((len(pieces), 2 * most)),
            pltpu.SemaphoreType.DMA((len(pieces), 2 * most)),
            pltpu.SemaphoreType.DMA((len(pieces),)),
        ],
        compiler_params=pltpu.CompilerParams(collective_id=collective_id, has_side_effects=True, vmem_limit_bytes=16 << 20),
        name="gather_rows",
    )(*arrays)


def reduce_plan(sizes, order, weight):
    plan, now, held = [], 0.0, 1
    for dim in order:
        held *= sizes[dim]
    for dim in order:
        held //= sizes[dim]
        for step in range(sizes[dim] - 1):
            plan.append((now, dim, step))
            now += weight * held * (0.25 if dim == 3 else 1.0)
    plan.append((now, None, 0))
    return plan


def landing_shapes(sizes, order, rows, width):
    shapes = []
    for rank, dim in enumerate(order):
        left = tuple(sizes[d] for d in sorted(order[rank + 1 :]))
        ways = 1 if sizes[dim] == 2 else 2
        shapes.extend([left + (rows, width)] * (ways * (sizes[dim] - 1)))
    return shapes


def kept_index(place, later, dim, dims, kept, spots):
    left = sorted(later)
    return tuple(spots[left.index(d)] if d in later else (kept if d == dim else place[d]) for d in range(dims))


def add_into(target, target_index, source, lead, rows):
    chunk = 16
    total = 1
    for size in lead:
        total *= size

    def step(number, carry):
        block, row = number // (rows // chunk), lax.rem(number, rows // chunk)
        spots, rest = [], block
        for size in reversed(lead):
            spots.append(lax.rem(rest, size))
            rest = rest // size
        spots = tuple(reversed(spots))
        span = pl.ds(pl.multiple_of(row * chunk, chunk), chunk)
        here = target_index(spots) + (span,)
        value = target[here].astype(jnp.float32) + source[spots + (span,)].astype(jnp.float32)
        target[here] = value.astype(target.dtype)
        return carry

    lax.fori_loop(0, total * (rows // chunk), step, 0)


def reduce_body(grid, pieces, shared_flags, input_count, *refs):
    sizes = grid + (2,)
    inputs = refs[:input_count]
    outputs = refs[input_count : 2 * input_count]
    scratch = list(refs[2 * input_count :])
    held = [scratch.pop(0) for _ in pieces]
    landings = []
    for which, start, rows, order in pieces:
        count = len(landing_shapes(sizes, order, rows, inputs[which].shape[-1]))
        landings.append([scratch.pop(0) for _ in range(count)])
    send_sem, recv_sem, own_sem = scratch
    place = place_of(grid)

    loads = []
    for number, (which, start, rows, order) in enumerate(pieces):
        dims = 4 if shared_flags[which] else 3
        source = inputs[which].at[(slice(None),) * dims + (pl.ds(start, rows),)]
        copy = pltpu.make_async_copy(source, held[number], own_sem.at[number])
        copy.start()
        loads.append(copy)
    greet(grid, place)

    stages = []
    for number, (which, start, rows, order) in enumerate(pieces):
        weight = rows * inputs[which].shape[-1]
        for rank, (when, dim, step) in enumerate(reduce_plan(sizes, order, weight)):
            stages.append((when, number, rank, dim, step))
    stages.sort(key=lambda s: s[:3])
    pending = {number: [] for number in range(len(pieces))}
    slots = {number: 0 for number in range(len(pieces))}
    sends = []

    for when, number, rank, dim, step in stages:
        which, start, rows, order = pieces[number]
        dims = 4 if shared_flags[which] else 3
        if rank == 0:
            loads[number].wait()
        for arrives, copy, add in pending[number]:
            if arrives is None:
                copy.wait_recv()
                add()
            else:

                @pl.when(arrives)
                def _():
                    copy.wait_recv()
                    add()

        pending[number] = []
        if dim is None:
            result = outputs[which]

            def finish(chunk_number, carry):
                span = pl.ds(pl.multiple_of(chunk_number * 16, 16), 16)
                value = held[number][tuple(place[:dims]) + (span,)].astype(jnp.float32)
                result[pl.ds(pl.multiple_of(start + chunk_number * 16, 16), 16)] = value
                return carry

            lax.fori_loop(0, rows // 16, finish, 0)
            continue
        later = order[order.index(dim) + 1 :]
        lead = tuple(sizes[d] for d in sorted(later))
        size = sizes[dim]

        def whole(block):
            return tuple(slice(None) if d in later else (block if d == dim else place[d]) for d in range(dims))

        for sign in (1,) if size == 2 else (1, -1):
            landing = landings[number][slots[number]]
            sem = slots[number]
            slots[number] += 1
            if size == 2:
                to, block, kept = 1 - place[dim], 1 - place[dim], place[dim]
                goes = arrives = None
            else:
                to = place[dim] + sign
                block = place[dim] + sign * (size - 1 - step)
                back = place[dim] - sign
                kept = place[dim] + sign * (size - 2 - step)
                goes = (to >= 0) & (to < size) & (block >= 0) & (block < size)
                arrives = (back >= 0) & (back < size) & (kept >= 0) & (kept < size)
                to, block, kept = (jnp.clip(v, 0, size - 1) for v in (to, block, kept))
            copy = pltpu.make_async_remote_copy(
                held[number].at[whole(block)], landing, send_sem.at[number, sem], recv_sem.at[number, sem],
                device_id=device_at(grid, moved(place, dim, to)), device_id_type=MESH)
            if goes is None:
                copy.start()
            else:
                pl.when(goes)(copy.start)
            sends.append((goes, copy))

            index = functools.partial(kept_index, place, later, dim, dims, kept)
            add = functools.partial(add_into, held[number], index, landing, lead, rows)
            pending[number].append((arrives, copy, add))
    for condition, copy in sends:
        if condition is None:
            copy.wait_send()
        else:
            pl.when(condition)(copy.wait_send)


def reduce(grid, arrays, shared_flags, pieces, collective_id):
    sizes = grid + (2,)
    out_shape = [
        jax.ShapeDtypeStruct(array.shape[-2:], jnp.float32)
        for array in arrays
    ]
    scratch, most = [], 1
    for which, start, rows, order in pieces:
        scratch.append(pltpu.VMEM(arrays[which].shape[:-2] + (rows, arrays[which].shape[-1]), arrays[which].dtype))
    for which, start, rows, order in pieces:
        shapes = landing_shapes(sizes, order, rows, arrays[which].shape[-1])
        most = max(most, len(shapes) + 1)
        scratch.extend(pltpu.VMEM(shape, arrays[which].dtype) for shape in shapes)
    return pl.pallas_call(
        functools.partial(reduce_body, grid, pieces, shared_flags, len(arrays)),
        out_shape=out_shape,
        in_specs=[pl.BlockSpec(memory_space=pl.ANY)] * len(arrays),
        out_specs=[pl.BlockSpec(memory_space=pltpu.VMEM)] * len(arrays),
        scratch_shapes=scratch + [
            pltpu.SemaphoreType.DMA((len(pieces), most)),
            pltpu.SemaphoreType.DMA((len(pieces), most)),
            pltpu.SemaphoreType.DMA((len(pieces),)),
        ],
        compiler_params=pltpu.CompilerParams(collective_id=collective_id, has_side_effects=True, vmem_limit_bytes=60 << 20),
        name="reduce_rows",
    )(*arrays)


def pair_body(grid, keep, count, *refs):
    inputs, outputs = refs[:count], refs[count : 2 * count]
    send_sem, recv_sem, own_sem = refs[2 * count :]
    place = place_of(grid)
    partner = device_at(grid, moved(place, 3, 1 - place[3]))
    barrier = pltpu.get_barrier_semaphore()
    pl.semaphore_signal(barrier, inc=1, device_id=partner, device_id_type=MESH)
    own = []
    for number in range(count if keep else 0):
        copy = pltpu.make_async_copy(inputs[number], outputs[number].at[place[3]], own_sem.at[number])
        copy.start()
        own.append(copy)
    pl.semaphore_wait(barrier, 1)
    sent = []
    for number in range(count):
        target = outputs[number].at[place[3]] if keep else outputs[number]
        copy = pltpu.make_async_remote_copy(
            inputs[number], target, send_sem.at[number], recv_sem.at[number],
            device_id=partner, device_id_type=MESH)
        copy.start()
        sent.append(copy)
    for copy in own + sent:
        copy.wait()


def pair(grid, arrays, keep, collective_id):
    count = len(arrays)
    return pl.pallas_call(
        functools.partial(pair_body, grid, keep, count),
        out_shape=[jax.ShapeDtypeStruct(((2,) if keep else ()) + array.shape, array.dtype) for array in arrays],
        in_specs=[pl.BlockSpec(memory_space=pltpu.VMEM if keep else pl.ANY)] * count,
        out_specs=[pl.BlockSpec(memory_space=pl.ANY)] * count,
        scratch_shapes=[pltpu.SemaphoreType.DMA((count,))] * 3,
        compiler_params=pltpu.CompilerParams(
            collective_id=collective_id, has_side_effects=True, vmem_limit_bytes=16 << 20),
        name="pair_rows",
    )(*arrays)


Z, Y, X, C = 0, 1, 2, 3


def cut(which, rows, orders, core_last=False, core_first=False):
    chunks = rows // 16
    total = sum(share for share, _ in orders)
    pieces, start, used = [], 0, 0
    for share, order in orders:
        used += share
        end = chunks * used // total * 16
        if end > start:
            full = ((C,) if core_first else ()) + order + ((C,) if core_last else ())
            pieces.append((which, start, end - start, full))
            start = end
    return pieces


GATHER_ORDERS = ((2, (Z, Y, X)), (2, (Z, X, Y)), (1, (Z, Y, X)), (1, (Z, X, Y)), (2, (Y, X, Z)))
REDUCE_ORDERS = ((1, (X, Y, Z)), (1, (Y, X, Z))) * 3 + ((1, (Z, X, Y)),) * 2


def spread_body(pick_ref, rows_ref, units_ref, weight_ref, out_ref):
    routed = lax.dot_general(
        pick_ref[0], rows_ref[0], (((0,), (0,)), ((), ())), preferred_element_type=jnp.float32
    )
    shared = lax.dot_general(
        units_ref[...], weight_ref[...], (((1,), (1,)), ((), ())), preferred_element_type=jnp.float32
    )
    out_ref[...] = (routed + shared).astype(out_ref.dtype)


def spread_rows(pick, rows, units, weight):
    count, capacity, length = pick.shape
    width = rows.shape[-1]
    lanes = units.shape[-1]
    return pl.pallas_call(
        spread_body,
        grid=(count,),
        out_shape=jax.ShapeDtypeStruct((count * length, width), rows.dtype),
        in_specs=[
            pl.BlockSpec((1, capacity, length), lambda s: (s, 0, 0)),
            pl.BlockSpec((1, capacity, width), lambda s: (s, 0, 0)),
            pl.BlockSpec((length, lanes), lambda s: (s, 0)),
            pl.BlockSpec((width, lanes), lambda s: (0, 0)),
        ],
        out_specs=pl.BlockSpec((length, width), lambda s: (s, 0)),
        compiler_params=pltpu.CompilerParams(vmem_limit_bytes=32 << 20),
        cost_estimate=pl.CostEstimate(
            flops=2 * count * length * width * (capacity + lanes),
            bytes_accessed=2 * count * (length + capacity) * width,
            transcendentals=0,
        ),
        name="spread_rows",
    )(pick, rows, units, weight)


def dense_shards(
    grid,
    hidden_in,
    norm_gain,
    w_query,
    w_latent,
    latent_gain,
    w_up,
    w_out,
    ffn_gain,
    shared_gate,
    shared_up,
    shared_down,
    expert_gate,
    expert_up,
    expert_down,
    gate_values,
    expert_ids,
    segment_ids,
    cotangent,
):
    f32, bf16 = jnp.float32, jnp.bfloat16
    length, width = hidden_in.shape
    half = length // 2
    topk_count = expert_ids.shape[1]
    chips = lax.axis_size("dp")
    head_count = w_query.shape[1] // (NOPE + ROPE)
    kv_rank = latent_gain.shape[0] * chips
    capacity = max(2, 2 * (length * topk_count * 7 // (12 * chips)))
    core = lax.axis_index("tensor")
    chip = lax.axis_index("dp")

    def rows_of(array, which):
        count = array.shape[0] // 2
        return lax.dynamic_slice_in_dim(array, which * count, count, 0)

    part_units = shared_gate.shape[1] // chips
    model_rows = shared_gate.shape[0]
    lanes = -(-part_units // 128) * 128

    def sliced(weight):
        slices = weight.reshape(model_rows, chips, part_units).transpose(1, 0, 2)
        return jnp.pad(slices, ((0, 0), (0, 0), (0, lanes - part_units)))

    stacked = jnp.concatenate([sliced(shared_gate), sliced(shared_up), sliced(shared_down.T)], axis=2)
    resharded = lax.all_to_all(stacked, "dp", split_axis=0, concat_axis=0, tiled=True)
    resharded = resharded.reshape(width, 3 * lanes)
    s_gate_up, s_down_t = resharded[:, : 2 * lanes], resharded[:, 2 * lanes :]
    gain_rows = norm_gain.shape[0]
    latent_rows = latent_gain.shape[0]
    gains = jnp.concatenate([norm_gain, ffn_gain, latent_gain])
    gains = jnp.pad(gains[None], ((0, 15), (0, gain_rows - latent_rows)))
    ids_t, gates_t = expert_ids.T, gate_values.T
    numbers = jnp.arange(chips, dtype=jnp.int32)[:, None]
    gate_map = jnp.zeros((chips, length), f32)
    for k in range(topk_count):
        gate_map += jnp.where(ids_t[k][None, :] == numbers, gates_t[k][None, :], 0.0)
    mine = [w_query, w_out.T, w_up, rows_of(w_latent, core), gains, gate_map]
    shared = [False, False, False, True, False, False]
    pieces = (
        cut(0, mine[0].shape[0], GATHER_ORDERS)
        + cut(1, mine[1].shape[0], GATHER_ORDERS)
        + cut(2, mine[2].shape[0], ((1, (Z, Y, X)), (1, (Z, X, Y))))
        + cut(3, mine[3].shape[0], ((1, (X, Y, Z)),), core_last=True)
        + cut(4, mine[4].shape[0], ((1, (Z, Y, X)),))
        + cut(5, mine[5].shape[0], ((1, (Z, X, Y)),))
    )
    got = gather(grid, mine, shared, pieces, 1)
    full_query = got[0].reshape(width, -1)
    full_out_t = got[1].reshape(width, -1)
    full_up = got[2].reshape(kv_rank, -1)
    full_latent = got[3].reshape(width, -1)
    all_gains = got[4].reshape(chips, 16, -1)[:, 0].astype(f32)
    gain_one = all_gains[:, :gain_rows].reshape(-1)
    gain_two = all_gains[:, gain_rows : 2 * gain_rows].reshape(-1)
    gain_latent = all_gains[:, 2 * gain_rows : 2 * gain_rows + latent_rows].reshape(-1)
    gates = lax.dynamic_index_in_dim(got[5].reshape(chips, -1, length), chip, 1, keepdims=False)

    def all_rows(part, after):
        part, after = lax.optimization_barrier((part, after))
        return lax.all_gather(part, ("dp", "tensor"), axis=0, tiled=True), after

    cot_half = rows_of(cotangent, core)
    cot_bf = cot_half.astype(bf16)
    cot_left, gain_two = all_rows(cot_bf[:, : width // 2], gain_two)

    cosine, sine = rope_tables(length)
    scale = (NOPE + ROPE) ** (-0.5)
    segment_row = segment_ids[0]
    position = jnp.arange(length, dtype=jnp.int32)
    allowed = (segment_row[:, None] == segment_row[None, :]) & (
        position[None, :] <= position[:, None]
    )
    tokens_f = hidden_in.astype(f32)
    normed_f, inverse_one = rms_forward(tokens_f, gain_one)
    normed = normed_f.astype(bf16)
    query_all = lax.optimization_barrier(jnp.dot(normed, full_query, preferred_element_type=f32))
    query_all = query_all.reshape(length, head_count, NOPE + ROPE)
    query_rope = rotate(query_all[..., NOPE:], cosine[:, None, :], sine[:, None, :])
    queries = jnp.concatenate([query_all[..., :NOPE], query_rope], axis=-1).astype(bf16)
    latent_all = jnp.dot(normed, full_latent, preferred_element_type=f32)
    latent = latent_all[:, :kv_rank]
    latent_normed, latent_inverse = rms_forward(latent, gain_latent)
    latent_bf = latent_normed.astype(bf16)
    key_rope = rotate(latent_all[:, kv_rank:], cosine, sine).astype(bf16)
    expanded = jnp.dot(latent_bf, full_up, preferred_element_type=f32).astype(bf16)
    expanded = expanded.reshape(length, head_count, NOPE + VDIM)
    key_all = jnp.concatenate(
        [expanded[..., :NOPE], jnp.broadcast_to(key_rope[:, None, :], (length, head_count, ROPE))],
        axis=-1,
    )
    values = expanded[..., NOPE:]
    scores = jnp.einsum("qhd,khd->hqk", queries, key_all, preferred_element_type=f32) * scale
    raw_probs = jnp.where(allowed[None], jnp.exp(scores), 0.0)
    totals = jnp.sum(raw_probs, axis=-1, keepdims=True)
    log_total = jnp.log(totals)
    attn_weights = (raw_probs / totals).astype(bf16)
    context = jnp.einsum("hqk,khd->qhd", attn_weights, values, preferred_element_type=f32)
    context = context.reshape(length, head_count * VDIM).astype(bf16)
    attended_part = lax.dot_general(
        context, full_out_t, (((1,), (1,)), ((), ())), preferred_element_type=f32
    )
    (other,) = pair(grid, [rows_of(attended_part, 1 - core)], False, 5)
    residual = rows_of(tokens_f, core) + (rows_of(attended_part, core) + other)
    ffn_f, inverse_two = rms_forward(residual, gain_two)
    ffn_in = ffn_f.astype(bf16)

    ffn_in, cot_left = lax.optimization_barrier((ffn_in, cot_left))
    (ffn_all,) = gather(grid, [ffn_in], [True], cut(0, half, GATHER_ORDERS, core_last=True), 2)
    ffn_all = ffn_all.reshape(-1, width)
    cot_right, ffn_all = all_rows(cot_bf[:, width // 2 :], ffn_all)

    routed = gates > 0.0
    triangle = (position[:, None] < position[None, :]).astype(bf16)
    slot = jnp.dot(routed.astype(bf16), triangle, preferred_element_type=f32).astype(jnp.int32)
    chosen = routed[:, None, :] & (slot[:, None, :] == jnp.arange(capacity, dtype=jnp.int32)[None, :, None])
    pick = chosen.astype(bf16)
    gate_slot = jnp.sum(jnp.where(chosen, gates[:, None, :], 0.0), axis=-1)[..., None]

    def take(rows):
        return jnp.einsum(
            "sct,std->scd", pick, rows.reshape(chips, length, -1), preferred_element_type=f32
        )

    def spread(rows, units, weight):
        return spread_rows(pick, rows.reshape(chips, capacity, width), units, weight)

    expert_rows = take(ffn_all).astype(bf16).reshape(-1, width)
    gate_rows = gate_slot.reshape(-1, 1)
    local_gate, local_up, local_down = expert_gate[0], expert_up[0], expert_down[0]
    gate_projected = jnp.dot(expert_rows, local_gate, preferred_element_type=f32)
    up_projected = jnp.dot(expert_rows, local_up, preferred_element_type=f32)
    expert_hidden = (jax.nn.silu(gate_projected) * up_projected).astype(bf16)
    expert_part = jnp.dot(expert_hidden, local_down, preferred_element_type=f32)
    weighted = (gate_rows * expert_part).astype(bf16)
    shared_gu = jnp.dot(ffn_all, s_gate_up, preferred_element_type=f32)
    shared_g, shared_u = shared_gu[:, :lanes], shared_gu[:, lanes:]
    shared_hidden = (jax.nn.silu(shared_g) * shared_u).astype(bf16)
    forward_part = spread(weighted, shared_hidden, s_down_t)
    block_shape = grid + (2, half, width)
    reduce_pieces = cut(0, half, REDUCE_ORDERS, core_first=True)
    forward_part, cot_left, cot_right = lax.optimization_barrier((forward_part, cot_left, cot_right))
    grad_rows = jnp.concatenate(
        [(gate_slot * take(part)).astype(bf16) for part in (cot_left, cot_right)], axis=-1
    ).reshape(-1, width)
    ffn_total = lax.psum_scatter(forward_part, ("dp", "tensor"), scatter_dimension=0, tiled=True)

    hidden_gradient = lax.dot_general(
        grad_rows, local_down, (((1,), (1,)), ((), ())), preferred_element_type=f32
    )
    gate_gradient = (hidden_gradient * up_projected * silu_slope(gate_projected)).astype(bf16)
    up_gradient = (hidden_gradient * jax.nn.silu(gate_projected)).astype(bf16)
    back_part = lax.dot_general(
        gate_gradient, local_gate, (((1,), (1,)), ((), ())), preferred_element_type=f32
    ) + lax.dot_general(up_gradient, local_up, (((1,), (1,)), ((), ())), preferred_element_type=f32)
    shared_hg = jnp.dot(cot_left, s_down_t[: width // 2], preferred_element_type=f32) + jnp.dot(
        cot_right, s_down_t[width // 2 :], preferred_element_type=f32
    )
    grad_units = jnp.concatenate(
        [shared_hg * shared_u * silu_slope(shared_g), shared_hg * jax.nn.silu(shared_g)], axis=1
    ).astype(bf16)
    backward_part = spread(back_part.astype(bf16), grad_units, s_gate_up)
    (grad_ffn,) = reduce(grid, [backward_part.reshape(block_shape)], [True], reduce_pieces, 3)

    grad_expert_down = jnp.dot(expert_hidden.T, grad_rows, preferred_element_type=f32)
    grad_expert_gate = jnp.dot(expert_rows.T, gate_gradient, preferred_element_type=f32)
    gradient_expert_upward = jnp.dot(expert_rows.T, up_gradient, preferred_element_type=f32)
    over_rows = (((0,), (0,)), ((), ()))
    down_parts = [
        lax.dot_general(shared_hidden, part, over_rows, preferred_element_type=f32).astype(bf16)
        for part in (cot_left, cot_right)
    ]
    unit_grads = lax.dot_general(grad_units, ffn_all, over_rows, preferred_element_type=f32)
    unit_grads, *down_parts = lax.optimization_barrier((unit_grads.astype(bf16), *down_parts))
    shared_grads = jnp.concatenate([unit_grads, jnp.concatenate(down_parts, axis=1)])
    returned = lax.all_to_all(
        shared_grads.reshape(3 * lanes, chips, model_rows).transpose(1, 0, 2),
        "dp",
        split_axis=0,
        concat_axis=0,
        tiled=True,
    ).astype(f32)
    s_sgate, s_sup, s_sdown = (
        returned[:, i * lanes : i * lanes + part_units].reshape(-1, model_rows) for i in range(3)
    )
    s_sgate, s_sup = s_sgate.T, s_sup.T

    grad_res_part, g_fgain = rms_backward(residual, inverse_two, gain_two, grad_ffn)
    grad_residual = cot_half + grad_res_part
    (grad_attn,) = pair(grid, [grad_residual.astype(bf16)], True, 6)
    grad_attn = grad_attn.reshape(length, width)
    g_out_t = jnp.dot(grad_attn.T, context, preferred_element_type=f32)
    g_out_t, ffn_total = lax.optimization_barrier((g_out_t.astype(bf16), ffn_total))
    s_out_t = lax.psum_scatter(g_out_t, "dp", scatter_dimension=0, tiled=True)
    grad_context = (
        jnp.dot(grad_attn, full_out_t, preferred_element_type=f32)
        .astype(bf16)
        .reshape(length, head_count, VDIM)
    )
    probs = jnp.where(allowed[None], jnp.exp(scores - log_total), 0.0)
    weights_back = probs.astype(bf16)
    grad_values = jnp.einsum("hqk,qhd->khd", weights_back, grad_context, preferred_element_type=f32)
    grad_weights = jnp.einsum("qhd,khd->hqk", grad_context, values, preferred_element_type=f32)
    row_delta = jnp.sum(probs * grad_weights, axis=-1, keepdims=True)
    grad_scores = (probs * (grad_weights - row_delta) * scale).astype(bf16)
    grad_queries = jnp.einsum("hqk,khd->qhd", grad_scores, key_all, preferred_element_type=f32)
    grad_keys = jnp.einsum("hqk,qhd->khd", grad_scores, queries, preferred_element_type=f32)
    grad_qrope = rotate(grad_queries[..., NOPE:], cosine[:, None, :], -sine[:, None, :])
    grad_query_all = (
        jnp.concatenate([grad_queries[..., :NOPE], grad_qrope], axis=-1)
        .reshape(length, head_count * (NOPE + ROPE))
        .astype(bf16)
    )
    grad_expanded = (
        jnp.concatenate([grad_keys[..., :NOPE], grad_values], axis=-1)
        .reshape(length, head_count * (NOPE + VDIM))
        .astype(bf16)
    )
    g_up = jnp.dot(latent_bf.T, grad_expanded, preferred_element_type=f32)
    g_query = jnp.dot(normed.T, grad_query_all, preferred_element_type=f32)
    latent_part = lax.dot_general(
        grad_expanded, full_up, (((1,), (1,)), ((), ())), preferred_element_type=f32
    )
    rope_part = rotate(jnp.sum(grad_keys[..., NOPE:], axis=1), cosine, -sine)
    latent_part = jnp.concatenate([latent_part, rope_part], axis=-1)
    input_part = lax.dot_general(
        grad_query_all, full_query, (((1,), (1,)), ((), ())), preferred_element_type=f32
    )
    latent_other, input_other = pair(
        grid, [rows_of(latent_part, 1 - core), rows_of(input_part, 1 - core)], False, 7
    )
    latent_sum = rows_of(latent_part, core) + latent_other
    grad_latent, g_lgain = rms_backward(
        rows_of(latent, core), rows_of(latent_inverse, core), gain_latent, latent_sum[:, :kv_rank]
    )
    grad_latent_all = jnp.concatenate([grad_latent, latent_sum[:, kv_rank:]], axis=-1).astype(bf16)
    g_latent = jnp.dot(rows_of(normed, core).T, grad_latent_all, preferred_element_type=f32)
    grad_normed = (rows_of(input_part, core) + input_other) + lax.dot_general(
        grad_latent_all, full_latent, (((1,), (1,)), ((), ())), preferred_element_type=f32
    )
    grad_in_part, g_norm = rms_backward(
        rows_of(tokens_f, core), rows_of(inverse_one, core), gain_one, grad_normed
    )
    grad_input_half = grad_residual + grad_in_part

    g_gains = jnp.concatenate(
        [
            g_norm.reshape(chips, gain_rows),
            g_fgain.reshape(chips, gain_rows),
            jnp.pad(g_lgain.reshape(chips, latent_rows), ((0, 0), (0, gain_rows - latent_rows))),
        ],
        axis=1,
    )
    g_gains = jnp.pad(g_gains[:, None, :], ((0, 0), (0, 15), (0, 0)))
    terms = [
        g_query.astype(bf16).reshape(grid + (-1, g_query.shape[1])),
        g_up.astype(bf16).reshape(grid + (-1, g_up.shape[1])),
        g_latent.astype(bf16).reshape(grid + (2, -1, g_latent.shape[1])),
        g_gains.astype(bf16).reshape(grid + (16, -1)),
    ]
    pieces = (
        cut(0, terms[0].shape[-2], REDUCE_ORDERS)
        + cut(1, terms[1].shape[-2], ((1, (X, Y, Z)), (1, (Y, X, Z))))
        + cut(2, terms[2].shape[-2], ((1, (Z, X, Y)),), core_first=True)
        + cut(3, terms[3].shape[-2], ((1, (X, Y, Z)),))
    )
    s_query, s_up, latent_half, gain_sums = reduce(
        grid, terms, [False, False, True, False], pieces, 4
    )
    ffn_total, s_out_t, gain_sums = lax.optimization_barrier((ffn_total, s_out_t, gain_sums))
    s_out_t = s_out_t.astype(f32)
    output_half = (residual + ffn_total.astype(f32)).astype(bf16)
    output, grad_input, s_latent, gain_sums = pair(
        grid, [output_half, grad_input_half, latent_half, gain_sums], True, 8
    )
    gain_sums = gain_sums[0, 0] + gain_sums[1, 0]
    return (
        output.reshape(length, width),
        grad_input.reshape(length, width),
        gain_sums[:gain_rows],
        s_query,
        s_latent.reshape(-1, s_latent.shape[-1]),
        gain_sums[2 * gain_rows : 2 * gain_rows + latent_rows],
        s_up,
        s_out_t.T,
        gain_sums[gain_rows : 2 * gain_rows],
        s_sgate,
        s_sup,
        s_sdown,
        grad_expert_gate[None],
        gradient_expert_upward[None],
        grad_expert_down[None],
    )


def chip_grid(mesh):
    coords = [tuple(getattr(device, "coords", ())) for device in mesh.devices[:, 0]]
    if any(len(spot) != 3 for spot in coords):
        return None
    low = [min(spot[axis] for spot in coords) for axis in range(3)]
    sizes = [max(spot[axis] for spot in coords) - low[axis] + 1 for axis in range(3)]
    steps = []
    for axis in range(3):
        steps.append(next((i for i, spot in enumerate(coords) if spot[axis] != low[axis]), 0))
    order = sorted(range(3), key=lambda axis: -steps[axis])
    grid = tuple(sizes[axis] for axis in order)
    for index, spot in enumerate(coords):
        for axis in reversed(order):
            if index % sizes[axis] != spot[axis] - low[axis]:
                return None
            index //= sizes[axis]
    return grid if min(grid) >= 2 else None


def solution(mesh):
    in_specs = (
        P("dp", None),
        P("dp"),
        P("dp", "tensor"),
        P("dp", None),
        P("dp"),
        P("dp", "tensor"),
        P("tensor", "dp"),
        P("dp"),
        P("dp", "tensor"),
        P("dp", "tensor"),
        P("tensor", "dp"),
        P("dp", None, "tensor"),
        P("dp", None, "tensor"),
        P("dp", "tensor", None),
        P("dp", None),
        P("dp", None),
        P("dp", None),
        P("dp", None),
    )
    out_specs = (
        P("dp", None),
        P("dp", None),
        P("dp"),
        P("dp", "tensor"),
        P("dp", None),
        P("dp"),
        P("dp", "tensor"),
        P("tensor", "dp"),
        P("dp"),
        P("dp", "tensor"),
        P("dp", "tensor"),
        P("tensor", "dp"),
        P("dp", None, "tensor"),
        P("dp", None, "tensor"),
        P("dp", "tensor", None),
    )
    grid = chip_grid(mesh)

    def step(*args):
        dense = grid is not None and 4 * args[15].shape[1] >= mesh.shape["dp"]
        body = functools.partial(dense_shards, grid) if dense else shards
        return jax.shard_map(
            body, mesh=mesh, in_specs=in_specs, out_specs=out_specs, check_vma=False
        )(*args)

    return step
```

```python
import functools

import jax
import jax.numpy as jnp
from jax import lax
from jax.experimental import pallas as pl
from jax.experimental.pallas import tpu as pltpu
from jax.sharding import PartitionSpec as P


NOPE = 128
ROPE = 64
VDIM = 128


EPSILON = 1e-06


def rope_tables(length):
    half_width = ROPE // 2
    frequency = 10000.0 ** (-(jnp.arange(half_width, dtype=jnp.float32) * 2.0 / ROPE))
    angles = jnp.arange(length, dtype=jnp.float32)[:, None] * frequency[None, :]
    return (jnp.cos(angles), jnp.sin(angles))


def rotate(vectors, cosine, sine):
    half_width = vectors.shape[-1] // 2
    first_half = vectors[..., :half_width]
    second = vectors[..., half_width:]
    return jnp.concatenate(
        [first_half * cosine - second * sine, second * cosine + first_half * sine], axis=-1
    )


def silu_slope(gate_projected):
    sigmoid_value = jax.nn.sigmoid(gate_projected)
    return sigmoid_value * (1.0 + gate_projected * (1.0 - sigmoid_value))


def rms_forward(vectors, gain):
    inverse = lax.rsqrt(jnp.mean(vectors * vectors, axis=-1, keepdims=True) + EPSILON)
    return (vectors * inverse * gain, inverse)


def rms_backward(vectors, inverse, gain, grad_out):
    scaled = gain * grad_out
    grad_in = inverse * scaled - vectors * inverse**3 * jnp.mean(
        scaled * vectors, axis=-1, keepdims=True
    )
    return (grad_in, jnp.sum(grad_out * vectors * inverse, axis=0))


def pick_owned(
    returned_rows, flat_ids, slot_index, half_rows, core_index, length, topk_count, width
):
    owned = slot_index // half_rows == core_index
    place = jnp.where(owned, flat_ids * half_rows + slot_index - core_index * half_rows, 0)
    picked = returned_rows[place].astype(jnp.float32) * owned[:, None].astype(jnp.float32)
    return picked.reshape(length, topk_count, width)


def shards(
    hidden_in,
    norm_gain,
    w_query,
    w_latent,
    latent_gain,
    w_up,
    w_out,
    ffn_gain,
    shared_gate,
    shared_up,
    shared_down,
    expert_gate,
    expert_up,
    expert_down,
    gate_values,
    expert_ids,
    segment_ids,
    cotangent,
):
    kept = (
        lax.all_gather(norm_gain, "dp", axis=0, tiled=True),
        lax.all_gather(w_query, "dp", axis=0, tiled=True),
        lax.all_gather(w_latent, "dp", axis=0, tiled=True),
        lax.all_gather(latent_gain, "dp", axis=0, tiled=True),
        lax.all_gather(w_up, "dp", axis=0, tiled=True),
        lax.all_gather(w_out, "dp", axis=1, tiled=True),
        lax.all_gather(ffn_gain, "dp", axis=0, tiled=True),
        lax.all_gather(shared_gate, "dp", axis=0, tiled=True),
        lax.all_gather(shared_up, "dp", axis=0, tiled=True),
        lax.all_gather(shared_down, "dp", axis=1, tiled=True),
    )
    (
        full_norm,
        full_query,
        full_latent,
        full_lgain,
        full_up,
        full_out,
        full_fgain,
        full_sgate,
        full_sup,
        full_sdown,
    ) = kept
    length = hidden_in.shape[0]
    width = hidden_in.shape[1]
    topk_count = expert_ids.shape[1]
    head_count = full_query.shape[1] // (NOPE + ROPE)
    kv_rank = full_up.shape[0]
    experts_total = lax.axis_size("dp")
    capacity = max(2, 2 * (length * topk_count * 7 // (12 * experts_total)))
    cosine, sine = rope_tables(length)
    scale = (NOPE + ROPE) ** (-0.5)
    segment_row = segment_ids[0]
    position = jnp.arange(length, dtype=jnp.int32)
    allowed = (segment_row[:, None] == segment_row[None, :]) & (
        position[None, :] <= position[:, None]
    )
    tokens_f = hidden_in.astype(jnp.float32)
    normed_f, inverse_one = rms_forward(tokens_f, full_norm.astype(jnp.float32))
    normed = normed_f.astype(jnp.bfloat16)
    query_all = jnp.dot(normed, full_query, preferred_element_type=jnp.float32).reshape(
        length, head_count, NOPE + ROPE
    )
    query_rope = rotate(query_all[..., NOPE:], cosine[:, None, :], sine[:, None, :])
    queries = jnp.concatenate([query_all[..., :NOPE], query_rope], axis=-1).astype(jnp.bfloat16)
    latent_all = jnp.dot(normed, full_latent, preferred_element_type=jnp.float32)
    latent = latent_all[:, :kv_rank]
    latent_normed, latent_inverse = rms_forward(latent, full_lgain.astype(jnp.float32))
    latent_bf = latent_normed.astype(jnp.bfloat16)
    key_rope = rotate(latent_all[:, kv_rank:], cosine, sine).astype(jnp.bfloat16)
    expanded = jnp.dot(latent_bf, full_up, preferred_element_type=jnp.float32).astype(jnp.bfloat16)
    expanded = expanded.reshape(length, head_count, NOPE + VDIM)
    key_all = jnp.concatenate(
        [expanded[..., :NOPE], jnp.broadcast_to(key_rope[:, None, :], (length, head_count, ROPE))],
        axis=-1,
    )
    values = expanded[..., NOPE:]
    scores = (
        jnp.einsum("qhd,khd->hqk", queries, key_all, preferred_element_type=jnp.float32) * scale
    )
    raw_probs = jnp.where(allowed[None], jnp.exp(scores), 0.0)
    totals = jnp.sum(raw_probs, axis=-1, keepdims=True)
    log_total = jnp.log(totals)
    attn_weights = (raw_probs / totals).astype(jnp.bfloat16)
    context = jnp.einsum("hqk,khd->qhd", attn_weights, values, preferred_element_type=jnp.float32)
    context = context.reshape(length, head_count * VDIM).astype(jnp.bfloat16)
    attended_part = jnp.dot(context, full_out, preferred_element_type=jnp.float32)
    attended = lax.psum(attended_part, "tensor")
    residual = tokens_f + attended
    ffn_gain_f = full_fgain.astype(jnp.float32)
    ffn_f, inverse_two = rms_forward(residual, ffn_gain_f)
    ffn_in = ffn_f.astype(jnp.bfloat16)
    pair_count = length * topk_count
    flat_ids = expert_ids.reshape(-1)
    onehot = (flat_ids[:, None] == jnp.arange(experts_total, dtype=jnp.int32)[None, :]).astype(
        jnp.int32
    )
    earlier = jnp.cumsum(onehot, axis=0) - onehot
    slot_index = jnp.sum(earlier * onehot, axis=1)
    target = flat_ids * capacity + slot_index
    pair_of_slot = (
        jnp.full((experts_total * capacity,), pair_count, jnp.int32)
        .at[target]
        .set(jnp.arange(pair_count, dtype=jnp.int32))
    )
    token_of_slot = pair_of_slot // topk_count
    ffn_padded = jnp.concatenate([ffn_in, jnp.zeros((1, width), jnp.bfloat16)], axis=0)
    outgoing = ffn_padded[token_of_slot].reshape(experts_total, capacity, width)
    cot_bf = cotangent.astype(jnp.bfloat16)
    grad_rows = (
        (gate_values[:, :, None] * cotangent[:, None, :])
        .astype(jnp.bfloat16)
        .reshape(pair_count, width)
    )
    grad_padded = jnp.concatenate([grad_rows, jnp.zeros((1, width), jnp.bfloat16)], axis=0)
    grad_outgoing = grad_padded[pair_of_slot].reshape(experts_total, capacity, width)
    half_rows = capacity // lax.axis_size("tensor")
    core_index = lax.axis_index("tensor")
    portion = lax.dynamic_slice_in_dim(outgoing, core_index * half_rows, half_rows, 1)
    grad_portion = lax.dynamic_slice_in_dim(grad_outgoing, core_index * half_rows, half_rows, 1)
    arrived_half, grad_half = (
        lax.all_to_all(portion, "dp", split_axis=0, concat_axis=0, tiled=True),
        lax.all_to_all(grad_portion, "dp", split_axis=0, concat_axis=0, tiled=True),
    )
    arrived, grad_arrived = (
        lax.all_gather(arrived_half, "tensor", axis=1, tiled=True),
        lax.all_gather(grad_half, "tensor", axis=1, tiled=True),
    )
    rows_per_expert = arrived.reshape(-1, width)
    grad_arrived = grad_arrived.reshape(-1, width)
    local_gate = expert_gate[0]
    resident_up_weight = expert_up[0]
    local_down = expert_down[0]
    gate_projected = jnp.dot(rows_per_expert, local_gate, preferred_element_type=jnp.float32)
    up_proj = jnp.dot(rows_per_expert, resident_up_weight, preferred_element_type=jnp.float32)
    expert_hidden = (jax.nn.silu(gate_projected) * up_proj).astype(jnp.bfloat16)
    expert_part = jnp.dot(expert_hidden, local_down, preferred_element_type=jnp.float32)
    shared_gproj = jnp.dot(ffn_in, full_sgate, preferred_element_type=jnp.float32)
    shared_uproj = jnp.dot(ffn_in, full_sup, preferred_element_type=jnp.float32)
    shared_hidden = (jax.nn.silu(shared_gproj) * shared_uproj).astype(jnp.bfloat16)
    shared_part = jnp.dot(shared_hidden, full_sdown, preferred_element_type=jnp.float32)
    expert_half = lax.psum_scatter(
        expert_part.reshape(experts_total, capacity, width),
        "tensor",
        scatter_dimension=1,
        tiled=True,
    )
    returned_half = lax.all_to_all(
        expert_half.astype(jnp.bfloat16), "dp", split_axis=0, concat_axis=0, tiled=True
    ).reshape(-1, width)
    picked = pick_owned(
        returned_half, flat_ids, slot_index, half_rows, core_index, length, topk_count, width
    )
    routed_part = jnp.sum(picked * gate_values[:, :, None], axis=1)
    ffn_total = lax.psum(shared_part + routed_part, "tensor")
    output = (residual + ffn_total).astype(jnp.bfloat16)
    expert_hidden_gradient = jnp.dot(grad_arrived, local_down.T, preferred_element_type=jnp.float32)
    expert_gate_gradient = (expert_hidden_gradient * up_proj * silu_slope(gate_projected)).astype(
        jnp.bfloat16
    )
    expert_up_gradient = (expert_hidden_gradient * jax.nn.silu(gate_projected)).astype(jnp.bfloat16)
    grad_expert_down = jnp.dot(expert_hidden.T, grad_arrived, preferred_element_type=jnp.float32)
    grad_expert_gate = jnp.dot(
        rows_per_expert.T, expert_gate_gradient, preferred_element_type=jnp.float32
    )
    gradient_expert_upward = jnp.dot(
        rows_per_expert.T, expert_up_gradient, preferred_element_type=jnp.float32
    )
    expert_back_part = jnp.dot(
        expert_gate_gradient, local_gate.T, preferred_element_type=jnp.float32
    ) + jnp.dot(expert_up_gradient, resident_up_weight.T, preferred_element_type=jnp.float32)
    grad_shidden = jnp.dot(cot_bf, full_sdown.T, preferred_element_type=jnp.float32)
    grad_sgate = (grad_shidden * shared_uproj * silu_slope(shared_gproj)).astype(jnp.bfloat16)
    grad_sup = (grad_shidden * jax.nn.silu(shared_gproj)).astype(jnp.bfloat16)
    g_sdown = jnp.dot(shared_hidden.T, cot_bf, preferred_element_type=jnp.float32)
    g_sgate = jnp.dot(ffn_in.T, grad_sgate, preferred_element_type=jnp.float32)
    g_sup = jnp.dot(ffn_in.T, grad_sup, preferred_element_type=jnp.float32)
    shared_back_part = jnp.dot(
        grad_sgate, full_sgate.T, preferred_element_type=jnp.float32
    ) + jnp.dot(grad_sup, full_sup.T, preferred_element_type=jnp.float32)
    back_half = lax.psum_scatter(
        expert_back_part.reshape(experts_total, capacity, width),
        "tensor",
        scatter_dimension=1,
        tiled=True,
    )
    back_returned_half = lax.all_to_all(
        back_half.astype(jnp.bfloat16), "dp", split_axis=0, concat_axis=0, tiled=True
    ).reshape(-1, width)
    back_picked = pick_owned(
        back_returned_half, flat_ids, slot_index, half_rows, core_index, length, topk_count, width
    )
    grad_ffn = lax.psum(shared_back_part + jnp.sum(back_picked, axis=1), "tensor")
    grad_res_part, g_fgain = rms_backward(residual, inverse_two, ffn_gain_f, grad_ffn)
    grad_residual = cotangent + grad_res_part
    grad_attn = grad_residual.astype(jnp.bfloat16)
    g_out = jnp.dot(context.T, grad_attn, preferred_element_type=jnp.float32)
    grad_context = (
        jnp.dot(grad_attn, full_out.T, preferred_element_type=jnp.float32)
        .astype(jnp.bfloat16)
        .reshape(length, head_count, VDIM)
    )
    probs = jnp.where(allowed[None], jnp.exp(scores - log_total), 0.0)
    weights_back = probs.astype(jnp.bfloat16)
    grad_values = jnp.einsum(
        "hqk,qhd->khd", weights_back, grad_context, preferred_element_type=jnp.float32
    )
    grad_weights = jnp.einsum(
        "qhd,khd->hqk", grad_context, values, preferred_element_type=jnp.float32
    )
    row_delta = jnp.sum(probs * grad_weights, axis=-1, keepdims=True)
    grad_scores = (probs * (grad_weights - row_delta) * scale).astype(jnp.bfloat16)
    grad_queries = jnp.einsum(
        "hqk,khd->qhd", grad_scores, key_all, preferred_element_type=jnp.float32
    )
    grad_keys = jnp.einsum("hqk,qhd->khd", grad_scores, queries, preferred_element_type=jnp.float32)
    grad_qrope = rotate(grad_queries[..., NOPE:], cosine[:, None, :], -sine[:, None, :])
    grad_query_all = (
        jnp.concatenate([grad_queries[..., :NOPE], grad_qrope], axis=-1)
        .reshape(length, head_count * (NOPE + ROPE))
        .astype(jnp.bfloat16)
    )
    grad_expanded = (
        jnp.concatenate([grad_keys[..., :NOPE], grad_values], axis=-1)
        .reshape(length, head_count * (NOPE + VDIM))
        .astype(jnp.bfloat16)
    )
    g_up = jnp.dot(latent_bf.T, grad_expanded, preferred_element_type=jnp.float32)
    g_query = jnp.dot(normed.T, grad_query_all, preferred_element_type=jnp.float32)
    latent_part = jnp.dot(grad_expanded, full_up.T, preferred_element_type=jnp.float32)
    rope_part = rotate(jnp.sum(grad_keys[..., NOPE:], axis=1), cosine, -sine)
    grad_latent_normed, grad_key_rope = lax.psum((latent_part, rope_part), "tensor")
    grad_latent, g_lgain = rms_backward(
        latent, latent_inverse, full_lgain.astype(jnp.float32), grad_latent_normed
    )
    grad_latent_all = jnp.concatenate([grad_latent, grad_key_rope], axis=-1).astype(jnp.bfloat16)
    g_latent = jnp.dot(normed.T, grad_latent_all, preferred_element_type=jnp.float32)
    input_part = jnp.dot(grad_query_all, full_query.T, preferred_element_type=jnp.float32)
    grad_normed = lax.psum(input_part, "tensor") + jnp.dot(
        grad_latent_all, full_latent.T, preferred_element_type=jnp.float32
    )
    grad_in_part, g_norm = rms_backward(
        tokens_f, inverse_one, full_norm.astype(jnp.float32), grad_normed
    )
    grad_input = grad_residual + grad_in_part
    summed = (
        lax.psum_scatter(g_norm, "dp", scatter_dimension=0, tiled=True),
        lax.psum_scatter(g_query, "dp", scatter_dimension=0, tiled=True),
        lax.psum_scatter(g_latent, "dp", scatter_dimension=0, tiled=True),
        lax.psum_scatter(g_lgain, "dp", scatter_dimension=0, tiled=True),
        lax.psum_scatter(g_up, "dp", scatter_dimension=0, tiled=True),
        lax.psum_scatter(g_out, "dp", scatter_dimension=1, tiled=True),
        lax.psum_scatter(g_fgain, "dp", scatter_dimension=0, tiled=True),
        lax.psum_scatter(g_sgate, "dp", scatter_dimension=0, tiled=True),
        lax.psum_scatter(g_sup, "dp", scatter_dimension=0, tiled=True),
        lax.psum_scatter(g_sdown, "dp", scatter_dimension=1, tiled=True),
    )
    s_norm, s_query, s_latent, s_lgain, s_up, s_out, s_fgain, s_sgate, s_sup, s_sdown = summed
    return (
        output,
        grad_input,
        s_norm,
        s_query,
        s_latent,
        s_lgain,
        s_up,
        s_out,
        s_fgain,
        s_sgate,
        s_sup,
        s_sdown,
        grad_expert_gate[None],
        gradient_expert_upward[None],
        grad_expert_down[None],
    )


MESH = pl.DeviceIdType.MESH


def place_of(grid):
    index = lax.axis_index("dp")
    place = []
    for size in reversed(grid):
        place.append(lax.rem(index, size))
        index = index // size
    return tuple(reversed(place)) + (lax.axis_index("tensor"),)


def device_at(grid, place):
    index = place[0]
    for size, spot in zip(grid[1:], place[1:-1]):
        index = index * size + spot
    return (index, place[-1])


def moved(place, dim, spot):
    return tuple(spot if axis == dim else at for axis, at in enumerate(place))


def greet(grid, place):
    sizes = grid + (2,)
    barrier = pltpu.get_barrier_semaphore()
    for dim, size in enumerate(sizes):
        for step in (-1, 1):
            if size == 2:
                if step == 1:
                    pl.semaphore_signal(barrier, inc=1, device_id=device_at(grid, moved(place, dim, 1 - place[dim])), device_id_type=MESH)
                continue
            spot = place[dim] + step

            @pl.when((spot >= 0) & (spot < size))
            def _():
                pl.semaphore_signal(barrier, inc=1, device_id=device_at(grid, moved(place, dim, spot)), device_id_type=MESH)

    peers = 0
    for dim, size in enumerate(sizes):
        if size == 2:
            peers += 1
        else:
            peers += jnp.minimum(place[dim], 1) + jnp.minimum(size - 1 - place[dim], 1)
    pl.semaphore_wait(barrier, peers)


def stage_plan(sizes, order, weight):
    plan, now, held = [], 0.0, 1
    for dim in order:
        for step in range(sizes[dim] - 1):
            cost = weight * held * (0.15 if dim == 3 else 1.0)
            plan.append((now, dim, step))
            now += cost
        held *= sizes[dim]
    plan.append((now, None, 0))
    return plan


def gather_body(grid, pieces, shared_flags, input_count, *refs):
    sizes = grid + (2,)
    inputs = refs[:input_count]
    outputs = refs[input_count : 2 * input_count]
    send_sem, recv_sem, own_sem = refs[2 * input_count :]
    place = place_of(grid)

    def window(piece, chosen):
        which, start, rows, _ = piece
        spots = tuple(chosen.get(dim, place[dim]) for dim in range(4 if shared_flags[which] else 3))
        return outputs[which].at[spots + (pl.ds(start, rows),)]

    own = []
    for number, piece in enumerate(pieces):
        which, start, rows, order = piece
        copy = pltpu.make_async_copy(inputs[which].at[pl.ds(start, rows)], window(piece, {}), own_sem.at[number])
        copy.start()
        own.append(copy)
    greet(grid, place)

    stages = []
    for number, piece in enumerate(pieces):
        which, start, rows, order = piece
        weight = rows * inputs[which].shape[1]
        for rank, (when, dim, step) in enumerate(stage_plan(sizes, order, weight)):
            stages.append((when, number, rank, dim, step))
    stages.sort(key=lambda s: s[:3])
    pending_recv = {number: [] for number in range(len(pieces))}
    sends = []

    def copies(number, rank, dim, step):
        piece = pieces[number]
        which, start, rows, order = piece
        gathered = {}
        for earlier in order[: order.index(dim)]:
            gathered[earlier] = slice(None)
        size = sizes[dim]
        made = []
        base = 2 * rank
        if size == 2:
            part = window(piece, gathered)
            if not gathered:
                source = inputs[which].at[pl.ds(start, rows)]
            else:
                source = part
            copy = pltpu.make_async_remote_copy(
                source, part, send_sem.at[number, base], recv_sem.at[number, base],
                device_id=device_at(grid, moved(place, dim, 1 - place[dim])), device_id_type=MESH)
            made.append((None, None, copy))
            return made
        for way, sign in enumerate((1, -1)):
            spot = place[dim] + sign
            block = place[dim] - sign * step
            inside = (spot >= 0) & (spot < size) & (block >= 0) & (block < size)
            back = place[dim] - sign
            back_block = back - sign * step
            arrives = (back >= 0) & (back < size) & (back_block >= 0) & (back_block < size)
            chosen = dict(gathered)
            chosen[dim] = jnp.clip(block, 0, size - 1)
            part = window(piece, chosen)
            if not gathered and step == 0:
                source = inputs[which].at[pl.ds(start, rows)]
            else:
                source = part
            copy = pltpu.make_async_remote_copy(
                source, part, send_sem.at[number, base + way], recv_sem.at[number, base + way],
                device_id=device_at(grid, moved(place, dim, jnp.clip(spot, 0, size - 1))), device_id_type=MESH)
            made.append((inside, arrives, copy))
        return made

    for when, number, rank, dim, step in stages:
        for condition, copy in pending_recv[number]:
            if condition is None:
                copy.wait_recv()
            else:
                pl.when(condition)(copy.wait_recv)
        pending_recv[number] = []
        if rank == 1:
            own[number].wait()
        if dim is None:
            continue
        for send_ok, recv_ok, copy in copies(number, rank, dim, step):
            if send_ok is None:
                copy.start()
            else:
                pl.when(send_ok)(copy.start)
            sends.append((send_ok, copy))
            pending_recv[number].append((recv_ok, copy))
    for condition, copy in sends:
        if condition is None:
            copy.wait_send()
        else:
            pl.when(condition)(copy.wait_send)


def gather(grid, arrays, shared_flags, pieces, collective_id):
    out_shape = [
        jax.ShapeDtypeStruct(grid + ((2,) if shared else ()) + array.shape, array.dtype)
        for array, shared in zip(arrays, shared_flags)
    ]
    most = sum(size - 1 for size in grid) + 1
    return pl.pallas_call(
        functools.partial(gather_body, grid, pieces, shared_flags, len(arrays)),
        out_shape=out_shape,
        in_specs=[pl.BlockSpec(memory_space=pltpu.VMEM)] * len(arrays),
        out_specs=[pl.BlockSpec(memory_space=pl.ANY)] * len(arrays),
        scratch_shapes=[
            pltpu.SemaphoreType.DMA((len(pieces), 2 * most)),
            pltpu.SemaphoreType.DMA((len(pieces), 2 * most)),
            pltpu.SemaphoreType.DMA((len(pieces),)),
        ],
        compiler_params=pltpu.CompilerParams(collective_id=collective_id, has_side_effects=True, vmem_limit_bytes=16 << 20),
        name="gather_rows",
    )(*arrays)


def reduce_plan(sizes, order, weight):
    plan, now, held = [], 0.0, 1
    for dim in order:
        held *= sizes[dim]
    for dim in order:
        held //= sizes[dim]
        for step in range(sizes[dim] - 1):
            plan.append((now, dim, step))
            now += weight * held * (0.25 if dim == 3 else 1.0)
    plan.append((now, None, 0))
    return plan


def landing_shapes(sizes, order, rows, width):
    shapes = []
    for rank, dim in enumerate(order):
        left = tuple(sizes[d] for d in sorted(order[rank + 1 :]))
        ways = 1 if sizes[dim] == 2 else 2
        shapes.extend([left + (rows, width)] * (ways * (sizes[dim] - 1)))
    return shapes


def kept_index(place, later, dim, dims, kept, spots):
    left = sorted(later)
    return tuple(spots[left.index(d)] if d in later else (kept if d == dim else place[d]) for d in range(dims))


def add_into(target, target_index, source, lead, rows):
    chunk = 16
    total = 1
    for size in lead:
        total *= size

    def step(number, carry):
        block, row = number // (rows // chunk), lax.rem(number, rows // chunk)
        spots, rest = [], block
        for size in reversed(lead):
            spots.append(lax.rem(rest, size))
            rest = rest // size
        spots = tuple(reversed(spots))
        span = pl.ds(pl.multiple_of(row * chunk, chunk), chunk)
        here = target_index(spots) + (span,)
        value = target[here].astype(jnp.float32) + source[spots + (span,)].astype(jnp.float32)
        target[here] = value.astype(target.dtype)
        return carry

    lax.fori_loop(0, total * (rows // chunk), step, 0)


def reduce_body(grid, pieces, shared_flags, input_count, *refs):
    sizes = grid + (2,)
    inputs = refs[:input_count]
    outputs = refs[input_count : 2 * input_count]
    scratch = list(refs[2 * input_count :])
    held = [scratch.pop(0) for _ in pieces]
    landings = []
    for which, start, rows, order in pieces:
        count = len(landing_shapes(sizes, order, rows, inputs[which].shape[-1]))
        landings.append([scratch.pop(0) for _ in range(count)])
    send_sem, recv_sem, own_sem = scratch
    place = place_of(grid)

    loads = []
    for number, (which, start, rows, order) in enumerate(pieces):
        dims = 4 if shared_flags[which] else 3
        source = inputs[which].at[(slice(None),) * dims + (pl.ds(start, rows),)]
        copy = pltpu.make_async_copy(source, held[number], own_sem.at[number])
        copy.start()
        loads.append(copy)
    greet(grid, place)

    stages = []
    for number, (which, start, rows, order) in enumerate(pieces):
        weight = rows * inputs[which].shape[-1]
        for rank, (when, dim, step) in enumerate(reduce_plan(sizes, order, weight)):
            stages.append((when, number, rank, dim, step))
    stages.sort(key=lambda s: s[:3])
    pending = {number: [] for number in range(len(pieces))}
    slots = {number: 0 for number in range(len(pieces))}
    sends = []

    for when, number, rank, dim, step in stages:
        which, start, rows, order = pieces[number]
        dims = 4 if shared_flags[which] else 3
        if rank == 0:
            loads[number].wait()
        for arrives, copy, add in pending[number]:
            if arrives is None:
                copy.wait_recv()
                add()
            else:

                @pl.when(arrives)
                def _():
                    copy.wait_recv()
                    add()

        pending[number] = []
        if dim is None:
            result = outputs[which]

            def finish(chunk_number, carry):
                span = pl.ds(pl.multiple_of(chunk_number * 16, 16), 16)
                value = held[number][tuple(place[:dims]) + (span,)].astype(jnp.float32)
                result[pl.ds(pl.multiple_of(start + chunk_number * 16, 16), 16)] = value
                return carry

            lax.fori_loop(0, rows // 16, finish, 0)
            continue
        later = order[order.index(dim) + 1 :]
        lead = tuple(sizes[d] for d in sorted(later))
        size = sizes[dim]

        def whole(block):
            return tuple(slice(None) if d in later else (block if d == dim else place[d]) for d in range(dims))

        for sign in (1,) if size == 2 else (1, -1):
            landing = landings[number][slots[number]]
            sem = slots[number]
            slots[number] += 1
            if size == 2:
                to, block, kept = 1 - place[dim], 1 - place[dim], place[dim]
                goes = arrives = None
            else:
                to = place[dim] + sign
                block = place[dim] + sign * (size - 1 - step)
                back = place[dim] - sign
                kept = place[dim] + sign * (size - 2 - step)
                goes = (to >= 0) & (to < size) & (block >= 0) & (block < size)
                arrives = (back >= 0) & (back < size) & (kept >= 0) & (kept < size)
                to, block, kept = (jnp.clip(v, 0, size - 1) for v in (to, block, kept))
            copy = pltpu.make_async_remote_copy(
                held[number].at[whole(block)], landing, send_sem.at[number, sem], recv_sem.at[number, sem],
                device_id=device_at(grid, moved(place, dim, to)), device_id_type=MESH)
            if goes is None:
                copy.start()
            else:
                pl.when(goes)(copy.start)
            sends.append((goes, copy))

            index = functools.partial(kept_index, place, later, dim, dims, kept)
            add = functools.partial(add_into, held[number], index, landing, lead, rows)
            pending[number].append((arrives, copy, add))
    for condition, copy in sends:
        if condition is None:
            copy.wait_send()
        else:
            pl.when(condition)(copy.wait_send)


def reduce(grid, arrays, shared_flags, pieces, collective_id):
    sizes = grid + (2,)
    out_shape = [
        jax.ShapeDtypeStruct(array.shape[-2:], jnp.float32)
        for array in arrays
    ]
    scratch, most = [], 1
    for which, start, rows, order in pieces:
        scratch.append(pltpu.VMEM(arrays[which].shape[:-2] + (rows, arrays[which].shape[-1]), arrays[which].dtype))
    for which, start, rows, order in pieces:
        shapes = landing_shapes(sizes, order, rows, arrays[which].shape[-1])
        most = max(most, len(shapes) + 1)
        scratch.extend(pltpu.VMEM(shape, arrays[which].dtype) for shape in shapes)
    return pl.pallas_call(
        functools.partial(reduce_body, grid, pieces, shared_flags, len(arrays)),
        out_shape=out_shape,
        in_specs=[pl.BlockSpec(memory_space=pl.ANY)] * len(arrays),
        out_specs=[pl.BlockSpec(memory_space=pltpu.VMEM)] * len(arrays),
        scratch_shapes=scratch + [
            pltpu.SemaphoreType.DMA((len(pieces), most)),
            pltpu.SemaphoreType.DMA((len(pieces), most)),
            pltpu.SemaphoreType.DMA((len(pieces),)),
        ],
        compiler_params=pltpu.CompilerParams(collective_id=collective_id, has_side_effects=True, vmem_limit_bytes=60 << 20),
        name="reduce_rows",
    )(*arrays)


def pair_body(grid, keep, count, *refs):
    inputs, outputs = refs[:count], refs[count : 2 * count]
    send_sem, recv_sem, own_sem = refs[2 * count :]
    place = place_of(grid)
    partner = device_at(grid, moved(place, 3, 1 - place[3]))
    barrier = pltpu.get_barrier_semaphore()
    pl.semaphore_signal(barrier, inc=1, device_id=partner, device_id_type=MESH)
    own = []
    for number in range(count if keep else 0):
        copy = pltpu.make_async_copy(inputs[number], outputs[number].at[place[3]], own_sem.at[number])
        copy.start()
        own.append(copy)
    pl.semaphore_wait(barrier, 1)
    sent = []
    for number in range(count):
        target = outputs[number].at[place[3]] if keep else outputs[number]
        copy = pltpu.make_async_remote_copy(
            inputs[number], target, send_sem.at[number], recv_sem.at[number],
            device_id=partner, device_id_type=MESH)
        copy.start()
        sent.append(copy)
    for copy in own + sent:
        copy.wait()


def pair(grid, arrays, keep, collective_id):
    count = len(arrays)
    return pl.pallas_call(
        functools.partial(pair_body, grid, keep, count),
        out_shape=[jax.ShapeDtypeStruct(((2,) if keep else ()) + array.shape, array.dtype) for array in arrays],
        in_specs=[pl.BlockSpec(memory_space=pltpu.VMEM if keep else pl.ANY)] * count,
        out_specs=[pl.BlockSpec(memory_space=pl.ANY)] * count,
        scratch_shapes=[pltpu.SemaphoreType.DMA((count,))] * 3,
        compiler_params=pltpu.CompilerParams(
            collective_id=collective_id, has_side_effects=True, vmem_limit_bytes=16 << 20),
        name="pair_rows",
    )(*arrays)


Z, Y, X, C = 0, 1, 2, 3


def cut(which, rows, orders, core_last=False, core_first=False):
    chunks = rows // 16
    total = sum(share for share, _ in orders)
    pieces, start, used = [], 0, 0
    for share, order in orders:
        used += share
        end = chunks * used // total * 16
        if end > start:
            full = ((C,) if core_first else ()) + order + ((C,) if core_last else ())
            pieces.append((which, start, end - start, full))
            start = end
    return pieces


GATHER_ORDERS = ((2, (Z, Y, X)), (2, (Z, X, Y)), (1, (Z, Y, X)), (1, (Z, X, Y)), (2, (Y, X, Z)))
REDUCE_ORDERS = ((1, (X, Y, Z)), (1, (Y, X, Z))) * 3 + ((1, (Z, X, Y)),) * 2


def spread_body(pick_ref, rows_ref, units_ref, weight_ref, out_ref):
    routed = lax.dot_general(
        pick_ref[0], rows_ref[0], (((0,), (0,)), ((), ())), preferred_element_type=jnp.float32
    )
    shared = lax.dot_general(
        units_ref[...], weight_ref[...], (((1,), (1,)), ((), ())), preferred_element_type=jnp.float32
    )
    out_ref[...] = (routed + shared).astype(out_ref.dtype)


def spread_rows(pick, rows, units, weight):
    count, capacity, length = pick.shape
    width = rows.shape[-1]
    lanes = units.shape[-1]
    return pl.pallas_call(
        spread_body,
        grid=(count,),
        out_shape=jax.ShapeDtypeStruct((count * length, width), rows.dtype),
        in_specs=[
            pl.BlockSpec((1, capacity, length), lambda s: (s, 0, 0)),
            pl.BlockSpec((1, capacity, width), lambda s: (s, 0, 0)),
            pl.BlockSpec((length, lanes), lambda s: (s, 0)),
            pl.BlockSpec((width, lanes), lambda s: (0, 0)),
        ],
        out_specs=pl.BlockSpec((length, width), lambda s: (s, 0)),
        compiler_params=pltpu.CompilerParams(vmem_limit_bytes=32 << 20),
        cost_estimate=pl.CostEstimate(
            flops=2 * count * length * width * (capacity + lanes),
            bytes_accessed=2 * count * (length + capacity) * width,
            transcendentals=0,
        ),
        name="spread_rows",
    )(pick, rows, units, weight)


def dense_shards(
    grid,
    hidden_in,
    norm_gain,
    w_query,
    w_latent,
    latent_gain,
    w_up,
    w_out,
    ffn_gain,
    shared_gate,
    shared_up,
    shared_down,
    expert_gate,
    expert_up,
    expert_down,
    gate_values,
    expert_ids,
    segment_ids,
    cotangent,
):
    f32, bf16 = jnp.float32, jnp.bfloat16
    length, width = hidden_in.shape
    half = length // 2
    topk_count = expert_ids.shape[1]
    chips = lax.axis_size("dp")
    head_count = w_query.shape[1] // (NOPE + ROPE)
    kv_rank = latent_gain.shape[0] * chips
    capacity = max(2, 2 * (length * topk_count * 7 // (12 * chips)))
    core = lax.axis_index("tensor")
    chip = lax.axis_index("dp")

    def rows_of(array, which):
        count = array.shape[0] // 2
        return lax.dynamic_slice_in_dim(array, which * count, count, 0)

    part_units = shared_gate.shape[1] // chips
    model_rows = shared_gate.shape[0]
    lanes = -(-part_units // 128) * 128

    def sliced(weight):
        slices = weight.reshape(model_rows, chips, part_units).transpose(1, 0, 2)
        return jnp.pad(slices, ((0, 0), (0, 0), (0, lanes - part_units)))

    stacked = jnp.concatenate([sliced(shared_gate), sliced(shared_up), sliced(shared_down.T)], axis=2)
    resharded = lax.all_to_all(stacked, "dp", split_axis=0, concat_axis=0, tiled=True)
    resharded = resharded.reshape(width, 3 * lanes)
    s_gate_up, s_down_t = resharded[:, : 2 * lanes], resharded[:, 2 * lanes :]
    gain_rows = norm_gain.shape[0]
    latent_rows = latent_gain.shape[0]
    gains = jnp.concatenate([norm_gain, ffn_gain, latent_gain])
    gains = jnp.pad(gains[None], ((0, 15), (0, gain_rows - latent_rows)))
    ids_t, gates_t = expert_ids.T, gate_values.T
    numbers = jnp.arange(chips, dtype=jnp.int32)[:, None]
    gate_map = jnp.zeros((chips, length), f32)
    for k in range(topk_count):
        gate_map += jnp.where(ids_t[k][None, :] == numbers, gates_t[k][None, :], 0.0)
    mine = [w_query, w_out.T, w_up, rows_of(w_latent, core), gains, gate_map]
    shared = [False, False, False, True, False, False]
    pieces = (
        cut(0, mine[0].shape[0], GATHER_ORDERS)
        + cut(1, mine[1].shape[0], GATHER_ORDERS)
        + cut(2, mine[2].shape[0], ((1, (Z, Y, X)), (1, (Z, X, Y))))
        + cut(3, mine[3].shape[0], ((1, (X, Y, Z)),), core_last=True)
        + cut(4, mine[4].shape[0], ((1, (Z, Y, X)),))
        + cut(5, mine[5].shape[0], ((1, (Z, X, Y)),))
    )
    got = gather(grid, mine, shared, pieces, 1)
    full_query = got[0].reshape(width, -1)
    full_out_t = got[1].reshape(width, -1)
    full_up = got[2].reshape(kv_rank, -1)
    full_latent = got[3].reshape(width, -1)
    all_gains = got[4].reshape(chips, 16, -1)[:, 0].astype(f32)
    gain_one = all_gains[:, :gain_rows].reshape(-1)
    gain_two = all_gains[:, gain_rows : 2 * gain_rows].reshape(-1)
    gain_latent = all_gains[:, 2 * gain_rows : 2 * gain_rows + latent_rows].reshape(-1)
    gates = lax.dynamic_index_in_dim(got[5].reshape(chips, -1, length), chip, 1, keepdims=False)

    def all_rows(part, after):
        part, after = lax.optimization_barrier((part, after))
        return lax.all_gather(part, ("dp", "tensor"), axis=0, tiled=True), after

    cot_half = rows_of(cotangent, core)
    cot_bf = cot_half.astype(bf16)
    left = width * 3 // 8 // 128 * 128
    cot_left, gain_two = all_rows(cot_bf[:, :left], gain_two)

    cosine, sine = rope_tables(length)
    scale = (NOPE + ROPE) ** (-0.5)
    segment_row = segment_ids[0]
    position = jnp.arange(length, dtype=jnp.int32)
    allowed = (segment_row[:, None] == segment_row[None, :]) & (
        position[None, :] <= position[:, None]
    )
    tokens_f = hidden_in.astype(f32)
    normed_f, inverse_one = rms_forward(tokens_f, gain_one)
    normed = normed_f.astype(bf16)
    query_all = lax.optimization_barrier(jnp.dot(normed, full_query, preferred_element_type=f32))
    query_all = query_all.reshape(length, head_count, NOPE + ROPE)
    query_rope = rotate(query_all[..., NOPE:], cosine[:, None, :], sine[:, None, :])
    queries = jnp.concatenate([query_all[..., :NOPE], query_rope], axis=-1).astype(bf16)
    latent_all = jnp.dot(normed, full_latent, preferred_element_type=f32)
    latent = latent_all[:, :kv_rank]
    latent_normed, latent_inverse = rms_forward(latent, gain_latent)
    latent_bf = latent_normed.astype(bf16)
    key_rope = rotate(latent_all[:, kv_rank:], cosine, sine).astype(bf16)
    expanded = jnp.dot(latent_bf, full_up, preferred_element_type=f32).astype(bf16)
    expanded = expanded.reshape(length, head_count, NOPE + VDIM)
    key_all = jnp.concatenate(
        [expanded[..., :NOPE], jnp.broadcast_to(key_rope[:, None, :], (length, head_count, ROPE))],
        axis=-1,
    )
    values = expanded[..., NOPE:]
    scores = jnp.einsum("qhd,khd->hqk", queries, key_all, preferred_element_type=f32) * scale
    raw_probs = jnp.where(allowed[None], jnp.exp(scores), 0.0)
    totals = jnp.sum(raw_probs, axis=-1, keepdims=True)
    log_total = jnp.log(totals)
    attn_weights = (raw_probs / totals).astype(bf16)
    context = jnp.einsum("hqk,khd->qhd", attn_weights, values, preferred_element_type=f32)
    context = context.reshape(length, head_count * VDIM).astype(bf16)
    attended_part = lax.dot_general(
        context, full_out_t, (((1,), (1,)), ((), ())), preferred_element_type=f32
    )
    (other,) = pair(grid, [rows_of(attended_part, 1 - core)], False, 5)
    residual = rows_of(tokens_f, core) + (rows_of(attended_part, core) + other)
    ffn_f, inverse_two = rms_forward(residual, gain_two)
    ffn_in = ffn_f.astype(bf16)

    ffn_in, cot_left = lax.optimization_barrier((ffn_in, cot_left))
    (ffn_all,) = gather(grid, [ffn_in], [True], cut(0, half, GATHER_ORDERS, core_last=True), 2)
    ffn_all = ffn_all.reshape(-1, width)
    cot_right, ffn_all = all_rows(cot_bf[:, left:], ffn_all)

    routed = gates > 0.0
    triangle = (position[:, None] < position[None, :]).astype(bf16)
    slot = jnp.dot(routed.astype(bf16), triangle, preferred_element_type=f32).astype(jnp.int32)
    chosen = routed[:, None, :] & (slot[:, None, :] == jnp.arange(capacity, dtype=jnp.int32)[None, :, None])
    pick = chosen.astype(bf16)
    gate_slot = jnp.sum(jnp.where(chosen, gates[:, None, :], 0.0), axis=-1)[..., None]

    def take(rows):
        return jnp.einsum(
            "sct,std->scd", pick, rows.reshape(chips, length, -1), preferred_element_type=f32
        )

    def spread(rows, units, weight):
        return spread_rows(pick, rows.reshape(chips, capacity, width), units, weight)

    expert_rows = take(ffn_all).astype(bf16).reshape(-1, width)
    gate_rows = gate_slot.reshape(-1, 1)
    local_gate, local_up, local_down = expert_gate[0], expert_up[0], expert_down[0]
    gate_projected = jnp.dot(expert_rows, local_gate, preferred_element_type=f32)
    up_projected = jnp.dot(expert_rows, local_up, preferred_element_type=f32)
    expert_hidden = (jax.nn.silu(gate_projected) * up_projected).astype(bf16)
    expert_part = jnp.dot(expert_hidden, local_down, preferred_element_type=f32)
    weighted = (gate_rows * expert_part).astype(bf16)
    shared_gu = jnp.dot(ffn_all, s_gate_up, preferred_element_type=f32)
    shared_g, shared_u = shared_gu[:, :lanes], shared_gu[:, lanes:]
    shared_hidden = (jax.nn.silu(shared_g) * shared_u).astype(bf16)
    forward_part = spread(weighted, shared_hidden, s_down_t)
    block_shape = grid + (2, half, width)
    reduce_pieces = cut(0, half, REDUCE_ORDERS, core_first=True)
    forward_part, cot_left, cot_right = lax.optimization_barrier((forward_part, cot_left, cot_right))
    grad_rows = jnp.concatenate(
        [(gate_slot * take(part)).astype(bf16) for part in (cot_left, cot_right)], axis=-1
    ).reshape(-1, width)
    ffn_total = lax.psum_scatter(forward_part, ("dp", "tensor"), scatter_dimension=0, tiled=True)

    hidden_gradient = lax.dot_general(
        grad_rows, local_down, (((1,), (1,)), ((), ())), preferred_element_type=f32
    )
    gate_gradient = (hidden_gradient * up_projected * silu_slope(gate_projected)).astype(bf16)
    up_gradient = (hidden_gradient * jax.nn.silu(gate_projected)).astype(bf16)
    back_part = lax.dot_general(
        gate_gradient, local_gate, (((1,), (1,)), ((), ())), preferred_element_type=f32
    ) + lax.dot_general(up_gradient, local_up, (((1,), (1,)), ((), ())), preferred_element_type=f32)
    shared_hg = jnp.dot(cot_left, s_down_t[:left], preferred_element_type=f32) + jnp.dot(
        cot_right, s_down_t[left:], preferred_element_type=f32
    )
    grad_units = jnp.concatenate(
        [shared_hg * shared_u * silu_slope(shared_g), shared_hg * jax.nn.silu(shared_g)], axis=1
    ).astype(bf16)
    backward_part = spread(back_part.astype(bf16), grad_units, s_gate_up)
    (grad_ffn,) = reduce(grid, [backward_part.reshape(block_shape)], [True], reduce_pieces, 3)

    grad_expert_down = jnp.dot(expert_hidden.T, grad_rows, preferred_element_type=f32)
    grad_expert_gate = jnp.dot(expert_rows.T, gate_gradient, preferred_element_type=f32)
    gradient_expert_upward = jnp.dot(expert_rows.T, up_gradient, preferred_element_type=f32)
    over_rows = (((0,), (0,)), ((), ()))
    down_parts = [
        lax.dot_general(shared_hidden, part, over_rows, preferred_element_type=f32).astype(bf16)
        for part in (cot_left, cot_right)
    ]
    unit_grads = lax.dot_general(grad_units, ffn_all, over_rows, preferred_element_type=f32)
    unit_grads, *down_parts = lax.optimization_barrier((unit_grads.astype(bf16), *down_parts))
    shared_grads = jnp.concatenate([unit_grads, jnp.concatenate(down_parts, axis=1)])
    returned = lax.all_to_all(
        shared_grads.reshape(3 * lanes, chips, model_rows).transpose(1, 0, 2),
        "dp",
        split_axis=0,
        concat_axis=0,
        tiled=True,
    ).astype(f32)
    s_sgate, s_sup, s_sdown = (
        returned[:, i * lanes : i * lanes + part_units].reshape(-1, model_rows) for i in range(3)
    )
    s_sgate, s_sup = s_sgate.T, s_sup.T

    grad_res_part, g_fgain = rms_backward(residual, inverse_two, gain_two, grad_ffn)
    grad_residual = cot_half + grad_res_part
    (grad_attn,) = pair(grid, [grad_residual.astype(bf16)], True, 6)
    grad_attn = grad_attn.reshape(length, width)
    g_out_t = jnp.dot(grad_attn.T, context, preferred_element_type=f32)
    grad_context = (
        jnp.dot(grad_attn, full_out_t, preferred_element_type=f32)
        .astype(bf16)
        .reshape(length, head_count, VDIM)
    )
    probs = jnp.where(allowed[None], jnp.exp(scores - log_total), 0.0)
    weights_back = probs.astype(bf16)
    grad_values = jnp.einsum("hqk,qhd->khd", weights_back, grad_context, preferred_element_type=f32)
    grad_weights = jnp.einsum("qhd,khd->hqk", grad_context, values, preferred_element_type=f32)
    row_delta = jnp.sum(probs * grad_weights, axis=-1, keepdims=True)
    grad_scores = (probs * (grad_weights - row_delta) * scale).astype(bf16)
    grad_queries = jnp.einsum("hqk,khd->qhd", grad_scores, key_all, preferred_element_type=f32)
    grad_keys = jnp.einsum("hqk,qhd->khd", grad_scores, queries, preferred_element_type=f32)
    grad_qrope = rotate(grad_queries[..., NOPE:], cosine[:, None, :], -sine[:, None, :])
    grad_query_all = (
        jnp.concatenate([grad_queries[..., :NOPE], grad_qrope], axis=-1)
        .reshape(length, head_count * (NOPE + ROPE))
        .astype(bf16)
    )
    grad_expanded = (
        jnp.concatenate([grad_keys[..., :NOPE], grad_values], axis=-1)
        .reshape(length, head_count * (NOPE + VDIM))
        .astype(bf16)
    )
    g_up = jnp.dot(latent_bf.T, grad_expanded, preferred_element_type=f32)
    g_query = jnp.dot(normed.T, grad_query_all, preferred_element_type=f32)
    latent_part = lax.dot_general(
        grad_expanded, full_up, (((1,), (1,)), ((), ())), preferred_element_type=f32
    )
    rope_part = rotate(jnp.sum(grad_keys[..., NOPE:], axis=1), cosine, -sine)
    latent_part = jnp.concatenate([latent_part, rope_part], axis=-1)
    input_part = lax.dot_general(
        grad_query_all, full_query, (((1,), (1,)), ((), ())), preferred_element_type=f32
    )
    latent_other, input_other = pair(
        grid, [rows_of(latent_part, 1 - core), rows_of(input_part, 1 - core)], False, 7
    )
    latent_sum = rows_of(latent_part, core) + latent_other
    grad_latent, g_lgain = rms_backward(
        rows_of(latent, core), rows_of(latent_inverse, core), gain_latent, latent_sum[:, :kv_rank]
    )
    grad_latent_all = jnp.concatenate([grad_latent, latent_sum[:, kv_rank:]], axis=-1).astype(bf16)
    g_latent = jnp.dot(rows_of(normed, core).T, grad_latent_all, preferred_element_type=f32)
    grad_normed = (rows_of(input_part, core) + input_other) + lax.dot_general(
        grad_latent_all, full_latent, (((1,), (1,)), ((), ())), preferred_element_type=f32
    )
    grad_in_part, g_norm = rms_backward(
        rows_of(tokens_f, core), rows_of(inverse_one, core), gain_one, grad_normed
    )
    grad_input_half = grad_residual + grad_in_part

    g_gains = jnp.concatenate(
        [
            g_norm.reshape(chips, gain_rows),
            g_fgain.reshape(chips, gain_rows),
            jnp.pad(g_lgain.reshape(chips, latent_rows), ((0, 0), (0, gain_rows - latent_rows))),
        ],
        axis=1,
    )
    g_gains = jnp.pad(g_gains[:, None, :], ((0, 0), (0, 15), (0, 0)))
    terms = [
        g_query.astype(bf16).reshape(grid + (-1, g_query.shape[1])),
        g_out_t.astype(bf16).reshape(grid + (-1, g_out_t.shape[1])),
        g_up.astype(bf16).reshape(grid + (-1, g_up.shape[1])),
        g_latent.astype(bf16).reshape(grid + (2, -1, g_latent.shape[1])),
        g_gains.astype(bf16).reshape(grid + (16, -1)),
    ]
    pieces = (
        cut(0, terms[0].shape[-2], REDUCE_ORDERS)
        + cut(1, terms[1].shape[-2], REDUCE_ORDERS)
        + cut(2, terms[2].shape[-2], ((1, (X, Y, Z)), (1, (Y, X, Z))))
        + cut(3, terms[3].shape[-2], ((1, (Z, X, Y)),), core_first=True)
        + cut(4, terms[4].shape[-2], ((1, (X, Y, Z)),))
    )
    s_query, s_out_t, s_up, latent_half, gain_sums = reduce(
        grid, terms, [False, False, False, True, False], pieces, 4
    )
    ffn_total, gain_sums = lax.optimization_barrier((ffn_total, gain_sums))
    output_half = (residual + ffn_total.astype(f32)).astype(bf16)
    output, grad_input, s_latent, gain_sums = pair(
        grid, [output_half, grad_input_half, latent_half, gain_sums], True, 8
    )
    gain_sums = gain_sums[0, 0] + gain_sums[1, 0]
    return (
        output.reshape(length, width),
        grad_input.reshape(length, width),
        gain_sums[:gain_rows],
        s_query,
        s_latent.reshape(-1, s_latent.shape[-1]),
        gain_sums[2 * gain_rows : 2 * gain_rows + latent_rows],
        s_up,
        s_out_t.T,
        gain_sums[gain_rows : 2 * gain_rows],
        s_sgate,
        s_sup,
        s_sdown,
        grad_expert_gate[None],
        gradient_expert_upward[None],
        grad_expert_down[None],
    )


def chip_grid(mesh):
    coords = [tuple(getattr(device, "coords", ())) for device in mesh.devices[:, 0]]
    if any(len(spot) != 3 for spot in coords):
        return None
    low = [min(spot[axis] for spot in coords) for axis in range(3)]
    sizes = [max(spot[axis] for spot in coords) - low[axis] + 1 for axis in range(3)]
    steps = []
    for axis in range(3):
        steps.append(next((i for i, spot in enumerate(coords) if spot[axis] != low[axis]), 0))
    order = sorted(range(3), key=lambda axis: -steps[axis])
    grid = tuple(sizes[axis] for axis in order)
    for index, spot in enumerate(coords):
        for axis in reversed(order):
            if index % sizes[axis] != spot[axis] - low[axis]:
                return None
            index //= sizes[axis]
    return grid if min(grid) >= 2 else None


def solution(mesh):
    in_specs = (
        P("dp", None),
        P("dp"),
        P("dp", "tensor"),
        P("dp", None),
        P("dp"),
        P("dp", "tensor"),
        P("tensor", "dp"),
        P("dp"),
        P("dp", "tensor"),
        P("dp", "tensor"),
        P("tensor", "dp"),
        P("dp", None, "tensor"),
        P("dp", None, "tensor"),
        P("dp", "tensor", None),
        P("dp", None),
        P("dp", None),
        P("dp", None),
        P("dp", None),
    )
    out_specs = (
        P("dp", None),
        P("dp", None),
        P("dp"),
        P("dp", "tensor"),
        P("dp", None),
        P("dp"),
        P("dp", "tensor"),
        P("tensor", "dp"),
        P("dp"),
        P("dp", "tensor"),
        P("dp", "tensor"),
        P("tensor", "dp"),
        P("dp", None, "tensor"),
        P("dp", None, "tensor"),
        P("dp", "tensor", None),
    )
    grid = chip_grid(mesh)

    def step(*args):
        dense = grid is not None and 4 * args[15].shape[1] >= mesh.shape["dp"]
        body = functools.partial(dense_shards, grid) if dense else shards
        return jax.shard_map(
            body, mesh=mesh, in_specs=in_specs, out_specs=out_specs, check_vma=False
        )(*args)

    return step
```
